32 devices in a mesh: dp: 4 (over y, z), tp: 8 (over x, core).
Axes of the slice: x: 4, y: 2, z: 2, core: 2. Of those that a mesh axis runs over, the one named last changes fastest.
The devices are a block of a 4x4x8 slice.
Arguments:
- x_norm: bfloat16 [16384, 896], P(('dp', 'tp')), parts along dimension 0
- grad_y: bfloat16 [16384, 896], P(('dp', 'tp')), parts along dimension 0
- u_gate: bfloat16 [16384, 4864], P('dp', 'tp'), parts along dimension 0
- u_up: bfloat16 [16384, 4864], P('dp', 'tp'), parts along dimension 0
- w_gate: bfloat16 [896, 4864], P(None, 'tp')
- w_up: bfloat16 [896, 4864], P(None, 'tp')
- w_down: bfloat16 [4864, 896], P('tp')
- x_in: bfloat16 [16384, 896], P(('dp', 'tp')), parts along dimension 0
- gamma: bfloat16 [896], replicated
- grad_res: bfloat16 [16384, 896], P(('dp', 'tp')), parts along dimension 0
- attn_out: bfloat16 [16384, 896], P('dp', 'tp'), parts along dimension 0
- w_out: bfloat16 [896, 896], P('tp')
Outputs:
- output 1: bfloat16 [16384, 896], P(('dp', 'tp')), parts along dimension 0
- output 2: bfloat16 [16384, 896], P('dp', 'tp'), parts along dimension 0
- output 3: float32 [3584, 4864], P('dp', 'tp'), parts along dimension 0
- output 4: float32 [3584, 4864], P('dp', 'tp'), parts along dimension 0
- output 5: float32 [19456, 896], P(('dp', 'tp')), parts along dimension 0
- output 6: float32 [3584, 896], P(('dp', 'tp')), parts along dimension 0
There are 4 independent parts. The reference program is written for one: setup_inputs(seed, part) draws one part's arguments, and reference() takes and returns one part's arrays. A program takes and returns all parts, laid end to end along the dimension named above; an argument that names none is the same for every part.
All inputs are finite; a program needn't handle non-finite values.
Results may differ from the reference program's by a relative error of at most 0.0148603.
Values are sent between devices in bfloat16 or wider.
A program may use at most 768 MiB of HBM per device.

```python
import jax
import jax.numpy as jnp
from jax import lax

HIDDEN = 896
FFN_DIM = 4864
TOKENS = 4096
NORM_EPS = 1e-5


def setup_inputs(seed: int = 0, part: int = 0) -> dict:
    part_keys = jax.random.split(jax.random.fold_in(jax.random.key(seed), part), 7)
    weight_keys = jax.random.split(jax.random.key(seed + 1), 5)
    xin_keys = jax.random.split(part_keys[4], 2)
    act_shape = (TOKENS, HIDDEN)
    ffn_shape = (TOKENS, FFN_DIM)
    x_norm = jax.random.normal(part_keys[0], act_shape, jnp.float32)
    grad_y = jax.random.normal(part_keys[1], act_shape, jnp.float32)
    u_gate = jax.random.normal(part_keys[2], ffn_shape, jnp.float32)
    u_up = jax.random.normal(part_keys[3], ffn_shape, jnp.float32)
    xin_scale = jnp.exp(jax.random.uniform(xin_keys[0], (TOKENS, 1), jnp.float32, -1.0, 1.0))
    x_in = jax.random.normal(xin_keys[1], act_shape, jnp.float32) * xin_scale
    grad_res = 0.5 * jax.random.normal(part_keys[5], act_shape, jnp.float32)
    attn_out = jax.random.normal(part_keys[6], act_shape, jnp.float32)
    w_gate = jax.random.normal(weight_keys[0], (HIDDEN, FFN_DIM), jnp.float32) * HIDDEN ** -0.5
    w_up = jax.random.normal(weight_keys[1], (HIDDEN, FFN_DIM), jnp.float32) * HIDDEN ** -0.5
    w_down = jax.random.normal(weight_keys[2], (FFN_DIM, HIDDEN), jnp.float32) * FFN_DIM ** -0.5
    w_out = jax.random.normal(weight_keys[3], (HIDDEN, HIDDEN), jnp.float32) * HIDDEN ** -0.5
    gamma = 1.0 + 0.3 * jax.random.normal(weight_keys[4], (HIDDEN,), jnp.float32)
    return dict(
        x_norm=x_norm.astype(jnp.bfloat16),
        grad_y=grad_y.astype(jnp.bfloat16),
        u_gate=u_gate.astype(jnp.bfloat16),
        u_up=u_up.astype(jnp.bfloat16),
        w_gate=w_gate.astype(jnp.bfloat16),
        w_up=w_up.astype(jnp.bfloat16),
        w_down=w_down.astype(jnp.bfloat16),
        x_in=x_in.astype(jnp.bfloat16),
        gamma=gamma.astype(jnp.bfloat16),
        grad_res=grad_res.astype(jnp.bfloat16),
        attn_out=attn_out.astype(jnp.bfloat16),
        w_out=w_out.astype(jnp.bfloat16),
    )


def reference(x_norm, grad_y, u_gate, u_up, w_gate, w_up, w_down, x_in, gamma, grad_res, attn_out, w_out):
    gate_f = u_gate.astype(jnp.float32)
    up_f = u_up.astype(jnp.float32)
    sig_gate = jax.nn.sigmoid(gate_f)
    act_gate = gate_f * sig_gate
    silu_grad = sig_gate * (1.0 + gate_f * (1.0 - sig_gate))
    hidden_z = (act_gate * up_f).astype(jnp.bfloat16)
    gw_down = jnp.dot(hidden_z.T, grad_y, preferred_element_type=jnp.float32)
    grad_h = jnp.dot(grad_y, w_down.T, preferred_element_type=jnp.float32)
    grad_up = (grad_h * act_gate).astype(jnp.bfloat16)
    grad_gate = (grad_h * up_f * silu_grad).astype(jnp.bfloat16)
    grad_x = (jnp.dot(grad_gate, w_gate.T, preferred_element_type=jnp.float32)
              + jnp.dot(grad_up, w_up.T, preferred_element_type=jnp.float32)).astype(jnp.bfloat16)
    gw_gate = jnp.dot(x_norm.T, grad_gate, preferred_element_type=jnp.float32)
    gw_up = jnp.dot(x_norm.T, grad_up, preferred_element_type=jnp.float32)
    xin_f = x_in.astype(jnp.float32)
    inv_rms = lax.rsqrt(jnp.mean(xin_f * xin_f, axis=-1, keepdims=True) + NORM_EPS)
    scaled = grad_x.astype(jnp.float32) * gamma.astype(jnp.float32)
    proj_mean = jnp.mean(scaled * xin_f, axis=-1, keepdims=True)
    grad_sum = (grad_res.astype(jnp.float32)
                + inv_rms * (scaled - xin_f * (inv_rms * inv_rms) * proj_mean)).astype(jnp.bfloat16)
    grad_attn = jnp.dot(grad_sum, w_out.T, preferred_element_type=jnp.float32).astype(jnp.bfloat16)
    gw_out = jnp.dot(attn_out.T, grad_sum, preferred_element_type=jnp.float32)
    return grad_sum, grad_attn, gw_gate, gw_up, gw_down, gw_out
```

```python
import functools

import jax
import jax.numpy as jnp
from jax import lax
from jax.experimental import pallas as pl
from jax.experimental.pallas import tpu as pltpu
from jax.sharding import PartitionSpec as P

NORM_EPS = 1e-5
F32 = jnp.float32
BF16 = jnp.bfloat16
ROWS_ROWS = (((0,), (0,)), ((), ()))
COLS_COLS = (((1,), (1,)), ((), ()))
COLS_ROWS = (((1,), (0,)), ((), ()))
MESH = pl.DeviceIdType.MESH


def dot(a, b, dims):
    return lax.dot_general(a, b, dims, preferred_element_type=F32)


def kernel(tp, x_hbm, gy_hbm, ug_hbm, uu_hbm, wg_hbm, wu_hbm, wd_hbm, xin_hbm, gamma_ref, gr_hbm, o_hbm, wo_hbm,
           ds_out, do_out, dwg_out, dwu_out, dwd_out, dwo_out,
           gy, xb, part, peer, hop, froml, fromr, du, wgu, wd, wo, dwgu, dwd, dwo, ugb, uub, ob, dob, xin, gr,
           s_gy, r_gy, s_x, r_x, s_p, r_p, s_h, r_h, s_t, r_t, s_ds, r_ds,
           l_w, l_own, l_u, l_o, l_do, l_tok, l_out):
    half = gy.shape[1]
    cols = wd.shape[0]
    quarter = half // 2
    me = lax.axis_index("tp")
    core = lax.rem(me, 2)
    right = lax.rem(me + 2, tp)
    left = lax.rem(me + tp - 2, tp)
    partner = me + 1 - 2 * core

    def send(src, dst, ssem, rsem, dev):
        return pltpu.make_async_remote_copy(
            src_ref=src, dst_ref=dst, send_sem=ssem, recv_sem=rsem, device_id={"tp": dev}, device_id_type=MESH)

    def slot_row(k):
        g, b, i = k // 4, lax.rem(k, 4) // 2, lax.rem(k, 2)
        dx = jnp.where(g == 0, 0, jnp.where(g == 3, 2, 2 * i - 1))
        h = jnp.where(g == 2, 1 - i, i)
        chip = lax.rem(me // 2 + dx + tp // 2, tp // 2)
        shard = 2 * chip + lax.rem(core + b, 2)
        return pl.multiple_of((2 * shard + h) * half, half)

    def u_copies(k):
        tokens = pl.ds(slot_row(k), half)
        at = lax.rem(k, 2)
        return (pltpu.make_async_copy(ug_hbm.at[:, tokens], ugb.at[at], l_u.at[2 * at]),
                pltpu.make_async_copy(uu_hbm.at[:, tokens], uub.at[at], l_u.at[2 * at + 1]))

    def o_copy(n):
        tokens = pl.ds(pl.multiple_of(slot_row(n // 2) + lax.rem(n, 2) * quarter, quarter), quarter)
        return pltpu.make_async_copy(o_hbm.at[:, tokens], ob.at[n], l_o.at[n])

    def own(hbm, h):
        return hbm.at[pl.ds(h * half, half)]

    barrier = pltpu.get_barrier_semaphore()
    for dev in (left, right, partner):
        pl.semaphore_signal(barrier, inc=1, device_id={"tp": dev}, device_id_type=MESH)
    pl.semaphore_wait(barrier, 3)

    def send_own(hbm, buf, ssem, rsem):
        for src, dst, dev in ((0, 4, right), (1, 5, left), (1, 8, right), (0, 9, left), (0, 2, partner), (1, 3, partner)):
            send(own(hbm, src), buf.at[dst], ssem.at[dst], rsem.at[dst], dev).start()

    def arrived(buf, ssem, rsem, k):
        send(buf.at[k], buf.at[k], ssem.at[k], rsem.at[k], partner).wait_recv()

    def drain(buf, ssem, k):
        send(buf.at[k], buf.at[k], ssem.at[k], ssem.at[k], partner).wait_send()

    def gather_step(buf, ssem, rsem, k, also):
        place = lax.rem(k, 4)

        @pl.when((place == 0) & (k > 0))
        def _():
            arrived(buf, ssem, rsem, k)
            arrived(buf, ssem, rsem, k + 1)

            @pl.when(k == 4)
            def _():
                send(buf.at[4], buf.at[12], ssem.at[12], rsem.at[12], right).start()
                send(buf.at[5], buf.at[13], ssem.at[13], rsem.at[13], left).start()

            send(buf.at[k], buf.at[k + 2], ssem.at[k + 2], rsem.at[k + 2], partner).start()
            send(buf.at[k + 1], buf.at[k + 3], ssem.at[k + 3], rsem.at[k + 3], partner).start()
            if also is not None:
                pl.when(k == 4)(also)

        @pl.when(place >= 2)
        def _():
            arrived(buf, ssem, rsem, k)

    send_own(gy_hbm, gy, s_gy, r_gy)
    for h in range(2):
        pltpu.make_async_copy(own(gy_hbm, h), gy.at[h], l_own.at[h]).start()
        pltpu.make_async_copy(own(x_hbm, h), xb.at[h], l_own.at[2 + h]).start()
    weights = ((wd_hbm, wd), (wg_hbm, wgu.at[pl.ds(0, cols)]), (wu_hbm, wgu.at[pl.ds(cols, cols)]), (wo_hbm, wo))
    for i, (src, dst) in enumerate(weights):
        pltpu.make_async_copy(src, dst, l_w.at[i]).start()
    for c in u_copies(0):
        c.start()
    pltpu.make_async_copy(xin_hbm, xin, l_tok.at[0]).start()
    pltpu.make_async_copy(gr_hbm, gr, l_tok.at[1]).start()

    @pl.loop(0, 32)
    def _(n):
        o_copy(n).start()

    dwd[...] = jnp.zeros_like(dwd)
    dwgu[...] = jnp.zeros_like(dwgu)
    dwo[...] = jnp.zeros_like(dwo)
    for i, (src, dst) in enumerate(weights):
        pltpu.make_async_copy(src, dst, l_w.at[i]).wait()
    for h in range(2):
        pltpu.make_async_copy(own(gy_hbm, h), gy.at[h], l_own.at[h]).wait()
        pltpu.make_async_copy(own(x_hbm, h), xb.at[h], l_own.at[2 + h]).wait()

    def part_copy(k):
        j = (k // 4) * 2 + lax.rem(k, 2)
        return send(part.at[k], peer.at[j], s_p.at[j], r_p.at[j], partner)

    @pl.loop(0, 16)
    def _(k):
        @pl.when(k + 1 < 16)
        def _():
            for c in u_copies(k + 1):
                c.start()

        @pl.when((k > 0) & (lax.rem(k + 3, 4) >= 2))
        def _():
            part_copy(k - 1).start()

        gather_step(gy, s_gy, r_gy, k, lambda: send_own(x_hbm, xb, s_x, r_x))
        for c in u_copies(k):
            c.wait()
        at = lax.rem(k, 2)
        gyk = gy[k]
        gh = dot(wd[...], gyk, COLS_COLS)
        gate = ugb[at].astype(F32)
        up = uub[at].astype(F32)
        sig = jax.nn.sigmoid(gate)
        act = gate * sig
        silu = sig * (1.0 + gate * (1.0 - sig))
        z = (act * up).astype(BF16)
        du_up = (gh * act).astype(BF16)
        du_gate = (gh * up * silu).astype(BF16)
        du[k, pl.ds(0, cols)] = du_gate
        du[k, pl.ds(cols, cols)] = du_up
        dwd[...] += dot(z, gyk, COLS_ROWS)
        part[k] = dot(du[k], wgu[...], ROWS_ROWS).astype(BF16)

    part_copy(15).start()

    @pl.loop(2, 16)
    def _(k):
        drain(gy, s_gy, k)

    def add_peer(k, more=()):
        j = (k // 4) * 2 + k % 2
        t = part[k].astype(F32) + peer[j].astype(F32)
        for m in more:
            t = t + m[...].astype(F32)
        part[k] = t.astype(BF16)

    def q(ref, i):
        return ref.at[pl.ds(i * quarter, quarter)]

    def peer_arrived(j):
        send(peer.at[j], peer.at[j], s_p.at[j], r_p.at[j], partner).wait_recv()

    for j in range(8):
        peer_arrived(j)

    def hop_copy(k, i):
        side = k - 12
        return send(q(part.at[k], i), q(hop.at[side], i), s_h.at[2 * side + i], r_h.at[2 * side + i], (right, left)[side])

    for k in (12, 13):
        add_peer(k)
    for i in range(2):
        for k in (12, 13):
            hop_copy(k, i).start()

    def dw_step(j):
        xk = xb[pl.ds(2 * j, 2)].reshape(2 * half, xb.shape[2])
        duk = jnp.concatenate((du[2 * j], du[2 * j + 1]), axis=1)
        dwgu[...] += dot(duk, xk, COLS_ROWS)

    def tail_copy(side, qi):
        k = ((9, 5), (4, 8))[side][qi // 2]
        dst = (froml, fromr)[side].at[qi]
        return send(q(part.at[k], qi % 2), dst, s_t.at[4 * side + qi], r_t.at[4 * side + qi], (right, left)[side])

    tail_order = ((2, 0, 3, 1), (0, 2, 1, 3))

    def tails():
        add_peer(5)
        add_peer(4)
        for side in range(2):
            for i in range(2):
                hop_copy(12 + side, i).wait_recv()
        add_peer(9, (hop.at[0],))
        add_peer(8, (hop.at[1],))
        for n in range(4):
            for side in range(2):
                tail_copy(side, tail_order[side][n]).start()

    @pl.loop(0, 8)
    def _(j):
        pl.when(j == 6)(tails)
        gather_step(xb, s_x, r_x, 2 * j, None)

        @pl.when(lax.rem(j, 2) == 1)
        def _():
            arrived(xb, s_x, r_x, 2 * j + 1)

        dw_step(j)

    outs = ((dwgu.at[pl.ds(0, cols)], dwg_out), (dwgu.at[pl.ds(cols, cols)], dwu_out), (dwd, dwd_out))
    for i, (src, dst) in enumerate(outs):
        pltpu.make_async_copy(src, dst, l_out.at[i]).start()

    ds = gy
    pltpu.make_async_copy(xin_hbm, xin, l_tok.at[0]).wait()
    pltpu.make_async_copy(gr_hbm, gr, l_tok.at[1]).wait()
    gamma = gamma_ref[...].astype(F32)

    def norm_quarter(qi):
        h, i = qi // 2, qi % 2
        tail_copy(0, qi).wait_recv()
        tail_copy(1, qi).wait_recv()
        step = 32

        @pl.loop(0, quarter // step)
        def _(n):
            rows = pl.ds(pl.multiple_of(n * step, step), step)
            inner = pl.ds(pl.multiple_of(i * quarter + n * step, step), step)
            tokens = pl.ds(pl.multiple_of(qi * quarter + n * step, step), step)
            dx = (part[h, inner].astype(F32) + peer[h, inner].astype(F32)
                  + froml[qi, rows].astype(F32) + fromr[qi, rows].astype(F32)).astype(BF16)
            xf = xin[tokens].astype(F32)
            inv = lax.rsqrt(jnp.mean(xf * xf, axis=-1, keepdims=True) + NORM_EPS)
            scaled = dx.astype(F32) * gamma
            proj = jnp.mean(scaled * xf, axis=-1, keepdims=True)
            ds[h, inner] = (gr[tokens].astype(F32) + inv * (scaled - xf * (inv * inv) * proj)).astype(BF16)

    def ds_copy(src, dst, i, dev):
        n = 2 * dst + i
        return send(q(ds.at[src], i), q(ds.at[dst], i), s_ds.at[n], r_ds.at[n], dev)

    for i in range(2):
        for h in (0, 1):
            norm_quarter(2 * h + i)
        for src, dst, dev in ((0, 4, right), (1, 5, left), (1, 8, right), (0, 9, left), (0, 2, partner), (1, 3, partner)):
            ds_copy(src, dst, i, dev).start()
    for h in range(2):
        pltpu.make_async_copy(ds.at[h], ds_out.at[pl.ds(h * half, half)], l_out.at[4 + h]).start()

    @pl.loop(0, 32)
    def _(n):
        o_copy(n).wait()

    def do_copy(k, i):
        tokens = pl.ds(pl.multiple_of(slot_row(k) + i * quarter, quarter), quarter)
        return pltpu.make_async_copy(dob.at[2 * k + i], do_out.at[:, tokens], l_do.at[2 * k + i])

    @pl.loop(0, 16)
    def _(u):
        v, w = u - 4, u - 12
        i = jnp.where(u < 4, lax.rem(u, 2), jnp.where(u < 12, v // 4, w // 2))
        k = jnp.where(u < 4, 2 * (u // 2), jnp.where(u < 12, 4 + 2 * lax.rem(v, 4), 12 + 2 * lax.rem(w, 2)))

        @pl.when(k > 0)
        def _():
            for d in range(2):
                n = 2 * (k + d) + i
                block = q(ds.at[k + d], i)
                send(block, block, s_ds.at[n], r_ds.at[n], partner).wait_recv()

        @pl.when(k == 4)
        def _():
            for src, dst, dev in ((4, 12, right), (5, 13, left)):
                n = 2 * dst + i
                send(q(ds.at[src], i), q(ds.at[dst], i), s_ds.at[n], r_ds.at[n], dev).start()

        @pl.when((k > 0) & (lax.rem(k, 4) == 0))
        def _():
            for d in range(2):
                n = 2 * (k + 2 + d) + i
                send(q(ds.at[k + d], i), q(ds.at[k + 2 + d], i), s_ds.at[n], r_ds.at[n], partner).start()

        rows = pl.ds(pl.multiple_of(i * quarter, quarter), quarter)
        for d in range(2):
            block = ds[k + d, rows]
            n = 2 * (k + d) + i
            dob[n] = dot(wo[...], block, COLS_COLS).astype(BF16)
            dwo[...] += dot(ob[n], block, COLS_ROWS)
        for d in range(2):
            do_copy(k + d, i).start()

    pltpu.make_async_copy(dwo, dwo_out, l_out.at[3]).start()

    for i, (src, dst) in enumerate((*outs, (dwo, dwo_out))):
        pltpu.make_async_copy(src, dst, l_out.at[i]).wait()
    for h in range(2):
        pltpu.make_async_copy(ds.at[h], ds_out.at[pl.ds(h * half, half)], l_out.at[4 + h]).wait()

    @pl.loop(0, 32)
    def _(n):
        do_copy(n // 2, lax.rem(n, 2)).wait()

    @pl.loop(2, 16)
    def _(k):
        drain(xb, s_x, k)

    @pl.loop(4, 32)
    def _(n):
        block = q(ds.at[n // 2], 0)
        send(block, block, s_ds.at[n], s_ds.at[n], partner).wait_send()

    for j in range(8):
        send(peer.at[j], peer.at[j], s_p.at[j], s_p.at[j], partner).wait_send()
    for side in range(2):
        for i in range(2):
            hop_copy(12 + side, i).wait_send()
        for qi in range(4):
            tail_copy(side, qi).wait_send()


def solution(mesh):
    tp = mesh.shape["tp"]
    token_spec = P(("dp", "tp"), None)
    split_cols = P("dp", "tp")
    weight_cols = P(None, "tp")
    weight_rows = P("tp", None)

    def local_backward(x_norm, grad_y, u_gate, u_up, w_gate, w_up, w_down, x_in, gamma, grad_res, attn_out, w_out):
        rows, hid = x_norm.shape
        tokens, cols = u_gate.shape
        ocols = attn_out.shape[1]
        half = rows // 2
        quarter = half // 2
        any_spec = pl.BlockSpec(memory_space=pl.ANY)
        vmem_spec = pl.BlockSpec(memory_space=pltpu.VMEM)
        dma = pltpu.SemaphoreType.DMA
        ds, do, dwg, dwu, dwd, dwo = pl.pallas_call(
            functools.partial(kernel, tp),
            out_shape=(
                jax.ShapeDtypeStruct((rows, hid), BF16),
                jax.ShapeDtypeStruct((ocols, tokens), BF16),
                jax.ShapeDtypeStruct((cols, hid), F32),
                jax.ShapeDtypeStruct((cols, hid), F32),
                jax.ShapeDtypeStruct((cols, hid), F32),
                jax.ShapeDtypeStruct((ocols, hid), F32),
            ),
            in_specs=[any_spec] * 8 + [vmem_spec] + [any_spec] * 3,
            out_specs=(any_spec,) * 6,
            scratch_shapes=[
                pltpu.VMEM((16, half, hid), BF16),
                pltpu.VMEM((16, half, hid), BF16),
                pltpu.VMEM((16, half, hid), BF16),
                pltpu.VMEM((8, half, hid), BF16),
                pltpu.VMEM((2, half, hid), BF16),
                pltpu.VMEM((4, quarter, hid), BF16),
                pltpu.VMEM((4, quarter, hid), BF16),
                pltpu.VMEM((16, 2 * cols, half), BF16),
                pltpu.VMEM((2 * cols, hid), BF16),
                pltpu.VMEM((cols, hid), BF16),
                pltpu.VMEM((ocols, hid), BF16),
                pltpu.VMEM((2 * cols, hid), F32),
                pltpu.VMEM((cols, hid), F32),
                pltpu.VMEM((ocols, hid), F32),
                pltpu.VMEM((2, cols, half), BF16),
                pltpu.VMEM((2, cols, half), BF16),
                pltpu.VMEM((32, ocols, quarter), BF16),
                pltpu.VMEM((32, ocols, quarter), BF16),
                pltpu.VMEM((rows, hid), BF16),
                pltpu.VMEM((rows, hid), BF16),
                dma((16,)), dma((16,)),
                dma((16,)), dma((16,)),
                dma((8,)), dma((8,)),
                dma((4,)), dma((4,)),
                dma((8,)), dma((8,)),
                dma((32,)), dma((32,)),
                dma((4,)), dma((4,)), dma((4,)), dma((32,)), dma((32,)), dma((2,)), dma((6,)),
            ],
            compiler_params=pltpu.CompilerParams(
                collective_id=0, has_side_effects=True, vmem_limit_bytes=67_000_000),
            name="layer_backward",
        )(x_norm, grad_y, u_gate.T, u_up.T, w_gate.T, w_up.T, w_down, x_in, gamma.reshape(1, hid), grad_res, attn_out.T,
          w_out)
        return ds, do.T, dwg.T, dwu.T, dwd, dwo

    return jax.shard_map(
        local_backward,
        mesh=mesh,
        in_specs=(token_spec, token_spec, split_cols, split_cols, weight_cols, weight_cols, weight_rows,
                  token_spec, P(None), token_spec, split_cols, weight_rows),
        out_specs=(token_spec, split_cols, split_cols, split_cols, token_spec, token_spec),
        check_vma=False,
    )
```

```python
import functools

import jax
import jax.numpy as jnp
from jax import lax
from jax.experimental import pallas as pl
from jax.experimental.pallas import tpu as pltpu
from jax.sharding import PartitionSpec as P

NORM_EPS = 1e-5
F32 = jnp.float32
BF16 = jnp.bfloat16
ROWS_ROWS = (((0,), (0,)), ((), ()))
COLS_COLS = (((1,), (1,)), ((), ()))
COLS_ROWS = (((1,), (0,)), ((), ()))
MESH = pl.DeviceIdType.MESH


def dot(a, b, dims):
    return lax.dot_general(a, b, dims, preferred_element_type=F32)


def slot_token(tp, half, k):
    me = lax.axis_index("tp")
    g, b, i = k // 4, lax.rem(k, 4) // 2, lax.rem(k, 2)
    dx = jnp.where(g == 0, 0, jnp.where(g == 3, 2, 2 * i - 1))
    h = jnp.where(g == 2, 1 - i, i)
    chip = lax.rem(me // 2 + dx + tp // 2, tp // 2)
    shard = 2 * chip + lax.rem(lax.rem(me, 2) + b, 2)
    return pl.multiple_of((2 * shard + h) * half, half)


def write_kernel(tp, half, dso, dob, dwgu, dwd, dwo, ds_out, do_out, dwg_out, dwu_out, dwd_out, dwo_out, sem, sem_do):
    cols, quarter = dwd.shape[0], half // 2
    copies = [pltpu.make_async_copy(src, dst, sem.at[i]) for i, (src, dst) in enumerate((
        (dwgu.at[pl.ds(0, cols)], dwg_out), (dwgu.at[pl.ds(cols, cols)], dwu_out), (dwd, dwd_out), (dso, ds_out),
        (dwo, dwo_out)))]

    def do_copy(n):
        tokens = pl.ds(pl.multiple_of(slot_token(tp, half, n // 2) + lax.rem(n, 2) * quarter, quarter), quarter)
        return pltpu.make_async_copy(dob.at[n], do_out.at[:, tokens], sem_do.at[n])

    for c in copies:
        c.start()

    @pl.loop(0, 2 * 2 * tp)
    def _(n):
        do_copy(n).start()

    @pl.loop(0, 2 * 2 * tp)
    def _(n):
        do_copy(n).wait()

    for c in copies:
        c.wait()


def kernel(tp, x_hbm, gy_hbm, ug_hbm, uu_hbm, wg_hbm, wu_hbm, wd_hbm, xin_hbm, gamma_ref, gr_hbm, o_hbm, wo_hbm,
           dso, dob, dwgu, dwd, dwo,
           gy, xb, part, peer, hop, froml, fromr, du, wgu, wd, wo, ugb, uub, ob, xin, gr,
           s_gy, r_gy, s_x, r_x, s_p, r_p, s_h, r_h, s_t, r_t, s_ds, r_ds,
           l_w, l_own, l_u, l_o, l_tok):
    half = gy.shape[1]
    cols = wd.shape[0]
    quarter = half // 2
    me = lax.axis_index("tp")
    right = lax.rem(me + 2, tp)
    left = lax.rem(me + tp - 2, tp)
    partner = me + 1 - 2 * lax.rem(me, 2)
    slot_row = functools.partial(slot_token, tp, half)

    def send(src, dst, ssem, rsem, dev):
        return pltpu.make_async_remote_copy(
            src_ref=src, dst_ref=dst, send_sem=ssem, recv_sem=rsem, device_id={"tp": dev}, device_id_type=MESH)

    def u_copies(k):
        tokens = pl.ds(slot_row(k), half)
        at = lax.rem(k, 2)
        return (pltpu.make_async_copy(ug_hbm.at[:, tokens], ugb.at[at], l_u.at[2 * at]),
                pltpu.make_async_copy(uu_hbm.at[:, tokens], uub.at[at], l_u.at[2 * at + 1]))

    def o_copy(n):
        tokens = pl.ds(pl.multiple_of(slot_row(n // 2) + lax.rem(n, 2) * quarter, quarter), quarter)
        return pltpu.make_async_copy(o_hbm.at[:, tokens], ob.at[n], l_o.at[n])

    def own(hbm, h):
        return hbm.at[pl.ds(h * half, half)]

    barrier = pltpu.get_barrier_semaphore()
    for dev in (left, right, partner):
        pl.semaphore_signal(barrier, inc=1, device_id={"tp": dev}, device_id_type=MESH)
    pl.semaphore_wait(barrier, 3)

    def send_own(hbm, buf, ssem, rsem):
        for src, dst, dev in ((0, 4, right), (1, 5, left), (1, 8, right), (0, 9, left), (0, 2, partner), (1, 3, partner)):
            send(own(hbm, src), buf.at[dst], ssem.at[dst], rsem.at[dst], dev).start()

    def arrived(buf, ssem, rsem, k):
        send(buf.at[k], buf.at[k], ssem.at[k], rsem.at[k], partner).wait_recv()

    def drain(buf, ssem, k):
        send(buf.at[k], buf.at[k], ssem.at[k], ssem.at[k], partner).wait_send()

    def gather_step(buf, ssem, rsem, k, also):
        place = lax.rem(k, 4)

        @pl.when((place == 0) & (k > 0))
        def _():
            arrived(buf, ssem, rsem, k)
            arrived(buf, ssem, rsem, k + 1)

            @pl.when(k == 4)
            def _():
                send(buf.at[4], buf.at[12], ssem.at[12], rsem.at[12], right).start()
                send(buf.at[5], buf.at[13], ssem.at[13], rsem.at[13], left).start()

            send(buf.at[k], buf.at[k + 2], ssem.at[k + 2], rsem.at[k + 2], partner).start()
            send(buf.at[k + 1], buf.at[k + 3], ssem.at[k + 3], rsem.at[k + 3], partner).start()
            if also is not None:
                pl.when(k == 4)(also)

        @pl.when(place >= 2)
        def _():
            arrived(buf, ssem, rsem, k)

    send_own(gy_hbm, gy, s_gy, r_gy)
    for h in range(2):
        pltpu.make_async_copy(own(gy_hbm, h), gy.at[h], l_own.at[h]).start()
        pltpu.make_async_copy(own(x_hbm, h), xb.at[h], l_own.at[2 + h]).start()
    weights = ((wd_hbm, wd), (wg_hbm, wgu.at[pl.ds(0, cols)]), (wu_hbm, wgu.at[pl.ds(cols, cols)]), (wo_hbm, wo))
    for i, (src, dst) in enumerate(weights):
        pltpu.make_async_copy(src, dst, l_w.at[i]).start()
    for c in u_copies(0):
        c.start()
    pltpu.make_async_copy(xin_hbm, xin, l_tok.at[0]).start()
    pltpu.make_async_copy(gr_hbm, gr, l_tok.at[1]).start()

    @pl.loop(0, 32)
    def _(n):
        o_copy(n).start()

    dwd[...] = jnp.zeros_like(dwd)
    dwgu[...] = jnp.zeros_like(dwgu)
    dwo[...] = jnp.zeros_like(dwo)
    for i, (src, dst) in enumerate(weights):
        pltpu.make_async_copy(src, dst, l_w.at[i]).wait()
    for h in range(2):
        pltpu.make_async_copy(own(gy_hbm, h), gy.at[h], l_own.at[h]).wait()
        pltpu.make_async_copy(own(x_hbm, h), xb.at[h], l_own.at[2 + h]).wait()

    def part_copy(k):
        j = (k // 4) * 2 + lax.rem(k, 2)
        return send(part.at[k], peer.at[j], s_p.at[j], r_p.at[j], partner)

    @pl.loop(0, 16)
    def _(k):
        @pl.when(k + 1 < 16)
        def _():
            for c in u_copies(k + 1):
                c.start()

        @pl.when((k > 0) & (lax.rem(k + 3, 4) >= 2))
        def _():
            part_copy(k - 1).start()

        gather_step(gy, s_gy, r_gy, k, lambda: send_own(x_hbm, xb, s_x, r_x))
        for c in u_copies(k):
            c.wait()
        at = lax.rem(k, 2)
        gyk = gy[k]
        gh = dot(wd[...], gyk, COLS_COLS)
        gate = ugb[at].astype(F32)
        up = uub[at].astype(F32)
        sig = jax.nn.sigmoid(gate)
        act = gate * sig
        silu = sig * (1.0 + gate * (1.0 - sig))
        z = (act * up).astype(BF16)
        du_up = (gh * act).astype(BF16)
        du_gate = (gh * up * silu).astype(BF16)
        du[k, pl.ds(0, cols)] = du_gate
        du[k, pl.ds(cols, cols)] = du_up
        dwd[...] += dot(z, gyk, COLS_ROWS)
        part[k] = dot(du[k], wgu[...], ROWS_ROWS).astype(BF16)

    part_copy(15).start()

    @pl.loop(2, 16)
    def _(k):
        drain(gy, s_gy, k)

    def add_peer(k, more=()):
        j = (k // 4) * 2 + k % 2
        t = part[k].astype(F32) + peer[j].astype(F32)
        for m in more:
            t = t + m[...].astype(F32)
        part[k] = t.astype(BF16)

    def q(ref, i):
        return ref.at[pl.ds(i * quarter, quarter)]

    def peer_arrived(j):
        send(peer.at[j], peer.at[j], s_p.at[j], r_p.at[j], partner).wait_recv()

    for j in range(8):
        peer_arrived(j)

    def hop_copy(k, i):
        side = k - 12
        return send(q(part.at[k], i), q(hop.at[side], i), s_h.at[2 * side + i], r_h.at[2 * side + i], (right, left)[side])

    for k in (12, 13):
        add_peer(k)
    for i in range(2):
        for k in (12, 13):
            hop_copy(k, i).start()

    def dw_step(j):
        xk = xb[pl.ds(2 * j, 2)].reshape(2 * half, xb.shape[2])
        duk = jnp.concatenate((du[2 * j], du[2 * j + 1]), axis=1)
        dwgu[...] += dot(duk, xk, COLS_ROWS)

    def tail_copy(side, qi):
        k = ((9, 5), (4, 8))[side][qi // 2]
        dst = (froml, fromr)[side].at[qi]
        return send(q(part.at[k], qi % 2), dst, s_t.at[4 * side + qi], r_t.at[4 * side + qi], (right, left)[side])

    tail_order = ((2, 0, 3, 1), (0, 2, 1, 3))

    def tails():
        add_peer(5)
        add_peer(4)
        for side in range(2):
            for i in range(2):
                hop_copy(12 + side, i).wait_recv()
        add_peer(9, (hop.at[0],))
        add_peer(8, (hop.at[1],))
        for n in range(4):
            for side in range(2):
                tail_copy(side, tail_order[side][n]).start()

    @pl.loop(0, 8)
    def _(j):
        pl.when(j == 6)(tails)
        gather_step(xb, s_x, r_x, 2 * j, None)

        @pl.when(lax.rem(j, 2) == 1)
        def _():
            arrived(xb, s_x, r_x, 2 * j + 1)

        dw_step(j)

    ds = gy
    pltpu.make_async_copy(xin_hbm, xin, l_tok.at[0]).wait()
    pltpu.make_async_copy(gr_hbm, gr, l_tok.at[1]).wait()
    gamma = gamma_ref[...].astype(F32).reshape(1, gamma_ref.shape[0])

    def norm_quarter(qi):
        h, i = qi // 2, qi % 2
        tail_copy(0, qi).wait_recv()
        tail_copy(1, qi).wait_recv()
        step = 32

        @pl.loop(0, quarter // step)
        def _(n):
            rows = pl.ds(pl.multiple_of(n * step, step), step)
            inner = pl.ds(pl.multiple_of(i * quarter + n * step, step), step)
            tokens = pl.ds(pl.multiple_of(qi * quarter + n * step, step), step)
            dx = (part[h, inner].astype(F32) + peer[h, inner].astype(F32)
                  + froml[qi, rows].astype(F32) + fromr[qi, rows].astype(F32)).astype(BF16)
            xf = xin[tokens].astype(F32)
            inv = lax.rsqrt(jnp.mean(xf * xf, axis=-1, keepdims=True) + NORM_EPS)
            scaled = dx.astype(F32) * gamma
            proj = jnp.mean(scaled * xf, axis=-1, keepdims=True)
            out = (gr[tokens].astype(F32) + inv * (scaled - xf * (inv * inv) * proj)).astype(BF16)
            ds[h, inner] = out
            dso[tokens] = out

    def ds_copy(src, dst, i, dev):
        n = 2 * dst + i
        return send(q(ds.at[src], i), q(ds.at[dst], i), s_ds.at[n], r_ds.at[n], dev)

    for i in range(2):
        for h in (0, 1):
            norm_quarter(2 * h + i)
        for src, dst, dev in ((0, 4, right), (1, 5, left), (1, 8, right), (0, 9, left), (0, 2, partner), (1, 3, partner)):
            ds_copy(src, dst, i, dev).start()

    @pl.loop(0, 32)
    def _(n):
        o_copy(n).wait()

    @pl.loop(0, 16)
    def _(u):
        v, w = u - 4, u - 12
        i = jnp.where(u < 4, lax.rem(u, 2), jnp.where(u < 12, v // 4, w // 2))
        k = jnp.where(u < 4, 2 * (u // 2), jnp.where(u < 12, 4 + 2 * lax.rem(v, 4), 12 + 2 * lax.rem(w, 2)))

        @pl.when(k > 0)
        def _():
            for d in range(2):
                n = 2 * (k + d) + i
                block = q(ds.at[k + d], i)
                send(block, block, s_ds.at[n], r_ds.at[n], partner).wait_recv()

        @pl.when(k == 4)
        def _():
            for src, dst, dev in ((4, 12, right), (5, 13, left)):
                n = 2 * dst + i
                send(q(ds.at[src], i), q(ds.at[dst], i), s_ds.at[n], r_ds.at[n], dev).start()

        @pl.when((k > 0) & (lax.rem(k, 4) == 0))
        def _():
            for d in range(2):
                n = 2 * (k + 2 + d) + i
                send(q(ds.at[k + d], i), q(ds.at[k + 2 + d], i), s_ds.at[n], r_ds.at[n], partner).start()

        rows = pl.ds(pl.multiple_of(i * quarter, quarter), quarter)
        for d in range(2):
            block = ds[k + d, rows]
            n = 2 * (k + d) + i
            dob[n] = dot(wo[...], block, COLS_COLS).astype(BF16)
            dwo[...] += dot(ob[n], block, COLS_ROWS)

    @pl.loop(2, 16)
    def _(k):
        drain(xb, s_x, k)

    @pl.loop(4, 32)
    def _(n):
        block = q(ds.at[n // 2], 0)
        send(block, block, s_ds.at[n], s_ds.at[n], partner).wait_send()

    for j in range(8):
        send(peer.at[j], peer.at[j], s_p.at[j], s_p.at[j], partner).wait_send()
    for side in range(2):
        for i in range(2):
            hop_copy(12 + side, i).wait_send()
        for qi in range(4):
            tail_copy(side, qi).wait_send()


def solution(mesh):
    tp = mesh.shape["tp"]
    token_spec = P(("dp", "tp"), None)
    split_cols = P("dp", "tp")
    weight_cols = P(None, "tp")
    weight_rows = P("tp", None)

    def local_backward(x_norm, grad_y, u_gate, u_up, w_gate, w_up, w_down, x_in, gamma, grad_res, attn_out, w_out):
        rows, hid = x_norm.shape
        tokens, cols = u_gate.shape
        ocols = attn_out.shape[1]
        half = rows // 2
        quarter = half // 2
        any_spec = pl.BlockSpec(memory_space=pl.ANY)
        vmem_spec = pl.BlockSpec(memory_space=pltpu.VMEM)
        dma = pltpu.SemaphoreType.DMA
        results = pl.pallas_call(
            functools.partial(kernel, tp),
            out_shape=(
                pltpu.VMEM((rows, hid), BF16),
                pltpu.VMEM((32, ocols, quarter), BF16),
                pltpu.VMEM((2 * cols, hid), F32),
                pltpu.VMEM((cols, hid), F32),
                pltpu.VMEM((ocols, hid), F32),
            ),
            in_specs=[any_spec] * 8 + [vmem_spec] + [any_spec] * 3,
            out_specs=(vmem_spec,) * 5,
            scratch_shapes=[
                pltpu.VMEM((16, half, hid), BF16),
                pltpu.VMEM((16, half, hid), BF16),
                pltpu.VMEM((16, half, hid), BF16),
                pltpu.VMEM((8, half, hid), BF16),
                pltpu.VMEM((2, half, hid), BF16),
                pltpu.VMEM((4, quarter, hid), BF16),
                pltpu.VMEM((4, quarter, hid), BF16),
                pltpu.VMEM((16, 2 * cols, half), BF16),
                pltpu.VMEM((2 * cols, hid), BF16),
                pltpu.VMEM((cols, hid), BF16),
                pltpu.VMEM((ocols, hid), BF16),
                pltpu.VMEM((2, cols, half), BF16),
                pltpu.VMEM((2, cols, half), BF16),
                pltpu.VMEM((32, ocols, quarter), BF16),
                pltpu.VMEM((rows, hid), BF16),
                pltpu.VMEM((rows, hid), BF16),
                dma((16,)), dma((16,)),
                dma((16,)), dma((16,)),
                dma((8,)), dma((8,)),
                dma((4,)), dma((4,)),
                dma((8,)), dma((8,)),
                dma((32,)), dma((32,)),
                dma((4,)), dma((4,)), dma((4,)), dma((32,)), dma((2,)),
            ],
            compiler_params=pltpu.CompilerParams(
                collective_id=0, has_side_effects=True, vmem_limit_bytes=54_000_000),
            name="layer_backward",
        )(x_norm, grad_y, u_gate.T, u_up.T, w_gate.T, w_up.T, w_down, x_in, gamma, grad_res, attn_out.T,
          w_out)
        results = [pltpu.with_memory_space_constraint(r, pltpu.VMEM) for r in results]
        ds, do, dwg, dwu, dwd, dwo = pl.pallas_call(
            functools.partial(write_kernel, tp, half),
            out_shape=(
                jax.ShapeDtypeStruct((rows, hid), BF16),
                jax.ShapeDtypeStruct((ocols, tokens), BF16),
                jax.ShapeDtypeStruct((cols, hid), F32),
                jax.ShapeDtypeStruct((cols, hid), F32),
                jax.ShapeDtypeStruct((cols, hid), F32),
                jax.ShapeDtypeStruct((ocols, hid), F32),
            ),
            in_specs=[vmem_spec] * 5,
            out_specs=(any_spec,) * 6,
            scratch_shapes=[dma((5,)), dma((32,))],
            compiler_params=pltpu.CompilerParams(vmem_limit_bytes=1_000_000),
            name="write_results",
        )(*results)
        return ds, do.T, dwg.T, dwu.T, dwd, dwo

    return jax.shard_map(
        local_backward,
        mesh=mesh,
        in_specs=(token_spec, token_spec, split_cols, split_cols, weight_cols, weight_cols, weight_rows,
                  token_spec, P(None), token_spec, split_cols, weight_rows),
        out_specs=(token_spec, split_cols, split_cols, split_cols, token_spec, token_spec),
        check_vma=False,
    )
```

```python
import functools

import jax
import jax.numpy as jnp
from jax import lax
from jax.experimental import pallas as pl
from jax.experimental.pallas import tpu as pltpu
from jax.sharding import PartitionSpec as P

NORM_EPS = 1e-5
F32 = jnp.float32
BF16 = jnp.bfloat16
ROWS_ROWS = (((0,), (0,)), ((), ()))
COLS_COLS = (((1,), (1,)), ((), ()))
COLS_ROWS = (((1,), (0,)), ((), ()))
MESH = pl.DeviceIdType.MESH


def dot(a, b, dims):
    return lax.dot_general(a, b, dims, preferred_element_type=F32)


def slot_token(tp, half, k):
    me = lax.axis_index("tp")
    g, b, i = k // 4, lax.rem(k, 4) // 2, lax.rem(k, 2)
    dx = jnp.where(g == 0, 0, jnp.where(g == 3, 2, 2 * i - 1))
    h = jnp.where(g == 2, 1 - i, i)
    chip = lax.rem(me // 2 + dx + tp // 2, tp // 2)
    shard = 2 * chip + lax.rem(lax.rem(me, 2) + b, 2)
    return pl.multiple_of((2 * shard + h) * half, half)


def write_kernel(tp, half, dso, dob, dwgu, dwd, dwo, ds_out, do_out, dwg_out, dwu_out, dwd_out, dwo_out, sem, sem_do):
    cols, quarter = dwd.shape[0], half // 2
    copies = [pltpu.make_async_copy(src, dst, sem.at[i]) for i, (src, dst) in enumerate((
        (dwgu.at[pl.ds(0, cols)], dwg_out), (dwgu.at[pl.ds(cols, cols)], dwu_out), (dwd, dwd_out), (dso, ds_out),
        (dwo, dwo_out)))]

    def do_copy(n):
        tokens = pl.ds(pl.multiple_of(slot_token(tp, half, n // 2) + lax.rem(n, 2) * quarter, quarter), quarter)
        return pltpu.make_async_copy(dob.at[n], do_out.at[:, tokens], sem_do.at[n])

    for c in copies:
        c.start()

    @pl.loop(0, 2 * 2 * tp)
    def _(n):
        do_copy(n).start()

    @pl.loop(0, 2 * 2 * tp)
    def _(n):
        do_copy(n).wait()

    for c in copies:
        c.wait()


def kernel(tp, x_hbm, gy_hbm, ug_hbm, uu_hbm, wg_hbm, wu_hbm, wd_hbm, xin_hbm, gamma_ref, gr_hbm, o_hbm, wo_hbm,
           dso, dob, dwgu, dwd, dwo,
           gy, xb, part, peer, hop, froml, fromr, du, wgu, wd, wo, ugb, uub, ob, xin, gr,
           s_gy, r_gy, s_x, r_x, s_p, r_p, s_h, r_h, s_t, r_t, s_ds, r_ds,
           l_w, l_own, l_u, l_o, l_tok):
    half = gy.shape[1]
    cols = wd.shape[0]
    quarter = half // 2
    me = lax.axis_index("tp")
    right = lax.rem(me + 2, tp)
    left = lax.rem(me + tp - 2, tp)
    partner = me + 1 - 2 * lax.rem(me, 2)
    slot_row = functools.partial(slot_token, tp, half)

    def send(src, dst, ssem, rsem, dev):
        return pltpu.make_async_remote_copy(
            src_ref=src, dst_ref=dst, send_sem=ssem, recv_sem=rsem, device_id={"tp": dev}, device_id_type=MESH)

    def u_copies(k):
        tokens = pl.ds(slot_row(k), half)
        at = lax.rem(k, 2)
        return (pltpu.make_async_copy(ug_hbm.at[:, tokens], ugb.at[at], l_u.at[2 * at]),
                pltpu.make_async_copy(uu_hbm.at[:, tokens], uub.at[at], l_u.at[2 * at + 1]))

    def o_copy(n):
        tokens = pl.ds(pl.multiple_of(slot_row(n // 2) + lax.rem(n, 2) * quarter, quarter), quarter)
        return pltpu.make_async_copy(o_hbm.at[:, tokens], ob.at[n], l_o.at[n])

    def own(hbm, h):
        return hbm.at[pl.ds(h * half, half)]

    def send_own(buf, ssem, rsem):
        for src, dst, dev in ((0, 4, right), (1, 5, left), (1, 8, right), (0, 9, left), (0, 2, partner), (1, 3, partner)):
            send(buf.at[src], buf.at[dst], ssem.at[dst], rsem.at[dst], dev).start()

    def arrived(buf, ssem, rsem, k):
        send(buf.at[k], buf.at[k], ssem.at[k], rsem.at[k], partner).wait_recv()

    def drain(buf, ssem, k):
        send(buf.at[k], buf.at[k], ssem.at[k], ssem.at[k], partner).wait_send()

    def gather_step(buf, ssem, rsem, k, also):
        place = lax.rem(k, 4)

        @pl.when((place == 0) & (k > 0))
        def _():
            arrived(buf, ssem, rsem, k)
            arrived(buf, ssem, rsem, k + 1)

            @pl.when(k == 4)
            def _():
                send(buf.at[4], buf.at[12], ssem.at[12], rsem.at[12], right).start()
                send(buf.at[5], buf.at[13], ssem.at[13], rsem.at[13], left).start()

            send(buf.at[k], buf.at[k + 2], ssem.at[k + 2], rsem.at[k + 2], partner).start()
            send(buf.at[k + 1], buf.at[k + 3], ssem.at[k + 3], rsem.at[k + 3], partner).start()
            if also is not None:
                pl.when(k == 4)(also)

        @pl.when(place >= 2)
        def _():
            arrived(buf, ssem, rsem, k)

    barrier = pltpu.get_barrier_semaphore()
    for dev in (left, right, partner):
        pl.semaphore_signal(barrier, inc=1, device_id={"tp": dev}, device_id_type=MESH)
    for h in range(2):
        pltpu.make_async_copy(own(gy_hbm, h), gy.at[h], l_own.at[h]).start()
    weights = ((wd_hbm, wd), (wg_hbm, wgu.at[pl.ds(0, cols)]), (wu_hbm, wgu.at[pl.ds(cols, cols)]), (wo_hbm, wo))
    for i, (src, dst) in enumerate(weights):
        pltpu.make_async_copy(src, dst, l_w.at[i]).start()
    for c in u_copies(0):
        c.start()
    for h in range(2):
        pltpu.make_async_copy(own(x_hbm, h), xb.at[h], l_own.at[2 + h]).start()
    for h in range(2):
        pltpu.make_async_copy(own(gy_hbm, h), gy.at[h], l_own.at[h]).wait()
    pl.semaphore_wait(barrier, 3)
    send_own(gy, s_gy, r_gy)
    pltpu.make_async_copy(xin_hbm, xin, l_tok.at[0]).start()
    pltpu.make_async_copy(gr_hbm, gr, l_tok.at[1]).start()

    @pl.loop(0, 32)
    def _(n):
        o_copy(n).start()

    dwd[...] = jnp.zeros_like(dwd)
    dwgu[...] = jnp.zeros_like(dwgu)
    dwo[...] = jnp.zeros_like(dwo)
    for i, (src, dst) in enumerate(weights):
        pltpu.make_async_copy(src, dst, l_w.at[i]).wait()
    for h in range(2):
        pltpu.make_async_copy(own(x_hbm, h), xb.at[h], l_own.at[2 + h]).wait()

    def part_copy(k):
        j = (k // 4) * 2 + lax.rem(k, 2)
        return send(part.at[k], peer.at[j], s_p.at[j], r_p.at[j], partner)

    @pl.loop(0, 16)
    def _(k):
        @pl.when(k + 1 < 16)
        def _():
            for c in u_copies(k + 1):
                c.start()

        @pl.when((k > 0) & (lax.rem(k + 3, 4) >= 2))
        def _():
            part_copy(k - 1).start()

        gather_step(gy, s_gy, r_gy, k, lambda: send_own(xb, s_x, r_x))
        for c in u_copies(k):
            c.wait()
        at = lax.rem(k, 2)
        gyk = gy[k]
        gh = dot(wd[...], gyk, COLS_COLS)
        gate = ugb[at].astype(F32)
        up = uub[at].astype(F32)
        sig = jax.nn.sigmoid(gate)
        act = gate * sig
        silu = sig * (1.0 + gate * (1.0 - sig))
        z = (act * up).astype(BF16)
        du_up = (gh * act).astype(BF16)
        du_gate = (gh * up * silu).astype(BF16)
        du[k, pl.ds(0, cols)] = du_gate
        du[k, pl.ds(cols, cols)] = du_up
        dwd[...] += dot(z, gyk, COLS_ROWS)
        part[k] = dot(du[k], wgu[...], ROWS_ROWS).astype(BF16)

    part_copy(15).start()

    @pl.loop(2, 16)
    def _(k):
        drain(gy, s_gy, k)

    def add_peer(k, more=()):
        j = (k // 4) * 2 + k % 2
        t = part[k].astype(F32) + peer[j].astype(F32)
        for m in more:
            t = t + m[...].astype(F32)
        part[k] = t.astype(BF16)

    def q(ref, i):
        return ref.at[pl.ds(i * quarter, quarter)]

    def peer_arrived(j):
        send(peer.at[j], peer.at[j], s_p.at[j], r_p.at[j], partner).wait_recv()

    for j in range(8):
        peer_arrived(j)

    def hop_copy(k, i):
        side = k - 12
        return send(q(part.at[k], i), q(hop.at[side], i), s_h.at[2 * side + i], r_h.at[2 * side + i], (right, left)[side])

    for k in (12, 13):
        add_peer(k)
    for i in range(2):
        for k in (12, 13):
            hop_copy(k, i).start()

    def dw_step(j):
        xk = xb[pl.ds(2 * j, 2)].reshape(2 * half, xb.shape[2])
        duk = jnp.concatenate((du[2 * j], du[2 * j + 1]), axis=1)
        dwgu[...] += dot(duk, xk, COLS_ROWS)

    def tail_copy(side, qi):
        k = ((9, 5), (4, 8))[side][qi // 2]
        dst = (froml, fromr)[side].at[qi]
        return send(q(part.at[k], qi % 2), dst, s_t.at[4 * side + qi], r_t.at[4 * side + qi], (right, left)[side])

    tail_order = ((2, 0, 3, 1), (0, 2, 1, 3))

    def tails():
        add_peer(5)
        add_peer(4)
        for side in range(2):
            for i in range(2):
                hop_copy(12 + side, i).wait_recv()
        add_peer(9, (hop.at[0],))
        add_peer(8, (hop.at[1],))
        for n in range(4):
            for side in range(2):
                tail_copy(side, tail_order[side][n]).start()

    @pl.loop(0, 8)
    def _(j):
        pl.when(j == 6)(tails)
        gather_step(xb, s_x, r_x, 2 * j, None)

        @pl.when(lax.rem(j, 2) == 1)
        def _():
            arrived(xb, s_x, r_x, 2 * j + 1)

        dw_step(j)

    ds = gy
    pltpu.make_async_copy(xin_hbm, xin, l_tok.at[0]).wait()
    pltpu.make_async_copy(gr_hbm, gr, l_tok.at[1]).wait()
    gamma = gamma_ref[...].astype(F32).reshape(1, gamma_ref.shape[0])

    def norm_quarter(qi):
        h, i = qi // 2, qi % 2
        tail_copy(0, qi).wait_recv()
        tail_copy(1, qi).wait_recv()
        step = 32

        @pl.loop(0, quarter // step)
        def _(n):
            rows = pl.ds(pl.multiple_of(n * step, step), step)
            inner = pl.ds(pl.multiple_of(i * quarter + n * step, step), step)
            tokens = pl.ds(pl.multiple_of(qi * quarter + n * step, step), step)
            dx = (part[h, inner].astype(F32) + peer[h, inner].astype(F32)
                  + froml[qi, rows].astype(F32) + fromr[qi, rows].astype(F32)).astype(BF16)
            xf = xin[tokens].astype(F32)
            inv = lax.rsqrt(jnp.mean(xf * xf, axis=-1, keepdims=True) + NORM_EPS)
            scaled = dx.astype(F32) * gamma
            proj = jnp.mean(scaled * xf, axis=-1, keepdims=True)
            out = (gr[tokens].astype(F32) + inv * (scaled - xf * (inv * inv) * proj)).astype(BF16)
            ds[h, inner] = out
            dso[tokens] = out

    def ds_copy(src, dst, i, dev):
        n = 2 * dst + i
        return send(q(ds.at[src], i), q(ds.at[dst], i), s_ds.at[n], r_ds.at[n], dev)

    for i in range(2):
        for h in (0, 1):
            norm_quarter(2 * h + i)
        for src, dst, dev in ((0, 4, right), (1, 5, left), (1, 8, right), (0, 9, left), (0, 2, partner), (1, 3, partner)):
            ds_copy(src, dst, i, dev).start()

    @pl.loop(0, 32)
    def _(n):
        o_copy(n).wait()

    @pl.loop(0, 16)
    def _(u):
        v, w = u - 4, u - 12
        i = jnp.where(u < 4, lax.rem(u, 2), jnp.where(u < 12, v // 4, w // 2))
        k = jnp.where(u < 4, 2 * (u // 2), jnp.where(u < 12, 4 + 2 * lax.rem(v, 4), 12 + 2 * lax.rem(w, 2)))

        @pl.when(k > 0)
        def _():
            for d in range(2):
                n = 2 * (k + d) + i
                block = q(ds.at[k + d], i)
                send(block, block, s_ds.at[n], r_ds.at[n], partner).wait_recv()

        @pl.when(k == 4)
        def _():
            for src, dst, dev in ((4, 12, right), (5, 13, left)):
                n = 2 * dst + i
                send(q(ds.at[src], i), q(ds.at[dst], i), s_ds.at[n], r_ds.at[n], dev).start()

        @pl.when((k > 0) & (lax.rem(k, 4) == 0))
        def _():
            for d in range(2):
                n = 2 * (k + 2 + d) + i
                send(q(ds.at[k + d], i), q(ds.at[k + 2 + d], i), s_ds.at[n], r_ds.at[n], partner).start()

        rows = pl.ds(pl.multiple_of(i * quarter, quarter), quarter)
        for d in range(2):
            block = ds[k + d, rows]
            n = 2 * (k + d) + i
            dob[n] = dot(wo[...], block, COLS_COLS).astype(BF16)
            dwo[...] += dot(ob[n], block, COLS_ROWS)

    @pl.loop(2, 16)
    def _(k):
        drain(xb, s_x, k)

    @pl.loop(4, 32)
    def _(n):
        block = q(ds.at[n // 2], 0)
        send(block, block, s_ds.at[n], s_ds.at[n], partner).wait_send()

    for j in range(8):
        send(peer.at[j], peer.at[j], s_p.at[j], s_p.at[j], partner).wait_send()
    for side in range(2):
        for i in range(2):
            hop_copy(12 + side, i).wait_send()
        for qi in range(4):
            tail_copy(side, qi).wait_send()


def solution(mesh):
    tp = mesh.shape["tp"]
    token_spec = P(("dp", "tp"), None)
    split_cols = P("dp", "tp")
    weight_cols = P(None, "tp")
    weight_rows = P("tp", None)

    def local_backward(x_norm, grad_y, u_gate, u_up, w_gate, w_up, w_down, x_in, gamma, grad_res, attn_out, w_out):
        rows, hid = x_norm.shape
        tokens, cols = u_gate.shape
        ocols = attn_out.shape[1]
        half = rows // 2
        quarter = half // 2
        any_spec = pl.BlockSpec(memory_space=pl.ANY)
        vmem_spec = pl.BlockSpec(memory_space=pltpu.VMEM)
        dma = pltpu.SemaphoreType.DMA
        results = pl.pallas_call(
            functools.partial(kernel, tp),
            out_shape=(
                pltpu.VMEM((rows, hid), BF16),
                pltpu.VMEM((32, ocols, quarter), BF16),
                pltpu.VMEM((2 * cols, hid), F32),
                pltpu.VMEM((cols, hid), F32),
                pltpu.VMEM((ocols, hid), F32),
            ),
            in_specs=[any_spec] * 8 + [vmem_spec] + [any_spec] * 3,
            out_specs=(vmem_spec,) * 5,
            scratch_shapes=[
                pltpu.VMEM((16, half, hid), BF16),
                pltpu.VMEM((16, half, hid), BF16),
                pltpu.VMEM((16, half, hid), BF16),
                pltpu.VMEM((8, half, hid), BF16),
                pltpu.VMEM((2, half, hid), BF16),
                pltpu.VMEM((4, quarter, hid), BF16),
                pltpu.VMEM((4, quarter, hid), BF16),
                pltpu.VMEM((16, 2 * cols, half), BF16),
                pltpu.VMEM((2 * cols, hid), BF16),
                pltpu.VMEM((cols, hid), BF16),
                pltpu.VMEM((ocols, hid), BF16),
                pltpu.VMEM((2, cols, half), BF16),
                pltpu.VMEM((2, cols, half), BF16),
                pltpu.VMEM((32, ocols, quarter), BF16),
                pltpu.VMEM((rows, hid), BF16),
                pltpu.VMEM((rows, hid), BF16),
                dma((16,)), dma((16,)),
                dma((16,)), dma((16,)),
                dma((8,)), dma((8,)),
                dma((4,)), dma((4,)),
                dma((8,)), dma((8,)),
                dma((32,)), dma((32,)),
                dma((4,)), dma((4,)), dma((4,)), dma((32,)), dma((2,)),
            ],
            compiler_params=pltpu.CompilerParams(
                collective_id=0, has_side_effects=True, vmem_limit_bytes=54_000_000),
            name="layer_backward",
        )(x_norm, grad_y, u_gate.T, u_up.T, w_gate.T, w_up.T, w_down, x_in, gamma, grad_res, attn_out.T,
          w_out)
        results = [pltpu.with_memory_space_constraint(r, pltpu.VMEM) for r in results]
        ds, do, dwg, dwu, dwd, dwo = pl.pallas_call(
            functools.partial(write_kernel, tp, half),
            out_shape=(
                jax.ShapeDtypeStruct((rows, hid), BF16),
                jax.ShapeDtypeStruct((ocols, tokens), BF16),
                jax.ShapeDtypeStruct((cols, hid), F32),
                jax.ShapeDtypeStruct((cols, hid), F32),
                jax.ShapeDtypeStruct((cols, hid), F32),
                jax.ShapeDtypeStruct((ocols, hid), F32),
            ),
            in_specs=[vmem_spec] * 5,
            out_specs=(any_spec,) * 6,
            scratch_shapes=[dma((5,)), dma((32,))],
            compiler_params=pltpu.CompilerParams(vmem_limit_bytes=1_000_000),
            name="write_results",
        )(*results)
        return ds, do.T, dwg.T, dwu.T, dwd, dwo

    return jax.shard_map(
        local_backward,
        mesh=mesh,
        in_specs=(token_spec, token_spec, split_cols, split_cols, weight_cols, weight_cols, weight_rows,
                  token_spec, P(None), token_spec, split_cols, weight_rows),
        out_specs=(token_spec, split_cols, split_cols, split_cols, token_spec, token_spec),
        check_vma=False,
    )
```

```python
import functools

import jax
import jax.numpy as jnp
from jax import lax
from jax.experimental import pallas as pl
from jax.experimental.pallas import tpu as pltpu
from jax.sharding import PartitionSpec as P

NORM_EPS = 1e-5
F32 = jnp.float32
BF16 = jnp.bfloat16
ROWS_ROWS = (((0,), (0,)), ((), ()))
COLS_COLS = (((1,), (1,)), ((), ()))
COLS_ROWS = (((1,), (0,)), ((), ()))
MESH = pl.DeviceIdType.MESH


def dot(a, b, dims):
    return lax.dot_general(a, b, dims, preferred_element_type=F32)


def slot_token(tp, half, k):
    me = lax.axis_index("tp")
    g, b, i = k // 4, lax.rem(k, 4) // 2, lax.rem(k, 2)
    dx = jnp.where(g == 0, 0, jnp.where(g == 3, 2, 2 * i - 1))
    h = jnp.where(g == 2, 1 - i, i)
    chip = lax.rem(me // 2 + dx + tp // 2, tp // 2)
    shard = 2 * chip + lax.rem(lax.rem(me, 2) + b, 2)
    return pl.multiple_of((2 * shard + h) * half, half)


def write_kernel(tp, half, dso, dob, dwgu, dwd, dwo, ds_out, do_out, dwg_out, dwu_out, dwd_out, dwo_out, sem, sem_do):
    cols, quarter = dwd.shape[0], half // 2
    copies = [pltpu.make_async_copy(src, dst, sem.at[i]) for i, (src, dst) in enumerate((
        (dwgu.at[pl.ds(0, cols)], dwg_out), (dwgu.at[pl.ds(cols, cols)], dwu_out), (dwd, dwd_out), (dso, ds_out),
        (dwo, dwo_out)))]

    def do_copy(n):
        tokens = pl.ds(pl.multiple_of(slot_token(tp, half, n // 2) + lax.rem(n, 2) * quarter, quarter), quarter)
        return pltpu.make_async_copy(dob.at[n], do_out.at[:, tokens], sem_do.at[n])

    for c in copies:
        c.start()

    @pl.loop(0, 2 * 2 * tp)
    def _(n):
        do_copy(n).start()

    @pl.loop(0, 2 * 2 * tp)
    def _(n):
        do_copy(n).wait()

    for c in copies:
        c.wait()


def kernel(tp, x_hbm, gy_hbm, ug_hbm, uu_hbm, wg_hbm, wu_hbm, wd_hbm, xin_hbm, gamma_ref, gr_hbm, o_hbm, wo_hbm,
           dso, dob, dwgu, dwd, dwo,
           gy, xb, part, peer, hop, froml, fromr, du, wgu, wd, wo, ugb, uub, ob, xin, gr,
           s_gy, r_gy, s_x, r_x, s_p, r_p, s_h, r_h, s_t, r_t, s_ds, r_ds,
           l_w, l_own, l_u, l_o, l_tok):
    half = gy.shape[1]
    cols = wd.shape[0]
    quarter = half // 2
    me = lax.axis_index("tp")
    right = lax.rem(me + 2, tp)
    left = lax.rem(me + tp - 2, tp)
    partner = me + 1 - 2 * lax.rem(me, 2)
    slot_row = functools.partial(slot_token, tp, half)

    def send(src, dst, ssem, rsem, dev):
        return pltpu.make_async_remote_copy(
            src_ref=src, dst_ref=dst, send_sem=ssem, recv_sem=rsem, device_id={"tp": dev}, device_id_type=MESH)

    def u_copies(k):
        tokens = pl.ds(slot_row(k), half)
        at = lax.rem(k, 2)
        return (pltpu.make_async_copy(ug_hbm.at[:, tokens], ugb.at[at], l_u.at[2 * at]),
                pltpu.make_async_copy(uu_hbm.at[:, tokens], uub.at[at], l_u.at[2 * at + 1]))

    def o_copy(n):
        tokens = pl.ds(pl.multiple_of(slot_row(n // 2) + lax.rem(n, 2) * quarter, quarter), quarter)
        return pltpu.make_async_copy(o_hbm.at[:, tokens], ob.at[n], l_o.at[n])

    def own(hbm, h):
        return hbm.at[pl.ds(h * half, half)]

    def send_own(buf, ssem, rsem):
        for src, dst, dev in ((0, 4, right), (1, 5, left), (1, 8, right), (0, 9, left), (0, 2, partner), (1, 3, partner)):
            send(buf.at[src], buf.at[dst], ssem.at[dst], rsem.at[dst], dev).start()

    def arrived(buf, ssem, rsem, k):
        send(buf.at[k], buf.at[k], ssem.at[k], rsem.at[k], partner).wait_recv()

    def drain(buf, ssem, k):
        send(buf.at[k], buf.at[k], ssem.at[k], ssem.at[k], partner).wait_send()

    def gather_step(buf, ssem, rsem, k, also):
        place = lax.rem(k, 4)

        @pl.when((place == 0) & (k > 0))
        def _():
            arrived(buf, ssem, rsem, k)
            arrived(buf, ssem, rsem, k + 1)

            @pl.when(k == 4)
            def _():
                send(buf.at[4], buf.at[12], ssem.at[12], rsem.at[12], right).start()
                send(buf.at[5], buf.at[13], ssem.at[13], rsem.at[13], left).start()

            send(buf.at[k], buf.at[k + 2], ssem.at[k + 2], rsem.at[k + 2], partner).start()
            send(buf.at[k + 1], buf.at[k + 3], ssem.at[k + 3], rsem.at[k + 3], partner).start()
            if also is not None:
                pl.when(k == 4)(also)

        @pl.when(place >= 2)
        def _():
            arrived(buf, ssem, rsem, k)

    barrier = pltpu.get_barrier_semaphore()
    for dev in (left, right, partner):
        pl.semaphore_signal(barrier, inc=1, device_id={"tp": dev}, device_id_type=MESH)
    for h in range(2):
        pltpu.make_async_copy(own(gy_hbm, h), gy.at[h], l_own.at[h]).start()
    pl.semaphore_wait(barrier, 3)
    for h in range(2):
        pltpu.make_async_copy(own(gy_hbm, h), gy.at[h], l_own.at[h]).wait()
    send_own(gy, s_gy, r_gy)
    weights = ((wd_hbm, wd), (wg_hbm, wgu.at[pl.ds(0, cols)]), (wu_hbm, wgu.at[pl.ds(cols, cols)]), (wo_hbm, wo))
    for i, (src, dst) in enumerate(weights):
        pltpu.make_async_copy(src, dst, l_w.at[i]).start()
    for c in u_copies(0):
        c.start()
    for h in range(2):
        pltpu.make_async_copy(own(x_hbm, h), xb.at[h], l_own.at[2 + h]).start()
    pltpu.make_async_copy(xin_hbm, xin, l_tok.at[0]).start()
    pltpu.make_async_copy(gr_hbm, gr, l_tok.at[1]).start()

    @pl.loop(0, 32)
    def _(n):
        o_copy(n).start()

    dwd[...] = jnp.zeros_like(dwd)
    dwgu[...] = jnp.zeros_like(dwgu)
    dwo[...] = jnp.zeros_like(dwo)
    for i, (src, dst) in enumerate(weights):
        pltpu.make_async_copy(src, dst, l_w.at[i]).wait()
    for h in range(2):
        pltpu.make_async_copy(own(x_hbm, h), xb.at[h], l_own.at[2 + h]).wait()

    def part_copy(k):
        j = (k // 4) * 2 + lax.rem(k, 2)
        return send(part.at[k], peer.at[j], s_p.at[j], r_p.at[j], partner)

    @pl.loop(0, 16)
    def _(k):
        @pl.when(k + 1 < 16)
        def _():
            for c in u_copies(k + 1):
                c.start()

        @pl.when((k > 0) & (lax.rem(k + 3, 4) >= 2))
        def _():
            part_copy(k - 1).start()

        gather_step(gy, s_gy, r_gy, k, lambda: send_own(xb, s_x, r_x))
        for c in u_copies(k):
            c.wait()
        at = lax.rem(k, 2)
        gyk = gy[k]
        gh = dot(wd[...], gyk, COLS_COLS)
        gate = ugb[at].astype(F32)
        up = uub[at].astype(F32)
        sig = jax.nn.sigmoid(gate)
        act = gate * sig
        silu = sig * (1.0 + gate * (1.0 - sig))
        z = (act * up).astype(BF16)
        du_up = (gh * act).astype(BF16)
        du_gate = (gh * up * silu).astype(BF16)
        du[k, pl.ds(0, cols)] = du_gate
        du[k, pl.ds(cols, cols)] = du_up
        dwd[...] += dot(z, gyk, COLS_ROWS)
        part[k] = dot(du[k], wgu[...], ROWS_ROWS).astype(BF16)

    part_copy(15).start()

    @pl.loop(2, 16)
    def _(k):
        drain(gy, s_gy, k)

    def add_peer(k, more=()):
        j = (k // 4) * 2 + k % 2
        t = part[k].astype(F32) + peer[j].astype(F32)
        for m in more:
            t = t + m[...].astype(F32)
        part[k] = t.astype(BF16)

    def q(ref, i):
        return ref.at[pl.ds(i * quarter, quarter)]

    def peer_arrived(j):
        send(peer.at[j], peer.at[j], s_p.at[j], r_p.at[j], partner).wait_recv()

    for j in range(8):
        peer_arrived(j)

    def hop_copy(k, i):
        side = k - 12
        return send(q(part.at[k], i), q(hop.at[side], i), s_h.at[2 * side + i], r_h.at[2 * side + i], (right, left)[side])

    for k in (12, 13):
        add_peer(k)
    for i in range(2):
        for k in (12, 13):
            hop_copy(k, i).start()

    def dw_step(j):
        xk = xb[pl.ds(2 * j, 2)].reshape(2 * half, xb.shape[2])
        duk = jnp.concatenate((du[2 * j], du[2 * j + 1]), axis=1)
        dwgu[...] += dot(duk, xk, COLS_ROWS)

    def tail_copy(side, qi):
        k = ((9, 5), (4, 8))[side][qi // 2]
        dst = (froml, fromr)[side].at[qi]
        return send(q(part.at[k], qi % 2), dst, s_t.at[4 * side + qi], r_t.at[4 * side + qi], (right, left)[side])

    tail_order = ((2, 0, 3, 1), (0, 2, 1, 3))

    def tails():
        add_peer(5)
        add_peer(4)
        for side in range(2):
            for i in range(2):
                hop_copy(12 + side, i).wait_recv()
        add_peer(9, (hop.at[0],))
        add_peer(8, (hop.at[1],))
        for n in range(4):
            for side in range(2):
                tail_copy(side, tail_order[side][n]).start()

    @pl.loop(0, 8)
    def _(j):
        pl.when(j == 6)(tails)
        gather_step(xb, s_x, r_x, 2 * j, None)

        @pl.when(lax.rem(j, 2) == 1)
        def _():
            arrived(xb, s_x, r_x, 2 * j + 1)

        dw_step(j)

    ds = gy
    pltpu.make_async_copy(xin_hbm, xin, l_tok.at[0]).wait()
    pltpu.make_async_copy(gr_hbm, gr, l_tok.at[1]).wait()
    gamma = gamma_ref[...].astype(F32).reshape(1, gamma_ref.shape[0])

    def norm_quarter(qi):
        h, i = qi // 2, qi % 2
        tail_copy(0, qi).wait_recv()
        tail_copy(1, qi).wait_recv()
        step = 32

        @pl.loop(0, quarter // step)
        def _(n):
            rows = pl.ds(pl.multiple_of(n * step, step), step)
            inner = pl.ds(pl.multiple_of(i * quarter + n * step, step), step)
            tokens = pl.ds(pl.multiple_of(qi * quarter + n * step, step), step)
            dx = (part[h, inner].astype(F32) + peer[h, inner].astype(F32)
                  + froml[qi, rows].astype(F32) + fromr[qi, rows].astype(F32)).astype(BF16)
            xf = xin[tokens].astype(F32)
            inv = lax.rsqrt(jnp.mean(xf * xf, axis=-1, keepdims=True) + NORM_EPS)
            scaled = dx.astype(F32) * gamma
            proj = jnp.mean(scaled * xf, axis=-1, keepdims=True)
            out = (gr[tokens].astype(F32) + inv * (scaled - xf * (inv * inv) * proj)).astype(BF16)
            ds[h, inner] = out
            dso[tokens] = out

    def ds_copy(src, dst, i, dev):
        n = 2 * dst + i
        return send(q(ds.at[src], i), q(ds.at[dst], i), s_ds.at[n], r_ds.at[n], dev)

    for i in range(2):
        for h in (0, 1):
            norm_quarter(2 * h + i)
        for src, dst, dev in ((0, 4, right), (1, 5, left), (1, 8, right), (0, 9, left), (0, 2, partner), (1, 3, partner)):
            ds_copy(src, dst, i, dev).start()

    @pl.loop(0, 32)
    def _(n):
        o_copy(n).wait()

    @pl.loop(0, 16)
    def _(u):
        v, w = u - 4, u - 12
        i = jnp.where(u < 4, lax.rem(u, 2), jnp.where(u < 12, v // 4, w // 2))
        k = jnp.where(u < 4, 2 * (u // 2), jnp.where(u < 12, 4 + 2 * lax.rem(v, 4), 12 + 2 * lax.rem(w, 2)))

        @pl.when(k > 0)
        def _():
            for d in range(2):
                n = 2 * (k + d) + i
                block = q(ds.at[k + d], i)
                send(block, block, s_ds.at[n], r_ds.at[n], partner).wait_recv()

        @pl.when(k == 4)
        def _():
            for src, dst, dev in ((4, 12, right), (5, 13, left)):
                n = 2 * dst + i
                send(q(ds.at[src], i), q(ds.at[dst], i), s_ds.at[n], r_ds.at[n], dev).start()

        @pl.when((k > 0) & (lax.rem(k, 4) == 0))
        def _():
            for d in range(2):
                n = 2 * (k + 2 + d) + i
                send(q(ds.at[k + d], i), q(ds.at[k + 2 + d], i), s_ds.at[n], r_ds.at[n], partner).start()

        rows = pl.ds(pl.multiple_of(i * quarter, quarter), quarter)
        for d in range(2):
            block = ds[k + d, rows]
            n = 2 * (k + d) + i
            dob[n] = dot(wo[...], block, COLS_COLS).astype(BF16)
            dwo[...] += dot(ob[n], block, COLS_ROWS)

    @pl.loop(2, 16)
    def _(k):
        drain(xb, s_x, k)

    @pl.loop(4, 32)
    def _(n):
        block = q(ds.at[n // 2], 0)
        send(block, block, s_ds.at[n], s_ds.at[n], partner).wait_send()

    for j in range(8):
        send(peer.at[j], peer.at[j], s_p.at[j], s_p.at[j], partner).wait_send()
    for side in range(2):
        for i in range(2):
            hop_copy(12 + side, i).wait_send()
        for qi in range(4):
            tail_copy(side, qi).wait_send()


def solution(mesh):
    tp = mesh.shape["tp"]
    token_spec = P(("dp", "tp"), None)
    split_cols = P("dp", "tp")
    weight_cols = P(None, "tp")
    weight_rows = P("tp", None)

    def local_backward(x_norm, grad_y, u_gate, u_up, w_gate, w_up, w_down, x_in, gamma, grad_res, attn_out, w_out):
        rows, hid = x_norm.shape
        tokens, cols = u_gate.shape
        ocols = attn_out.shape[1]
        half = rows // 2
        quarter = half // 2
        any_spec = pl.BlockSpec(memory_space=pl.ANY)
        vmem_spec = pl.BlockSpec(memory_space=pltpu.VMEM)
        dma = pltpu.SemaphoreType.DMA
        results = pl.pallas_call(
            functools.partial(kernel, tp),
            out_shape=(
                pltpu.VMEM((rows, hid), BF16),
                pltpu.VMEM((32, ocols, quarter), BF16),
                pltpu.VMEM((2 * cols, hid), F32),
                pltpu.VMEM((cols, hid), F32),
                pltpu.VMEM((ocols, hid), F32),
            ),
            in_specs=[any_spec] * 8 + [vmem_spec] + [any_spec] * 3,
            out_specs=(vmem_spec,) * 5,
            scratch_shapes=[
                pltpu.VMEM((16, half, hid), BF16),
                pltpu.VMEM((16, half, hid), BF16),
                pltpu.VMEM((16, half, hid), BF16),
                pltpu.VMEM((8, half, hid), BF16),
                pltpu.VMEM((2, half, hid), BF16),
                pltpu.VMEM((4, quarter, hid), BF16),
                pltpu.VMEM((4, quarter, hid), BF16),
                pltpu.VMEM((16, 2 * cols, half), BF16),
                pltpu.VMEM((2 * cols, hid), BF16),
                pltpu.VMEM((cols, hid), BF16),
                pltpu.VMEM((ocols, hid), BF16),
                pltpu.VMEM((2, cols, half), BF16),
                pltpu.VMEM((2, cols, half), BF16),
                pltpu.VMEM((32, ocols, quarter), BF16),
                pltpu.VMEM((rows, hid), BF16),
                pltpu.VMEM((rows, hid), BF16),
                dma((16,)), dma((16,)),
                dma((16,)), dma((16,)),
                dma((8,)), dma((8,)),
                dma((4,)), dma((4,)),
                dma((8,)), dma((8,)),
                dma((32,)), dma((32,)),
                dma((4,)), dma((4,)), dma((4,)), dma((32,)), dma((2,)),
            ],
            compiler_params=pltpu.CompilerParams(
                collective_id=0, has_side_effects=True, vmem_limit_bytes=54_000_000),
            name="layer_backward",
        )(x_norm, grad_y, u_gate.T, u_up.T, w_gate.T, w_up.T, w_down, x_in, gamma, grad_res, attn_out.T,
          w_out)
        results = [pltpu.with_memory_space_constraint(r, pltpu.VMEM) for r in results]
        ds, do, dwg, dwu, dwd, dwo = pl.pallas_call(
            functools.partial(write_kernel, tp, half),
            out_shape=(
                jax.ShapeDtypeStruct((rows, hid), BF16),
                jax.ShapeDtypeStruct((ocols, tokens), BF16),
                jax.ShapeDtypeStruct((cols, hid), F32),
                jax.ShapeDtypeStruct((cols, hid), F32),
                jax.ShapeDtypeStruct((cols, hid), F32),
                jax.ShapeDtypeStruct((ocols, hid), F32),
            ),
            in_specs=[vmem_spec] * 5,
            out_specs=(any_spec,) * 6,
            scratch_shapes=[dma((5,)), dma((32,))],
            compiler_params=pltpu.CompilerParams(vmem_limit_bytes=1_000_000),
            name="write_results",
        )(*results)
        return ds, do.T, dwg.T, dwu.T, dwd, dwo

    return jax.shard_map(
        local_backward,
        mesh=mesh,
        in_specs=(token_spec, token_spec, split_cols, split_cols, weight_cols, weight_cols, weight_rows,
                  token_spec, P(None), token_spec, split_cols, weight_rows),
        out_specs=(token_spec, split_cols, split_cols, split_cols, token_spec, token_spec),
        check_vma=False,
    )
```

```python
import functools

import jax
import jax.numpy as jnp
from jax import lax
from jax.experimental import pallas as pl
from jax.experimental.pallas import tpu as pltpu
from jax.sharding import PartitionSpec as P

NORM_EPS = 1e-5
F32 = jnp.float32
BF16 = jnp.bfloat16
ROWS_ROWS = (((0,), (0,)), ((), ()))
COLS_COLS = (((1,), (1,)), ((), ()))
COLS_ROWS = (((1,), (0,)), ((), ()))
MESH = pl.DeviceIdType.MESH


def dot(a, b, dims):
    return lax.dot_general(a, b, dims, preferred_element_type=F32)


def slot_token(tp, half, k):
    me = lax.axis_index("tp")
    g, b, i = k // 4, lax.rem(k, 4) // 2, lax.rem(k, 2)
    dx = jnp.where(g == 0, 0, jnp.where(g == 3, 2, 2 * i - 1))
    h = jnp.where(g == 2, 1 - i, i)
    chip = lax.rem(me // 2 + dx + tp // 2, tp // 2)
    shard = 2 * chip + lax.rem(lax.rem(me, 2) + b, 2)
    return pl.multiple_of((2 * shard + h) * half, half)


def write_kernel(tp, half, dso, dob, dwgu, dwd, dwo, ds_out, do_out, dwg_out, dwu_out, dwd_out, dwo_out, sem, sem_do):
    cols, quarter = dwd.shape[0], half // 2
    copies = [pltpu.make_async_copy(src, dst, sem.at[i]) for i, (src, dst) in enumerate((
        (dwgu.at[pl.ds(0, cols)], dwg_out), (dwgu.at[pl.ds(cols, cols)], dwu_out), (dwd, dwd_out), (dso, ds_out),
        (dwo, dwo_out)))]

    def do_copy(n):
        tokens = pl.ds(pl.multiple_of(slot_token(tp, half, n // 2) + lax.rem(n, 2) * quarter, quarter), quarter)
        return pltpu.make_async_copy(dob.at[n], do_out.at[:, tokens], sem_do.at[n])

    for c in copies:
        c.start()

    @pl.loop(0, 2 * 2 * tp)
    def _(n):
        do_copy(n).start()

    @pl.loop(0, 2 * 2 * tp)
    def _(n):
        do_copy(n).wait()

    for c in copies:
        c.wait()


def kernel(tp, x_hbm, gy_hbm, ug_hbm, uu_hbm, wg_hbm, wu_hbm, wd_hbm, xin_hbm, gamma_ref, gr_hbm, o_hbm, wo_hbm,
           dso, dob, dwgu, dwd, dwo,
           gy, xb, part, peer, hop, froml, fromr, du, wgu, wd, wo, ugb, uub, ob, xin, gr,
           s_gy, r_gy, s_x, r_x, s_p, r_p, s_h, r_h, s_t, r_t, s_ds, r_ds,
           l_w, l_own, l_u, l_o, l_tok):
    half = gy.shape[1]
    cols = wd.shape[0]
    quarter = half // 2
    me = lax.axis_index("tp")
    right = lax.rem(me + 2, tp)
    left = lax.rem(me + tp - 2, tp)
    core = lax.rem(me, 2)
    partner = me + 1 - 2 * core
    slot_row = functools.partial(slot_token, tp, half)

    def send(src, dst, ssem, rsem, dev):
        return pltpu.make_async_remote_copy(
            src_ref=src, dst_ref=dst, send_sem=ssem, recv_sem=rsem, device_id={"tp": dev}, device_id_type=MESH)

    def u_copies(k):
        tokens = pl.ds(slot_row(k), half)
        at = lax.rem(k, 2)
        return (pltpu.make_async_copy(ug_hbm.at[:, tokens], ugb.at[at], l_u.at[2 * at]),
                pltpu.make_async_copy(uu_hbm.at[:, tokens], uub.at[at], l_u.at[2 * at + 1]))

    def o_copy(n):
        tokens = pl.ds(pl.multiple_of(slot_row(n // 2) + lax.rem(n, 2) * quarter, quarter), quarter)
        return pltpu.make_async_copy(o_hbm.at[:, tokens], ob.at[n], l_o.at[n])

    def own(hbm, h):
        return hbm.at[pl.ds(h * half, half)]

    barrier = pltpu.get_barrier_semaphore()
    for dev in (left, right, partner):
        pl.semaphore_signal(barrier, inc=1, device_id={"tp": dev}, device_id_type=MESH)
    pl.semaphore_wait(barrier, 3)

    def send_own(hbm, buf, ssem, rsem, first=0):
        plan = ((0, 4, right), (1, 5, left), (1, 8, right), (0, 9, left), (0, 2, partner), (1, 3, partner))
        for src, dst, dev in plan[first:]:
            send(own(hbm, src), buf.at[dst], ssem.at[dst], rsem.at[dst], dev).start()

    def arrived(buf, ssem, rsem, k):
        send(buf.at[k], buf.at[k], ssem.at[k], rsem.at[k], partner).wait_recv()

    def drain(buf, ssem, k):
        send(buf.at[k], buf.at[k], ssem.at[k], ssem.at[k], partner).wait_send()

    def gather_step(buf, ssem, rsem, k, also):
        place = lax.rem(k, 4)

        @pl.when((place == 0) & (k > 0))
        def _():
            arrived(buf, ssem, rsem, k)
            arrived(buf, ssem, rsem, k + 1)

            @pl.when(k == 4)
            def _():
                send(buf.at[4], buf.at[12], ssem.at[12], rsem.at[12], right).start()
                send(buf.at[5], buf.at[13], ssem.at[13], rsem.at[13], left).start()

            send(buf.at[k], buf.at[k + 2], ssem.at[k + 2], rsem.at[k + 2], partner).start()
            send(buf.at[k + 1], buf.at[k + 3], ssem.at[k + 3], rsem.at[k + 3], partner).start()
            if also is not None:
                pl.when(k == 4)(also)

        @pl.when(place >= 2)
        def _():
            arrived(buf, ssem, rsem, k)

    cut = quarter // 2

    @pl.when(core == 0)
    def _():
        send_own(gy_hbm, gy, s_gy, r_gy)

    @pl.when(core == 1)
    def _():
        for src, dst, dev in ((0, 4, right), (1, 5, left)):
            for lo, n in ((0, cut), (cut, half - cut)):
                send(gy_hbm.at[pl.ds(src * half + lo, n)], gy.at[dst, pl.ds(lo, n)], s_gy.at[dst], r_gy.at[dst], dev).start()
        send_own(gy_hbm, gy, s_gy, r_gy, 2)

    for h in range(2):
        pltpu.make_async_copy(own(gy_hbm, h), gy.at[h], l_own.at[h]).start()
        pltpu.make_async_copy(own(x_hbm, h), xb.at[h], l_own.at[2 + h]).start()
    weights = ((wd_hbm, wd), (wg_hbm, wgu.at[pl.ds(0, cols)]), (wu_hbm, wgu.at[pl.ds(cols, cols)]), (wo_hbm, wo))
    for i, (src, dst) in enumerate(weights):
        pltpu.make_async_copy(src, dst, l_w.at[i]).start()
    for c in u_copies(0):
        c.start()
    pltpu.make_async_copy(xin_hbm, xin, l_tok.at[0]).start()
    pltpu.make_async_copy(gr_hbm, gr, l_tok.at[1]).start()

    @pl.loop(0, 32)
    def _(n):
        o_copy(n).start()

    dwd[...] = jnp.zeros_like(dwd)
    dwgu[...] = jnp.zeros_like(dwgu)
    dwo[...] = jnp.zeros_like(dwo)
    for i, (src, dst) in enumerate(weights):
        pltpu.make_async_copy(src, dst, l_w.at[i]).wait()
    for h in range(2):
        pltpu.make_async_copy(own(gy_hbm, h), gy.at[h], l_own.at[h]).wait()
        pltpu.make_async_copy(own(x_hbm, h), xb.at[h], l_own.at[2 + h]).wait()

    def part_copy(k):
        j = (k // 4) * 2 + lax.rem(k, 2)
        return send(part.at[k], peer.at[j], s_p.at[j], r_p.at[j], partner)

    @pl.loop(0, 16)
    def _(k):
        @pl.when(k + 1 < 16)
        def _():
            for c in u_copies(k + 1):
                c.start()

        @pl.when((k > 0) & (lax.rem(k + 3, 4) >= 2))
        def _():
            part_copy(k - 1).start()

        gather_step(gy, s_gy, r_gy, k, lambda: send_own(x_hbm, xb, s_x, r_x))
        for c in u_copies(k):
            c.wait()
        at = lax.rem(k, 2)
        gyk = gy[k]
        gh = dot(wd[...], gyk, COLS_COLS)
        gate = ugb[at].astype(F32)
        up = uub[at].astype(F32)
        sig = jax.nn.sigmoid(gate)
        act = gate * sig
        silu = sig * (1.0 + gate * (1.0 - sig))
        z = (act * up).astype(BF16)
        du_up = (gh * act).astype(BF16)
        du_gate = (gh * up * silu).astype(BF16)
        du[k, pl.ds(0, cols)] = du_gate
        du[k, pl.ds(cols, cols)] = du_up
        dwd[...] += dot(z, gyk, COLS_ROWS)
        part[k] = dot(du[k], wgu[...], ROWS_ROWS).astype(BF16)

    part_copy(15).start()

    @pl.loop(2, 16)
    def _(k):
        drain(gy, s_gy, k)

    def add_peer(k, more=()):
        j = (k // 4) * 2 + k % 2
        t = part[k].astype(F32) + peer[j].astype(F32)
        for m in more:
            t = t + m[...].astype(F32)
        part[k] = t.astype(BF16)

    def q(ref, i):
        return ref.at[pl.ds(i * quarter, quarter)]

    def peer_arrived(j):
        send(peer.at[j], peer.at[j], s_p.at[j], r_p.at[j], partner).wait_recv()

    for j in range(8):
        peer_arrived(j)

    def hop_copy(k, i):
        side = k - 12
        return send(q(part.at[k], i), q(hop.at[side], i), s_h.at[2 * side + i], r_h.at[2 * side + i], (right, left)[side])

    for k in (12, 13):
        add_peer(k)
    for i in range(2):
        for k in (12, 13):
            hop_copy(k, i).start()

    def dw_step(j):
        xk = xb[pl.ds(2 * j, 2)].reshape(2 * half, xb.shape[2])
        duk = jnp.concatenate((du[2 * j], du[2 * j + 1]), axis=1)
        dwgu[...] += dot(duk, xk, COLS_ROWS)

    def tail_copy(side, qi):
        k = ((9, 5), (4, 8))[side][qi // 2]
        dst = (froml, fromr)[side].at[qi]
        return send(q(part.at[k], qi % 2), dst, s_t.at[4 * side + qi], r_t.at[4 * side + qi], (right, left)[side])

    tail_order = ((2, 0, 3, 1), (0, 2, 1, 3))

    def tails():
        add_peer(5)
        add_peer(4)
        for side in range(2):
            for i in range(2):
                hop_copy(12 + side, i).wait_recv()
        add_peer(9, (hop.at[0],))
        add_peer(8, (hop.at[1],))
        for n in range(4):
            for side in range(2):
                tail_copy(side, tail_order[side][n]).start()

    @pl.loop(0, 8)
    def _(j):
        pl.when(j == 6)(tails)
        gather_step(xb, s_x, r_x, 2 * j, None)

        @pl.when(lax.rem(j, 2) == 1)
        def _():
            arrived(xb, s_x, r_x, 2 * j + 1)

        dw_step(j)

    ds = gy
    pltpu.make_async_copy(xin_hbm, xin, l_tok.at[0]).wait()
    pltpu.make_async_copy(gr_hbm, gr, l_tok.at[1]).wait()
    gamma = gamma_ref[...].astype(F32).reshape(1, gamma_ref.shape[0])

    def norm_quarter(qi):
        h, i = qi // 2, qi % 2
        tail_copy(0, qi).wait_recv()
        tail_copy(1, qi).wait_recv()
        step = 32

        @pl.loop(0, quarter // step)
        def _(n):
            rows = pl.ds(pl.multiple_of(n * step, step), step)
            inner = pl.ds(pl.multiple_of(i * quarter + n * step, step), step)
            tokens = pl.ds(pl.multiple_of(qi * quarter + n * step, step), step)
            dx = (part[h, inner].astype(F32) + peer[h, inner].astype(F32)
                  + froml[qi, rows].astype(F32) + fromr[qi, rows].astype(F32)).astype(BF16)
            xf = xin[tokens].astype(F32)
            inv = lax.rsqrt(jnp.mean(xf * xf, axis=-1, keepdims=True) + NORM_EPS)
            scaled = dx.astype(F32) * gamma
            proj = jnp.mean(scaled * xf, axis=-1, keepdims=True)
            out = (gr[tokens].astype(F32) + inv * (scaled - xf * (inv * inv) * proj)).astype(BF16)
            ds[h, inner] = out
            dso[tokens] = out

    def ds_copy(src, dst, i, dev):
        n = 2 * dst + i
        return send(q(ds.at[src], i), q(ds.at[dst], i), s_ds.at[n], r_ds.at[n], dev)

    for i in range(2):
        for h in (0, 1):
            norm_quarter(2 * h + i)
        for src, dst, dev in ((0, 4, right), (1, 5, left), (1, 8, right), (0, 9, left), (0, 2, partner), (1, 3, partner)):
            ds_copy(src, dst, i, dev).start()

    @pl.loop(0, 32)
    def _(n):
        o_copy(n).wait()

    @pl.loop(0, 16)
    def _(u):
        v, w = u - 4, u - 12
        i = jnp.where(u < 4, lax.rem(u, 2), jnp.where(u < 12, v // 4, w // 2))
        k = jnp.where(u < 4, 2 * (u // 2), jnp.where(u < 12, 4 + 2 * lax.rem(v, 4), 12 + 2 * lax.rem(w, 2)))

        @pl.when(k > 0)
        def _():
            for d in range(2):
                n = 2 * (k + d) + i
                block = q(ds.at[k + d], i)
                send(block, block, s_ds.at[n], r_ds.at[n], partner).wait_recv()

        @pl.when(k == 4)
        def _():
            for src, dst, dev in ((4, 12, right), (5, 13, left)):
                n = 2 * dst + i
                send(q(ds.at[src], i), q(ds.at[dst], i), s_ds.at[n], r_ds.at[n], dev).start()

        @pl.when((k > 0) & (lax.rem(k, 4) == 0))
        def _():
            for d in range(2):
                n = 2 * (k + 2 + d) + i
                send(q(ds.at[k + d], i), q(ds.at[k + 2 + d], i), s_ds.at[n], r_ds.at[n], partner).start()

        rows = pl.ds(pl.multiple_of(i * quarter, quarter), quarter)
        for d in range(2):
            block = ds[k + d, rows]
            n = 2 * (k + d) + i
            dob[n] = dot(wo[...], block, COLS_COLS).astype(BF16)
            dwo[...] += dot(ob[n], block, COLS_ROWS)

    @pl.loop(2, 16)
    def _(k):
        drain(xb, s_x, k)

    @pl.loop(4, 32)
    def _(n):
        block = q(ds.at[n // 2], 0)
        send(block, block, s_ds.at[n], s_ds.at[n], partner).wait_send()

    for j in range(8):
        send(peer.at[j], peer.at[j], s_p.at[j], s_p.at[j], partner).wait_send()
    for side in range(2):
        for i in range(2):
            hop_copy(12 + side, i).wait_send()
        for qi in range(4):
            tail_copy(side, qi).wait_send()


def solution(mesh):
    tp = mesh.shape["tp"]
    token_spec = P(("dp", "tp"), None)
    split_cols = P("dp", "tp")
    weight_cols = P(None, "tp")
    weight_rows = P("tp", None)

    def local_backward(x_norm, grad_y, u_gate, u_up, w_gate, w_up, w_down, x_in, gamma, grad_res, attn_out, w_out):
        rows, hid = x_norm.shape
        tokens, cols = u_gate.shape
        ocols = attn_out.shape[1]
        half = rows // 2
        quarter = half // 2
        any_spec = pl.BlockSpec(memory_space=pl.ANY)
        vmem_spec = pl.BlockSpec(memory_space=pltpu.VMEM)
        dma = pltpu.SemaphoreType.DMA
        results = pl.pallas_call(
            functools.partial(kernel, tp),
            out_shape=(
                pltpu.VMEM((rows, hid), BF16),
                pltpu.VMEM((32, ocols, quarter), BF16),
                pltpu.VMEM((2 * cols, hid), F32),
                pltpu.VMEM((cols, hid), F32),
                pltpu.VMEM((ocols, hid), F32),
            ),
            in_specs=[any_spec] * 8 + [vmem_spec] + [any_spec] * 3,
            out_specs=(vmem_spec,) * 5,
            scratch_shapes=[
                pltpu.VMEM((16, half, hid), BF16),
                pltpu.VMEM((16, half, hid), BF16),
                pltpu.VMEM((16, half, hid), BF16),
                pltpu.VMEM((8, half, hid), BF16),
                pltpu.VMEM((2, half, hid), BF16),
                pltpu.VMEM((4, quarter, hid), BF16),
                pltpu.VMEM((4, quarter, hid), BF16),
                pltpu.VMEM((16, 2 * cols, half), BF16),
                pltpu.VMEM((2 * cols, hid), BF16),
                pltpu.VMEM((cols, hid), BF16),
                pltpu.VMEM((ocols, hid), BF16),
                pltpu.VMEM((2, cols, half), BF16),
                pltpu.VMEM((2, cols, half), BF16),
                pltpu.VMEM((32, ocols, quarter), BF16),
                pltpu.VMEM((rows, hid), BF16),
                pltpu.VMEM((rows, hid), BF16),
                dma((16,)), dma((16,)),
                dma((16,)), dma((16,)),
                dma((8,)), dma((8,)),
                dma((4,)), dma((4,)),
                dma((8,)), dma((8,)),
                dma((32,)), dma((32,)),
                dma((4,)), dma((4,)), dma((4,)), dma((32,)), dma((2,)),
            ],
            compiler_params=pltpu.CompilerParams(
                collective_id=0, has_side_effects=True, vmem_limit_bytes=54_000_000),
            name="layer_backward",
        )(x_norm, grad_y, u_gate.T, u_up.T, w_gate.T, w_up.T, w_down, x_in, gamma, grad_res, attn_out.T,
          w_out)
        results = [pltpu.with_memory_space_constraint(r, pltpu.VMEM) for r in results]
        ds, do, dwg, dwu, dwd, dwo = pl.pallas_call(
            functools.partial(write_kernel, tp, half),
            out_shape=(
                jax.ShapeDtypeStruct((rows, hid), BF16),
                jax.ShapeDtypeStruct((ocols, tokens), BF16),
                jax.ShapeDtypeStruct((cols, hid), F32),
                jax.ShapeDtypeStruct((cols, hid), F32),
                jax.ShapeDtypeStruct((cols, hid), F32),
                jax.ShapeDtypeStruct((ocols, hid), F32),
            ),
            in_specs=[vmem_spec] * 5,
            out_specs=(any_spec,) * 6,
            scratch_shapes=[dma((5,)), dma((32,))],
            compiler_params=pltpu.CompilerParams(vmem_limit_bytes=1_000_000),
            name="write_results",
        )(*results)
        return ds, do.T, dwg.T, dwu.T, dwd, dwo

    return jax.shard_map(
        local_backward,
        mesh=mesh,
        in_specs=(token_spec, token_spec, split_cols, split_cols, weight_cols, weight_cols, weight_rows,
                  token_spec, P(None), token_spec, split_cols, weight_rows),
        out_specs=(token_spec, split_cols, split_cols, split_cols, token_spec, token_spec),
        check_vma=False,
    )
```

```python
import functools

import jax
import jax.numpy as jnp
from jax import lax
from jax.experimental import pallas as pl
from jax.experimental.pallas import tpu as pltpu
from jax.sharding import PartitionSpec as P

NORM_EPS = 1e-5
F32 = jnp.float32
BF16 = jnp.bfloat16
ROWS_ROWS = (((0,), (0,)), ((), ()))
COLS_COLS = (((1,), (1,)), ((), ()))
COLS_ROWS = (((1,), (0,)), ((), ()))
MESH = pl.DeviceIdType.MESH
PIECES = 4


def dot(a, b, dims):
    return lax.dot_general(a, b, dims, preferred_element_type=F32)


def slot_token(tp, half, k):
    me = lax.axis_index("tp")
    g, b, i = k // 4, lax.rem(k, 4) // 2, lax.rem(k, 2)
    dx = jnp.where(g == 0, 0, jnp.where(g == 3, 2, 2 * i - 1))
    h = jnp.where(g == 2, 1 - i, i)
    chip = lax.rem(me // 2 + dx + tp // 2, tp // 2)
    shard = 2 * chip + lax.rem(lax.rem(me, 2) + b, 2)
    return pl.multiple_of((2 * shard + h) * half, half)


def write_kernel(tp, half, dso, dob, dwgu, dwd, dwo, ds_out, do_out, dwg_out, dwu_out, dwd_out, dwo_out, sem, sem_do):
    cols, quarter = dwd.shape[0], half // 2
    copies = [pltpu.make_async_copy(src, dst, sem.at[i]) for i, (src, dst) in enumerate((
        (dwgu.at[pl.ds(0, cols)], dwg_out), (dwgu.at[pl.ds(cols, cols)], dwu_out), (dwd, dwd_out), (dso, ds_out),
        (dwo, dwo_out)))]

    def do_copy(n):
        tokens = pl.ds(pl.multiple_of(slot_token(tp, half, n // 2) + lax.rem(n, 2) * quarter, quarter), quarter)
        return pltpu.make_async_copy(dob.at[n], do_out.at[:, tokens], sem_do.at[n])

    for c in copies:
        c.start()

    @pl.loop(0, 2 * 2 * tp)
    def _(n):
        do_copy(n).start()

    @pl.loop(0, 2 * 2 * tp)
    def _(n):
        do_copy(n).wait()

    for c in copies:
        c.wait()


def kernel(tp, x_hbm, gy_hbm, ug_hbm, uu_hbm, wg_hbm, wu_hbm, wd_hbm, xin_hbm, gamma_hbm, gr_hbm, o_hbm, wo_hbm,
           dso, dob, dwgu, dwd, dwo,
           gy, xb, part, peer, hop, froml, fromr, du, wgu, wd, wo, ugb, uub, ob, xin, gr, gamma_ref,
           s_gy, r_gy, s_x, r_x, s_p, r_p, s_h, r_h, s_t, r_t, s_ds, r_ds, s_e, r_e,
           l_w, l_own, l_u, l_o, l_tok):
    half = gy.shape[1]
    cols = wd.shape[0]
    quarter = half // 2
    me = lax.axis_index("tp")
    right = lax.rem(me + 2, tp)
    left = lax.rem(me + tp - 2, tp)
    partner = me + 1 - 2 * lax.rem(me, 2)
    slot_row = functools.partial(slot_token, tp, half)

    def send(src, dst, ssem, rsem, dev):
        return pltpu.make_async_remote_copy(
            src_ref=src, dst_ref=dst, send_sem=ssem, recv_sem=rsem, device_id={"tp": dev}, device_id_type=MESH)

    def u_copies(k):
        tokens = pl.ds(slot_row(k), half)
        at = lax.rem(k, 2)
        return (pltpu.make_async_copy(ug_hbm.at[:, tokens], ugb.at[at], l_u.at[2 * at]),
                pltpu.make_async_copy(uu_hbm.at[:, tokens], uub.at[at], l_u.at[2 * at + 1]))

    def o_copy(n):
        tokens = pl.ds(pl.multiple_of(slot_row(n // 2) + lax.rem(n, 2) * quarter, quarter), quarter)
        return pltpu.make_async_copy(o_hbm.at[:, tokens], ob.at[n], l_o.at[n])

    def own(hbm, h):
        return hbm.at[pl.ds(h * half, half)]

    barrier = pltpu.get_barrier_semaphore()
    for dev in (left, right, partner):
        pl.semaphore_signal(barrier, inc=1, device_id={"tp": dev}, device_id_type=MESH)
    pl.semaphore_wait(barrier, 3)

    def send_own(hbm, buf, ssem, rsem):
        for src, dst, dev in ((0, 4, right), (1, 5, left), (1, 8, right), (0, 9, left), (0, 2, partner), (1, 3, partner)):
            send(own(hbm, src), buf.at[dst], ssem.at[dst], rsem.at[dst], dev).start()

    def arrived(buf, ssem, rsem, k):
        send(buf.at[k], buf.at[k], ssem.at[k], rsem.at[k], partner).wait_recv()

    def drain(buf, ssem, k):
        send(buf.at[k], buf.at[k], ssem.at[k], ssem.at[k], partner).wait_send()

    def gather_step(buf, ssem, rsem, k, also):
        place = lax.rem(k, 4)

        @pl.when((place == 0) & (k > 0))
        def _():
            arrived(buf, ssem, rsem, k)
            arrived(buf, ssem, rsem, k + 1)

            @pl.when(k == 4)
            def _():
                send(buf.at[4], buf.at[12], ssem.at[12], rsem.at[12], right).start()
                send(buf.at[5], buf.at[13], ssem.at[13], rsem.at[13], left).start()

            send(buf.at[k], buf.at[k + 2], ssem.at[k + 2], rsem.at[k + 2], partner).start()
            send(buf.at[k + 1], buf.at[k + 3], ssem.at[k + 3], rsem.at[k + 3], partner).start()
            if also is not None:
                pl.when(k == 4)(also)

        @pl.when(place >= 2)
        def _():
            arrived(buf, ssem, rsem, k)

    send_own(gy_hbm, gy, s_gy, r_gy)
    for h in range(2):
        pltpu.make_async_copy(own(gy_hbm, h), gy.at[h], l_own.at[h]).start()
        pltpu.make_async_copy(own(x_hbm, h), xb.at[h], l_own.at[2 + h]).start()
    weights = ((wd_hbm, wd), (wg_hbm, wgu.at[pl.ds(0, cols)]), (wu_hbm, wgu.at[pl.ds(cols, cols)]), (wo_hbm, wo))
    for i, (src, dst) in enumerate(weights):
        pltpu.make_async_copy(src, dst, l_w.at[i]).start()
    for c in u_copies(0):
        c.start()
    pltpu.make_async_copy(xin_hbm, xin, l_tok.at[0]).start()
    pltpu.make_async_copy(gr_hbm, gr, l_tok.at[1]).start()
    pltpu.make_async_copy(gamma_hbm, gamma_ref, l_tok.at[2]).start()

    @pl.loop(0, 32)
    def _(n):
        o_copy(n).start()

    dwd[...] = jnp.zeros_like(dwd)
    dwgu[...] = jnp.zeros_like(dwgu)
    dwo[...] = jnp.zeros_like(dwo)
    for i, (src, dst) in enumerate(weights):
        pltpu.make_async_copy(src, dst, l_w.at[i]).wait()
    for h in range(2):
        pltpu.make_async_copy(own(gy_hbm, h), gy.at[h], l_own.at[h]).wait()
        pltpu.make_async_copy(own(x_hbm, h), xb.at[h], l_own.at[2 + h]).wait()

    def part_copy(k):
        j = (k // 4) * 2 + lax.rem(k, 2)
        return send(part.at[k], peer.at[j], s_p.at[j], r_p.at[j], partner)

    @pl.loop(0, 16)
    def _(k):
        @pl.when(k + 1 < 16)
        def _():
            for c in u_copies(k + 1):
                c.start()

        @pl.when((k > 0) & (lax.rem(k + 3, 4) >= 2))
        def _():
            part_copy(k - 1).start()

        gather_step(gy, s_gy, r_gy, k, lambda: send_own(x_hbm, xb, s_x, r_x))
        for c in u_copies(k):
            c.wait()
        at = lax.rem(k, 2)
        gyk = gy[k]
        gh = dot(wd[...], gyk, COLS_COLS)
        gate = ugb[at].astype(F32)
        up = uub[at].astype(F32)
        sig = jax.nn.sigmoid(gate)
        act = gate * sig
        silu = sig * (1.0 + gate * (1.0 - sig))
        z = (act * up).astype(BF16)
        du_up = (gh * act).astype(BF16)
        du_gate = (gh * up * silu).astype(BF16)
        du[k, pl.ds(0, cols)] = du_gate
        du[k, pl.ds(cols, cols)] = du_up
        dwd[...] += dot(z, gyk, COLS_ROWS)
        part[k] = dot(du[k], wgu[...], ROWS_ROWS).astype(BF16)

    part_copy(15).start()

    @pl.loop(2, 16)
    def _(k):
        drain(gy, s_gy, k)

    def add_peer(k, more=()):
        j = (k // 4) * 2 + k % 2
        t = part[k].astype(F32) + peer[j].astype(F32)
        for m in more:
            t = t + m[...].astype(F32)
        part[k] = t.astype(BF16)

    def q(ref, i):
        return ref.at[pl.ds(i * quarter, quarter)]

    def peer_arrived(j):
        send(peer.at[j], peer.at[j], s_p.at[j], r_p.at[j], partner).wait_recv()

    for j in range(8):
        peer_arrived(j)

    def hop_copy(k, i):
        side = k - 12
        return send(q(part.at[k], i), q(hop.at[side], i), s_h.at[2 * side + i], r_h.at[2 * side + i], (right, left)[side])

    for k in (12, 13):
        add_peer(k)
    for i in range(2):
        for k in (12, 13):
            hop_copy(k, i).start()

    def dw_step(j):
        xk = xb[pl.ds(2 * j, 2)].reshape(2 * half, xb.shape[2])
        duk = jnp.concatenate((du[2 * j], du[2 * j + 1]), axis=1)
        dwgu[...] += dot(duk, xk, COLS_ROWS)

    def tail_copy(side, qi):
        k = ((9, 5), (4, 8))[side][qi // 2]
        dst = (froml, fromr)[side].at[qi]
        return send(q(part.at[k], qi % 2), dst, s_t.at[4 * side + qi], r_t.at[4 * side + qi], (right, left)[side])

    tail_order = ((2, 0, 3, 1), (0, 2, 1, 3))

    def tails():
        add_peer(5)
        add_peer(4)
        for side in range(2):
            for i in range(2):
                hop_copy(12 + side, i).wait_recv()
        add_peer(9, (hop.at[0],))
        add_peer(8, (hop.at[1],))
        for n in range(4):
            for side in range(2):
                tail_copy(side, tail_order[side][n]).start()

    @pl.loop(0, 8)
    def _(j):
        pl.when(j == 6)(tails)
        gather_step(xb, s_x, r_x, 2 * j, None)

        @pl.when(lax.rem(j, 2) == 1)
        def _():
            arrived(xb, s_x, r_x, 2 * j + 1)

        dw_step(j)

    ds = gy
    pltpu.make_async_copy(xin_hbm, xin, l_tok.at[0]).wait()
    pltpu.make_async_copy(gr_hbm, gr, l_tok.at[1]).wait()
    pltpu.make_async_copy(gamma_hbm, gamma_ref, l_tok.at[2]).wait()
    gamma = gamma_ref[...].astype(F32).reshape(1, gamma_ref.shape[0])

    def norm_quarter(qi):
        h, i = qi // 2, qi % 2
        tail_copy(0, qi).wait_recv()
        tail_copy(1, qi).wait_recv()
        step = 32

        @pl.loop(0, quarter // step)
        def _(n):
            rows = pl.ds(pl.multiple_of(n * step, step), step)
            inner = pl.ds(pl.multiple_of(i * quarter + n * step, step), step)
            tokens = pl.ds(pl.multiple_of(qi * quarter + n * step, step), step)
            dx = (part[h, inner].astype(F32) + peer[h, inner].astype(F32)
                  + froml[qi, rows].astype(F32) + fromr[qi, rows].astype(F32)).astype(BF16)
            xf = xin[tokens].astype(F32)
            inv = lax.rsqrt(jnp.mean(xf * xf, axis=-1, keepdims=True) + NORM_EPS)
            scaled = dx.astype(F32) * gamma
            proj = jnp.mean(scaled * xf, axis=-1, keepdims=True)
            out = (gr[tokens].astype(F32) + inv * (scaled - xf * (inv * inv) * proj)).astype(BF16)
            ds[h, inner] = out
            dso[tokens] = out

    def ds_copy(src, dst, i, dev):
        n = 2 * dst + i
        return send(q(ds.at[src], i), q(ds.at[dst], i), s_ds.at[n], r_ds.at[n], dev)

    for i in range(2):
        for h in (0, 1):
            norm_quarter(2 * h + i)
        for src, dst, dev in ((0, 4, right), (1, 5, left), (1, 8, right), (0, 9, left), (0, 2, partner), (1, 3, partner)):
            ds_copy(src, dst, i, dev).start()

    @pl.loop(0, 32)
    def _(n):
        o_copy(n).wait()

    @pl.loop(2, 16)
    def _(k):
        drain(xb, s_x, k)

    for j in range(8):
        send(peer.at[j], peer.at[j], s_p.at[j], s_p.at[j], partner).wait_send()
    for side in range(2):
        for i in range(2):
            hop_copy(12 + side, i).wait_send()
        for qi in range(4):
            tail_copy(side, qi).wait_send()

    def piece_copy(src, dst, e, dev):
        n = PIECES * (dst - 12) + e
        rows = pl.ds(quarter + e * (quarter // PIECES), quarter // PIECES)
        return send(ds.at[src, rows], ds.at[dst, rows], s_e.at[n], r_e.at[n], dev)

    def products(k, i):
        rows = pl.ds(pl.multiple_of(i * quarter, quarter), quarter)
        for d in range(2):
            block = ds[k + d, rows]
            n = 2 * (k + d) + i
            dob[n] = dot(wo[...], block, COLS_COLS).astype(BF16)
            dwo[...] += dot(ob[n], block, COLS_ROWS)

    @pl.loop(0, 14)
    def _(u):
        v, w = u - 4, u - 12
        i = jnp.where(u < 4, lax.rem(u, 2), jnp.where(u < 12, v // 4, w // 2))
        k = jnp.where(u < 4, 2 * (u // 2), jnp.where(u < 12, 4 + 2 * lax.rem(v, 4), 12 + 2 * lax.rem(w, 2)))

        @pl.when(k > 0)
        def _():
            for d in range(2):
                n = 2 * (k + d) + i
                block = q(ds.at[k + d], i)
                send(block, block, s_ds.at[n], r_ds.at[n], partner).wait_recv()

        @pl.when((k == 4) & (i == 0))
        def _():
            for src, dst, dev in ((4, 12, right), (5, 13, left)):
                ds_copy(src, dst, 0, dev).start()

        @pl.when((k == 4) & (i == 1))
        def _():
            for e in range(PIECES):
                for src, dst, dev in ((4, 12, right), (5, 13, left)):
                    piece_copy(src, dst, e, dev).start()

        @pl.when((k > 0) & (lax.rem(k, 4) == 0))
        def _():
            for d in range(2):
                n = 2 * (k + 2 + d) + i
                send(q(ds.at[k + d], i), q(ds.at[k + 2 + d], i), s_ds.at[n], r_ds.at[n], partner).start()

        products(k, i)

    for e in range(PIECES):
        for d in range(2):
            piece_copy(12 + d, 12 + d, e, partner).wait_recv()
            piece_copy(12 + d, 14 + d, e, partner).start()
    products(12, 1)
    for e in range(PIECES):
        for d in range(2):
            piece_copy(14 + d, 14 + d, e, partner).wait_recv()
    products(14, 1)

    @pl.loop(4, 28)
    def _(n):
        @pl.when((n < 24) | (lax.rem(n, 2) == 0))
        def _():
            block = q(ds.at[n // 2], 0)
            send(block, block, s_ds.at[n], s_ds.at[n], partner).wait_send()

    for i in (28, 30):
        ds_copy(14, i // 2, 0, partner).wait_send()
    for e in range(PIECES):
        for dst in range(12, 16):
            piece_copy(dst, dst, e, partner).wait_send()


def solution(mesh):
    tp = mesh.shape["tp"]
    token_spec = P(("dp", "tp"), None)
    split_cols = P("dp", "tp")
    weight_cols = P(None, "tp")
    weight_rows = P("tp", None)

    def local_backward(x_norm, grad_y, u_gate, u_up, w_gate, w_up, w_down, x_in, gamma, grad_res, attn_out, w_out):
        rows, hid = x_norm.shape
        tokens, cols = u_gate.shape
        ocols = attn_out.shape[1]
        half = rows // 2
        quarter = half // 2
        any_spec = pl.BlockSpec(memory_space=pl.ANY)
        vmem_spec = pl.BlockSpec(memory_space=pltpu.VMEM)
        dma = pltpu.SemaphoreType.DMA
        results = pl.pallas_call(
            functools.partial(kernel, tp),
            out_shape=(
                pltpu.VMEM((rows, hid), BF16),
                pltpu.VMEM((32, ocols, quarter), BF16),
                pltpu.VMEM((2 * cols, hid), F32),
                pltpu.VMEM((cols, hid), F32),
                pltpu.VMEM((ocols, hid), F32),
            ),
            in_specs=[any_spec] * 12,
            out_specs=(vmem_spec,) * 5,
            scratch_shapes=[
                pltpu.VMEM((16, half, hid), BF16),
                pltpu.VMEM((16, half, hid), BF16),
                pltpu.VMEM((16, half, hid), BF16),
                pltpu.VMEM((8, half, hid), BF16),
                pltpu.VMEM((2, half, hid), BF16),
                pltpu.VMEM((4, quarter, hid), BF16),
                pltpu.VMEM((4, quarter, hid), BF16),
                pltpu.VMEM((16, 2 * cols, half), BF16),
                pltpu.VMEM((2 * cols, hid), BF16),
                pltpu.VMEM((cols, hid), BF16),
                pltpu.VMEM((ocols, hid), BF16),
                pltpu.VMEM((2, cols, half), BF16),
                pltpu.VMEM((2, cols, half), BF16),
                pltpu.VMEM((32, ocols, quarter), BF16),
                pltpu.VMEM((rows, hid), BF16),
                pltpu.VMEM((rows, hid), BF16),
                pltpu.VMEM((hid,), BF16),
                dma((16,)), dma((16,)),
                dma((16,)), dma((16,)),
                dma((8,)), dma((8,)),
                dma((4,)), dma((4,)),
                dma((8,)), dma((8,)),
                dma((32,)), dma((32,)),
                dma((4 * PIECES,)), dma((4 * PIECES,)),
                dma((4,)), dma((4,)), dma((4,)), dma((32,)), dma((3,)),
            ],
            compiler_params=pltpu.CompilerParams(
                collective_id=0, has_side_effects=True, vmem_limit_bytes=54_000_000),
            name="layer_backward",
        )(x_norm, grad_y, u_gate.T, u_up.T, w_gate.T, w_up.T, w_down, x_in, gamma, grad_res, attn_out.T,
          w_out)
        results = [pltpu.with_memory_space_constraint(r, pltpu.VMEM) for r in results]
        ds, do, dwg, dwu, dwd, dwo = pl.pallas_call(
            functools.partial(write_kernel, tp, half),
            out_shape=(
                jax.ShapeDtypeStruct((rows, hid), BF16),
                jax.ShapeDtypeStruct((ocols, tokens), BF16),
                jax.ShapeDtypeStruct((cols, hid), F32),
                jax.ShapeDtypeStruct((cols, hid), F32),
                jax.ShapeDtypeStruct((cols, hid), F32),
                jax.ShapeDtypeStruct((ocols, hid), F32),
            ),
            in_specs=[vmem_spec] * 5,
            out_specs=(any_spec,) * 6,
            scratch_shapes=[dma((5,)), dma((32,))],
            compiler_params=pltpu.CompilerParams(vmem_limit_bytes=1_000_000),
            name="write_results",
        )(*results)
        return ds, do.T, dwg.T, dwu.T, dwd, dwo

    return jax.shard_map(
        local_backward,
        mesh=mesh,
        in_specs=(token_spec, token_spec, split_cols, split_cols, weight_cols, weight_cols, weight_rows,
                  token_spec, P(None), token_spec, split_cols, weight_rows),
        out_specs=(token_spec, split_cols, split_cols, split_cols, token_spec, token_spec),
        check_vma=False,
    )
```

```python
import functools

import jax
import jax.numpy as jnp
from jax import lax
from jax.experimental import pallas as pl
from jax.experimental.pallas import tpu as pltpu
from jax.sharding import PartitionSpec as P

NORM_EPS = 1e-5
F32 = jnp.float32
BF16 = jnp.bfloat16
ROWS_ROWS = (((0,), (0,)), ((), ()))
COLS_COLS = (((1,), (1,)), ((), ()))
COLS_ROWS = (((1,), (0,)), ((), ()))
MESH = pl.DeviceIdType.MESH
PIECES = 4


def dot(a, b, dims):
    return lax.dot_general(a, b, dims, preferred_element_type=F32)


def slot_token(tp, half, k):
    me = lax.axis_index("tp")
    g, b, i = k // 4, lax.rem(k, 4) // 2, lax.rem(k, 2)
    dx = jnp.where(g == 0, 0, jnp.where(g == 3, 2, 2 * i - 1))
    h = jnp.where(g == 2, 1 - i, i)
    chip = lax.rem(me // 2 + dx + tp // 2, tp // 2)
    shard = 2 * chip + lax.rem(lax.rem(me, 2) + b, 2)
    return pl.multiple_of((2 * shard + h) * half, half)


def write_kernel(dso, dob, dwgu, dwd, dwo, ds_out, do_out, dwg_out, dwu_out, dwd_out, dwo_out, sem):
    cols = dwd.shape[0]
    copies = [pltpu.make_async_copy(src, dst, sem) for src, dst in (
        (dwgu.at[pl.ds(0, cols)], dwg_out), (dwgu.at[pl.ds(cols, cols)], dwu_out), (dwd, dwd_out), (dso, ds_out),
        (dob, do_out), (dwo, dwo_out))]
    for c in copies:
        c.start()
    for c in copies:
        c.wait()


def kernel(tp, x_hbm, gy_hbm, ug_hbm, uu_hbm, wg_hbm, wu_hbm, wd_hbm, xin_hbm, gamma_hbm, gr_hbm, o_hbm, wo_hbm,
           dso, dob, dwgu, dwd, dwo,
           gy, xb, part, peer, hop, frm, du, weights, ub, ob, tok, gamma_ref,
           sent, r_gy, r_x, r_e, r_t, r_p, r_h, l_u, l_w, l_o, l_tok, l_gamma):
    half = gy.shape[1]
    cols, ocols = dwd.shape[0], dwo.shape[0]
    wgu = weights.at[pl.ds(0, 2 * cols)]
    wd = weights.at[pl.ds(2 * cols, cols)]
    wo = weights.at[pl.ds(3 * cols, ocols)]
    s_gy, s_x, s_p, s_h, s_t, s_ds = (sent.at[i] for i in range(6))
    quarter = half // 2
    me = lax.axis_index("tp")
    right = lax.rem(me + 2, tp)
    left = lax.rem(me + tp - 2, tp)
    partner = me + 1 - 2 * lax.rem(me, 2)
    slot_row = functools.partial(slot_token, tp, half)

    def send(src, dst, ssem, rsem, dev):
        return pltpu.make_async_remote_copy(
            src_ref=src, dst_ref=dst, send_sem=ssem, recv_sem=rsem, device_id={"tp": dev}, device_id_type=MESH)

    def u_copies(k):
        tokens = pl.ds(slot_row(k), half)
        at = lax.rem(k, 2)
        return (pltpu.make_async_copy(ug_hbm.at[:, tokens], ub.at[at, 0], l_u.at[at]),
                pltpu.make_async_copy(uu_hbm.at[:, tokens], ub.at[at, 1], l_u.at[at]))

    def o_copy(n):
        tokens = pl.ds(pl.multiple_of(slot_row(n // 2) + lax.rem(n, 2) * quarter, quarter), quarter)
        return pltpu.make_async_copy(o_hbm.at[:, tokens], ob.at[n], l_o)

    def own(hbm, h):
        return hbm.at[pl.ds(h * half, half)]

    barrier = pltpu.get_barrier_semaphore()
    for dev in (left, right, partner):
        pl.semaphore_signal(barrier, inc=1, device_id={"tp": dev}, device_id_type=MESH)
    pl.semaphore_wait(barrier, 3)

    def send_own(hbm, buf, ssem, rsem):
        for src, dst, dev in ((0, 4, right), (1, 5, left), (1, 8, right), (0, 9, left), (0, 2, partner), (1, 3, partner)):
            send(own(hbm, src), buf.at[dst], ssem, rsem.at[dst // 2], dev).start()

    def arrived(ref, rsem):
        pltpu.make_async_copy(ref, ref, rsem).wait()

    def left_here(ref, ssem):
        send(ref, ref, ssem, ssem, partner).wait_send()

    def gather_step(buf, ssem, rsem, k, also):
        place = lax.rem(k, 4)

        @pl.when((k >= 2) & (lax.rem(place, 2) == 0))
        def _():
            arrived(buf.at[pl.ds(k, 2)], rsem.at[k // 2])

        @pl.when(k == 4)
        def _():
            send(buf.at[4], buf.at[12], ssem, rsem.at[6], right).start()
            send(buf.at[5], buf.at[13], ssem, rsem.at[6], left).start()

        @pl.when((k >= 4) & (place == 0))
        def _():
            for d in range(2):
                send(buf.at[k + d], buf.at[k + 2 + d], ssem, rsem.at[k // 2 + 1], partner).start()
            if also is not None:
                pl.when(k == 4)(also)

    send_own(gy_hbm, gy, s_gy, r_gy)
    for h in range(2):
        pltpu.make_async_copy(own(gy_hbm, h), gy.at[h], r_gy.at[0]).start()
        pltpu.make_async_copy(own(x_hbm, h), xb.at[h], r_x.at[0]).start()
    for i, src in enumerate((wg_hbm, wu_hbm, wd_hbm, wo_hbm)):
        pltpu.make_async_copy(src, weights.at[pl.ds(i * cols, src.shape[0])], l_w).start()
    for c in u_copies(0):
        c.start()
    pltpu.make_async_copy(xin_hbm, tok.at[0], l_tok).start()
    pltpu.make_async_copy(gr_hbm, tok.at[1], l_tok).start()
    pltpu.make_async_copy(gamma_hbm, gamma_ref, l_gamma).start()

    @pl.loop(0, 32)
    def _(n):
        o_copy(n).start()

    dwd[...] = jnp.zeros_like(dwd)
    dwgu[...] = jnp.zeros_like(dwgu)
    dwo[...] = jnp.zeros_like(dwo)
    arrived(weights, l_w)
    arrived(gy.at[pl.ds(0, 2)], r_gy.at[0])
    arrived(xb.at[pl.ds(0, 2)], r_x.at[0])

    def part_copy(k):
        j = (k // 4) * 2 + lax.rem(k, 2)
        return send(part.at[k], peer.at[j], s_p, r_p, partner)

    @pl.loop(0, 16)
    def _(k):
        @pl.when(k + 1 < 16)
        def _():
            for c in u_copies(k + 1):
                c.start()

        @pl.when((k > 0) & (lax.rem(k + 3, 4) >= 2))
        def _():
            part_copy(k - 1).start()

        gather_step(gy, s_gy, r_gy, k, lambda: send_own(x_hbm, xb, s_x, r_x))
        at = lax.rem(k, 2)
        arrived(ub.at[at], l_u.at[at])
        gyk = gy[k]
        gh = dot(wd[...], gyk, COLS_COLS)
        gate = ub[at, 0].astype(F32)
        up = ub[at, 1].astype(F32)
        sig = jax.nn.sigmoid(gate)
        act = gate * sig
        silu = sig * (1.0 + gate * (1.0 - sig))
        z = (act * up).astype(BF16)
        du_up = (gh * act).astype(BF16)
        du_gate = (gh * up * silu).astype(BF16)
        du[k, pl.ds(0, cols)] = du_gate
        du[k, pl.ds(cols, cols)] = du_up
        dwd[...] += dot(z, gyk, COLS_ROWS)
        part[k] = dot(du[k], wgu[...], ROWS_ROWS).astype(BF16)

    part_copy(15).start()

    left_here(gy.at[pl.ds(0, 14)], s_gy)

    def add_peer(k, more=()):
        j = (k // 4) * 2 + k % 2
        t = part[k].astype(F32) + peer[j].astype(F32)
        for m in more:
            t = t + m[...].astype(F32)
        part[k] = t.astype(BF16)

    def q(ref, i):
        return ref.at[pl.ds(i * quarter, quarter)]

    arrived(peer, r_p)

    def hop_copy(k, i):
        side = k - 12
        return send(q(part.at[k], i), q(hop.at[side], i), s_h, r_h, (right, left)[side])

    for k in (12, 13):
        add_peer(k)
    for i in range(2):
        for k in (12, 13):
            hop_copy(k, i).start()

    def dw_step(j):
        xk = xb[pl.ds(2 * j, 2)].reshape(2 * half, xb.shape[2])
        duk = jnp.concatenate((du[2 * j], du[2 * j + 1]), axis=1)
        dwgu[...] += dot(duk, xk, COLS_ROWS)

    def tail_copy(side, qi):
        k = ((9, 5), (4, 8))[side][qi // 2]
        return send(q(part.at[k], qi % 2), frm.at[qi, side], s_t, r_t.at[qi], (right, left)[side])

    tail_order = ((2, 0, 3, 1), (0, 2, 1, 3))

    def tails():
        add_peer(5)
        add_peer(4)
        arrived(hop, r_h)
        add_peer(9, (hop.at[0],))
        add_peer(8, (hop.at[1],))
        for n in range(4):
            for side in range(2):
                tail_copy(side, tail_order[side][n]).start()

    @pl.loop(0, 8)
    def _(j):
        pl.when(j == 6)(tails)
        gather_step(xb, s_x, r_x, 2 * j, None)
        dw_step(j)

    ds = gy
    arrived(tok, l_tok)
    arrived(gamma_ref, l_gamma)
    gamma = gamma_ref[...].astype(F32).reshape(1, gamma_ref.shape[0])

    def norm_quarter(qi):
        h, i = qi // 2, qi % 2
        arrived(frm.at[qi], r_t.at[qi])
        step = 32

        @pl.loop(0, quarter // step)
        def _(n):
            rows = pl.ds(pl.multiple_of(n * step, step), step)
            inner = pl.ds(pl.multiple_of(i * quarter + n * step, step), step)
            tokens = pl.ds(pl.multiple_of(qi * quarter + n * step, step), step)
            dx = (part[h, inner].astype(F32) + peer[h, inner].astype(F32)
                  + frm[qi, 0, rows].astype(F32) + frm[qi, 1, rows].astype(F32)).astype(BF16)
            xf = tok[0, tokens].astype(F32)
            inv = lax.rsqrt(jnp.mean(xf * xf, axis=-1, keepdims=True) + NORM_EPS)
            scaled = dx.astype(F32) * gamma
            proj = jnp.mean(scaled * xf, axis=-1, keepdims=True)
            out = (tok[1, tokens].astype(F32) + inv * (scaled - xf * (inv * inv) * proj)).astype(BF16)
            ds[h, inner] = out
            dso[tokens] = out

    def ds_copy(src, dst, i, dev):
        return send(q(ds.at[src], i), q(ds.at[dst], i), s_ds, r_gy.at[dst // 2 + 7 * i], dev)

    for i in range(2):
        for h in (0, 1):
            norm_quarter(2 * h + i)
        for src, dst, dev in ((0, 4, right), (1, 5, left), (1, 8, right), (0, 9, left), (0, 2, partner), (1, 3, partner)):
            ds_copy(src, dst, i, dev).start()

    arrived(ob, l_o)
    left_here(xb.at[pl.ds(0, 14)], s_x)
    left_here(peer, s_p)
    left_here(hop, s_h)
    left_here(frm, s_t)

    def piece_copy(src, dst, e, dev):
        rows = pl.ds(quarter + e * (quarter // PIECES), quarter // PIECES)
        return send(ds.at[src, rows], ds.at[dst, rows], s_ds, r_e.at[PIECES * (dst // 2 - 6) + e], dev)

    def piece_arrived(k, e):
        rows = pl.ds(quarter + e * (quarter // PIECES), quarter // PIECES)
        arrived(ds.at[pl.ds(k, 2), rows], r_e.at[PIECES * (k // 2 - 6) + e])

    def products(k, i):
        rows = pl.ds(pl.multiple_of(i * quarter, quarter), quarter)
        for d in range(2):
            block = ds[k + d, rows]
            n = 2 * (k + d) + i
            tokens = pl.ds(pl.multiple_of(slot_row(k + d) + i * quarter, quarter), quarter)
            dob[:, tokens] = dot(wo[...], block, COLS_COLS).astype(BF16)
            dwo[...] += dot(ob[n], block, COLS_ROWS)

    @pl.loop(0, 14)
    def _(u):
        v, w = u - 4, u - 12
        i = jnp.where(u < 4, lax.rem(u, 2), jnp.where(u < 12, v // 4, w // 2))
        k = jnp.where(u < 4, 2 * (u // 2), jnp.where(u < 12, 4 + 2 * lax.rem(v, 4), 12 + 2 * lax.rem(w, 2)))

        @pl.when(k > 0)
        def _():
            rows = pl.ds(pl.multiple_of(i * quarter, quarter), quarter)
            arrived(ds.at[pl.ds(k, 2), rows], r_gy.at[k // 2 + 7 * i])

        @pl.when((k == 4) & (i == 0))
        def _():
            for src, dst, dev in ((4, 12, right), (5, 13, left)):
                ds_copy(src, dst, 0, dev).start()

        @pl.when((k == 4) & (i == 1))
        def _():
            for e in range(PIECES):
                for src, dst, dev in ((4, 12, right), (5, 13, left)):
                    piece_copy(src, dst, e, dev).start()

        @pl.when((k > 0) & (lax.rem(k, 4) == 0))
        def _():
            for d in range(2):
                ds_copy(k + d, k + 2 + d, i, partner).start()

        products(k, i)

    for e in range(PIECES):
        piece_arrived(12, e)
        for d in range(2):
            piece_copy(12 + d, 14 + d, e, partner).start()
    products(12, 1)
    for e in range(PIECES):
        piece_arrived(14, e)
    products(14, 1)
    left_here(ds.at[pl.ds(0, 14)], s_ds)


def solution(mesh):
    tp = mesh.shape["tp"]
    token_spec = P(("dp", "tp"), None)
    split_cols = P("dp", "tp")
    weight_cols = P(None, "tp")
    weight_rows = P("tp", None)

    def local_backward(x_norm, grad_y, u_gate, u_up, w_gate, w_up, w_down, x_in, gamma, grad_res, attn_out, w_out):
        rows, hid = x_norm.shape
        tokens, cols = u_gate.shape
        ocols = attn_out.shape[1]
        half = rows // 2
        quarter = half // 2
        any_spec = pl.BlockSpec(memory_space=pl.ANY)
        vmem_spec = pl.BlockSpec(memory_space=pltpu.VMEM)
        dma = pltpu.SemaphoreType.DMA
        results = pl.pallas_call(
            functools.partial(kernel, tp),
            out_shape=(
                pltpu.VMEM((rows, hid), BF16),
                pltpu.VMEM((ocols, tokens), BF16),
                pltpu.VMEM((2 * cols, hid), F32),
                pltpu.VMEM((cols, hid), F32),
                pltpu.VMEM((ocols, hid), F32),
            ),
            in_specs=[any_spec] * 12,
            out_specs=(vmem_spec,) * 5,
            scratch_shapes=[
                pltpu.VMEM((16, half, hid), BF16),
                pltpu.VMEM((16, half, hid), BF16),
                pltpu.VMEM((16, half, hid), BF16),
                pltpu.VMEM((8, half, hid), BF16),
                pltpu.VMEM((2, half, hid), BF16),
                pltpu.VMEM((4, 2, quarter, hid), BF16),
                pltpu.VMEM((16, 2 * cols, half), BF16),
                pltpu.VMEM((3 * cols + ocols, hid), BF16),
                pltpu.VMEM((2, 2, cols, half), BF16),
                pltpu.VMEM((32, ocols, quarter), BF16),
                pltpu.VMEM((2, rows, hid), BF16),
                pltpu.VMEM((hid,), BF16),
                dma((6,)),
                dma((13,)), dma((8,)), dma((2 * PIECES,)), dma((4,)), dma, dma, dma((2,)), dma, dma, dma, dma,
            ],
            compiler_params=pltpu.CompilerParams(
                collective_id=0, has_side_effects=True, vmem_limit_bytes=54_000_000),
            name="layer_backward",
        )(x_norm, grad_y, u_gate.T, u_up.T, w_gate.T, w_up.T, w_down, x_in, gamma, grad_res, attn_out.T,
          w_out)
        results = [pltpu.with_memory_space_constraint(r, pltpu.VMEM) for r in results]
        ds, do, dwg, dwu, dwd, dwo = pl.pallas_call(
            write_kernel,
            out_shape=(
                jax.ShapeDtypeStruct((rows, hid), BF16),
                jax.ShapeDtypeStruct((ocols, tokens), BF16),
                jax.ShapeDtypeStruct((cols, hid), F32),
                jax.ShapeDtypeStruct((cols, hid), F32),
                jax.ShapeDtypeStruct((cols, hid), F32),
                jax.ShapeDtypeStruct((ocols, hid), F32),
            ),
            in_specs=[vmem_spec] * 5,
            out_specs=(any_spec,) * 6,
            scratch_shapes=[dma],
            compiler_params=pltpu.CompilerParams(vmem_limit_bytes=1_000_000),
            name="write_results",
        )(*results)
        return ds, do.T, dwg.T, dwu.T, dwd, dwo

    return jax.shard_map(
        local_backward,
        mesh=mesh,
        in_specs=(token_spec, token_spec, split_cols, split_cols, weight_cols, weight_cols, weight_rows,
                  token_spec, P(None), token_spec, split_cols, weight_rows),
        out_specs=(token_spec, split_cols, split_cols, split_cols, token_spec, token_spec),
        check_vma=False,
    )
```

```python
import functools

import jax
import jax.numpy as jnp
from jax import lax
from jax.experimental import pallas as pl
from jax.experimental.pallas import tpu as pltpu
from jax.sharding import PartitionSpec as P

NORM_EPS = 1e-5
F32 = jnp.float32
BF16 = jnp.bfloat16
ROWS_ROWS = (((0,), (0,)), ((), ()))
COLS_COLS = (((1,), (1,)), ((), ()))
COLS_ROWS = (((1,), (0,)), ((), ()))
MESH = pl.DeviceIdType.MESH
PIECES = 4


def dot(a, b, dims):
    return lax.dot_general(a, b, dims, preferred_element_type=F32)


def slot_token(tp, half, k):
    me = lax.axis_index("tp")
    g, b, i = k // 4, lax.rem(k, 4) // 2, lax.rem(k, 2)
    dx = jnp.where(g == 0, 0, jnp.where(g == 3, 2, 2 * i - 1))
    h = jnp.where(g == 2, 1 - i, i)
    chip = lax.rem(me // 2 + dx + tp // 2, tp // 2)
    shard = 2 * chip + lax.rem(lax.rem(me, 2) + b, 2)
    return pl.multiple_of((2 * shard + h) * half, half)


def write_kernel(tp, half, dso, dob, dwgu, dwd, dwo, late, o_hbm, wo_hbm, ds_out, do_out, dwg_out, dwu_out, dwd_out, dwo_out,
                 ob, wo, dob_late, dwo_all, l_in, sem):
    cols, quarter = dwd.shape[0], half // 2
    first = slot_token(tp, half, 14)

    def tokens(n):
        return pl.ds(pl.multiple_of(first + n * quarter, quarter), quarter)

    def shard(n):
        rows = pl.ds(pl.multiple_of(lax.rem(first + n * 2 * half, tp * 2 * half), 2 * half), 2 * half)
        return dob.at[:, rows], do_out.at[:, rows]

    loads = [pltpu.make_async_copy(wo_hbm, wo, l_in)] + [
        pltpu.make_async_copy(o_hbm.at[:, tokens(2 * d + 1)], ob.at[d], l_in) for d in range(2)]
    for c in loads:
        c.start()
    copies = [pltpu.make_async_copy(src, dst, sem) for src, dst in (
        (dwgu.at[pl.ds(0, cols)], dwg_out), (dwgu.at[pl.ds(cols, cols)], dwu_out), (dwd, dwd_out), (dso, ds_out),
        *(shard(n) for n in range(1, tp)), *((dob.at[:, tokens(n)], do_out.at[:, tokens(n)]) for n in (0, 2)))]
    for c in copies:
        c.start()
    for c in loads:
        c.wait()
    total = dwo[...]
    for d in range(2):
        dob_late[d] = dot(wo[...], late[d], COLS_COLS).astype(BF16)
        total = total + dot(ob[d], late[d], COLS_ROWS)
    dwo_all[...] = total
    last = [pltpu.make_async_copy(dwo_all, dwo_out, sem)] + [
        pltpu.make_async_copy(dob_late.at[d], do_out.at[:, tokens(2 * d + 1)], sem) for d in range(2)]
    for c in last:
        c.start()
    for c in copies + last:
        c.wait()


def kernel(tp, x_hbm, gy_hbm, ug_hbm, uu_hbm, wg_hbm, wu_hbm, wd_hbm, xin_hbm, gamma_hbm, gr_hbm, o_hbm, wo_hbm,
           dso, dob, dwgu, dwd, dwo, late,
           gy, xb, part, peer, hop, frm, du, weights, ub, ob, tok, gamma_ref,
           sent, r_gy, r_x, r_e, r_t, r_p, r_h, l_u, l_w):
    half = gy.shape[1]
    cols, ocols = dwd.shape[0], dwo.shape[0]
    wgu = weights.at[pl.ds(0, 2 * cols)]
    wd = weights.at[pl.ds(2 * cols, cols)]
    wo = weights.at[pl.ds(3 * cols, ocols)]
    s_gy, s_x, s_p = (sent.at[i] for i in range(3))
    s_h = s_t = s_gy
    s_ds = s_x
    quarter = half // 2
    me = lax.axis_index("tp")
    right = lax.rem(me + 2, tp)
    left = lax.rem(me + tp - 2, tp)
    partner = me + 1 - 2 * lax.rem(me, 2)
    slot_row = functools.partial(slot_token, tp, half)

    def send(src, dst, ssem, rsem, dev):
        return pltpu.make_async_remote_copy(
            src_ref=src, dst_ref=dst, send_sem=ssem, recv_sem=rsem, device_id={"tp": dev}, device_id_type=MESH)

    def u_copies(k):
        tokens = pl.ds(slot_row(k), half)
        at = lax.rem(k, 2)
        return (pltpu.make_async_copy(ug_hbm.at[:, tokens], ub.at[at, 0], l_u.at[at]),
                pltpu.make_async_copy(uu_hbm.at[:, tokens], ub.at[at, 1], l_u.at[at]))

    def o_copy(n):
        tokens = pl.ds(pl.multiple_of(slot_row(n // 2) + lax.rem(n, 2) * quarter, quarter), quarter)
        return pltpu.make_async_copy(o_hbm.at[:, tokens], ob.at[n], l_w)

    def own(hbm, h):
        return hbm.at[pl.ds(h * half, half)]

    barrier = pltpu.get_barrier_semaphore()
    for dev in (left, right, partner):
        pl.semaphore_signal(barrier, inc=1, device_id={"tp": dev}, device_id_type=MESH)
    pl.semaphore_wait(barrier, 3)

    def send_own(hbm, buf, ssem, rsem):
        for src, dst, dev in ((0, 4, right), (1, 5, left), (1, 8, right), (0, 9, left), (0, 2, partner), (1, 3, partner)):
            send(own(hbm, src), buf.at[dst], ssem, rsem.at[dst // 2], dev).start()

    def arrived(ref, rsem):
        pltpu.make_async_copy(ref, ref, rsem).wait()

    def left_here(ref, ssem):
        send(ref, ref, ssem, ssem, partner).wait_send()

    def gather_step(buf, ssem, rsem, k, also):
        place = lax.rem(k, 4)

        @pl.when((k >= 2) & (lax.rem(place, 2) == 0))
        def _():
            arrived(buf.at[pl.ds(k, 2)], rsem.at[k // 2])

        @pl.when(k == 4)
        def _():
            send(buf.at[4], buf.at[12], ssem, rsem.at[6], right).start()
            send(buf.at[5], buf.at[13], ssem, rsem.at[6], left).start()

        @pl.when((k >= 4) & (place == 0))
        def _():
            for d in range(2):
                send(buf.at[k + d], buf.at[k + 2 + d], ssem, rsem.at[k // 2 + 1], partner).start()
            if also is not None:
                pl.when(k == 4)(also)

    send_own(gy_hbm, gy, s_gy, r_gy)
    for h in range(2):
        pltpu.make_async_copy(own(gy_hbm, h), gy.at[h], r_gy.at[0]).start()
        pltpu.make_async_copy(own(x_hbm, h), xb.at[h], r_x.at[0]).start()
    for i, src in enumerate((wg_hbm, wu_hbm, wd_hbm, wo_hbm)):
        pltpu.make_async_copy(src, weights.at[pl.ds(i * cols, src.shape[0])], l_w).start()
    for c in u_copies(0):
        c.start()
    dwd[...] = jnp.zeros_like(dwd)
    dwgu[...] = jnp.zeros_like(dwgu)
    dwo[...] = jnp.zeros_like(dwo)
    arrived(weights, l_w)
    arrived(gy.at[pl.ds(0, 2)], r_gy.at[0])
    arrived(xb.at[pl.ds(0, 2)], r_x.at[0])

    pltpu.make_async_copy(xin_hbm, tok.at[0], r_gy.at[0]).start()
    pltpu.make_async_copy(gr_hbm, tok.at[1], r_gy.at[0]).start()
    pltpu.make_async_copy(gamma_hbm, gamma_ref, r_x.at[0]).start()

    @pl.loop(0, 32)
    def _(n):
        o_copy(n).start()

    def part_copy(k):
        j = (k // 4) * 2 + lax.rem(k, 2)
        return send(part.at[k], peer.at[j], s_p, r_p, partner)

    @pl.loop(0, 16)
    def _(k):
        @pl.when(k + 1 < 16)
        def _():
            for c in u_copies(k + 1):
                c.start()

        @pl.when((k > 0) & (lax.rem(k + 3, 4) >= 2))
        def _():
            part_copy(k - 1).start()

        gather_step(gy, s_gy, r_gy, k, lambda: send_own(x_hbm, xb, s_x, r_x))
        at = lax.rem(k, 2)
        arrived(ub.at[at], l_u.at[at])
        gyk = gy[k]
        gh = dot(wd[...], gyk, COLS_COLS)
        gate = ub[at, 0].astype(F32)
        up = ub[at, 1].astype(F32)
        sig = jax.nn.sigmoid(gate)
        act = gate * sig
        silu = sig * (1.0 + gate * (1.0 - sig))
        z = (act * up).astype(BF16)
        du_up = (gh * act).astype(BF16)
        du_gate = (gh * up * silu).astype(BF16)
        du[k, pl.ds(0, cols)] = du_gate
        du[k, pl.ds(cols, cols)] = du_up
        dwd[...] += dot(z, gyk, COLS_ROWS)
        part[k] = dot(du[k], wgu[...], ROWS_ROWS).astype(BF16)

    part_copy(15).start()

    left_here(gy.at[pl.ds(0, 14)], s_gy)

    def add_peer(k, more=()):
        j = (k // 4) * 2 + k % 2
        t = part[k].astype(F32) + peer[j].astype(F32)
        for m in more:
            t = t + m[...].astype(F32)
        part[k] = t.astype(BF16)

    def q(ref, i):
        return ref.at[pl.ds(i * quarter, quarter)]

    arrived(peer, r_p)

    def hop_copy(k, i):
        side = k - 12
        return send(q(part.at[k], i), q(hop.at[side], i), s_h, r_h, (right, left)[side])

    for k in (12, 13):
        add_peer(k)
    for i in range(2):
        for k in (12, 13):
            hop_copy(k, i).start()

    def dw_step(j):
        xk = xb[pl.ds(2 * j, 2)].reshape(2 * half, xb.shape[2])
        duk = jnp.concatenate((du[2 * j], du[2 * j + 1]), axis=1)
        dwgu[...] += dot(duk, xk, COLS_ROWS)

    def tail_copy(side, qi):
        k = ((9, 5), (4, 8))[side][qi // 2]
        return send(q(part.at[k], qi % 2), frm.at[qi % 2, qi // 2, side], s_t, r_t.at[qi % 2], (right, left)[side])

    tail_order = ((2, 0, 3, 1), (0, 2, 1, 3))

    def tails():
        add_peer(5)
        add_peer(4)
        arrived(hop, r_h)
        add_peer(9, (hop.at[0],))
        add_peer(8, (hop.at[1],))
        for n in range(4):
            for side in range(2):
                tail_copy(side, tail_order[side][n]).start()

    @pl.loop(0, 8)
    def _(j):
        pl.when(j == 6)(tails)
        gather_step(xb, s_x, r_x, 2 * j, None)
        dw_step(j)

    ds = gy
    arrived(tok, r_gy.at[0])
    arrived(gamma_ref, r_x.at[0])
    left_here(xb.at[pl.ds(0, 14)], s_x)
    left_here(peer, s_p)
    gamma = gamma_ref[...].astype(F32).reshape(1, gamma_ref.shape[0])

    def norm_quarter(qi):
        h, i = qi // 2, qi % 2
        step = 32

        @pl.loop(0, quarter // step)
        def _(n):
            rows = pl.ds(pl.multiple_of(n * step, step), step)
            inner = pl.ds(pl.multiple_of(i * quarter + n * step, step), step)
            tokens = pl.ds(pl.multiple_of(qi * quarter + n * step, step), step)
            dx = (part[h, inner].astype(F32) + peer[h, inner].astype(F32)
                  + frm[i, h, 0, rows].astype(F32) + frm[i, h, 1, rows].astype(F32)).astype(BF16)
            xf = tok[0, tokens].astype(F32)
            inv = lax.rsqrt(jnp.mean(xf * xf, axis=-1, keepdims=True) + NORM_EPS)
            scaled = dx.astype(F32) * gamma
            proj = jnp.mean(scaled * xf, axis=-1, keepdims=True)
            out = (tok[1, tokens].astype(F32) + inv * (scaled - xf * (inv * inv) * proj)).astype(BF16)
            ds[h, inner] = out
            dso[tokens] = out

    def ds_copy(src, dst, i, dev):
        return send(q(ds.at[src], i), q(ds.at[dst], i), s_ds, r_gy.at[dst // 2 + 7 * i], dev)

    for i in range(2):
        arrived(frm.at[i], r_t.at[i])
        for h in (0, 1):
            norm_quarter(2 * h + i)
        for src, dst, dev in ((0, 4, right), (1, 5, left), (1, 8, right), (0, 9, left), (0, 2, partner), (1, 3, partner)):
            ds_copy(src, dst, i, dev).start()

    arrived(ob, l_w)
    left_here(part.at[pl.ds(0, 6)], s_t)

    def piece(e):
        return pl.ds(quarter + e * (quarter // PIECES), quarter // PIECES)

    def products(k, i):
        rows = pl.ds(pl.multiple_of(i * quarter, quarter), quarter)
        for d in range(2):
            block = ds[k + d, rows]
            n = 2 * (k + d) + i
            tokens = pl.ds(pl.multiple_of(slot_row(k + d) + i * quarter, quarter), quarter)
            dob[:, tokens] = dot(wo[...], block, COLS_COLS).astype(BF16)
            dwo[...] += dot(ob[n], block, COLS_ROWS)

    @pl.loop(0, 14)
    def _(u):
        v, w = u - 4, u - 12
        i = jnp.where(u < 4, lax.rem(u, 2), jnp.where(u < 12, v // 4, w // 2))
        k = jnp.where(u < 4, 2 * (u // 2), jnp.where(u < 12, 4 + 2 * lax.rem(v, 4), 12 + 2 * lax.rem(w, 2)))

        @pl.when(k > 0)
        def _():
            rows = pl.ds(pl.multiple_of(i * quarter, quarter), quarter)
            arrived(ds.at[pl.ds(k, 2), rows], r_gy.at[k // 2 + 7 * i])

        @pl.when((k == 4) & (i == 0))
        def _():
            for src, dst, dev in ((4, 12, right), (5, 13, left)):
                ds_copy(src, dst, 0, dev).start()

        @pl.when((k == 4) & (i == 1))
        def _():
            for e in range(PIECES):
                for src, dst, dev in ((4, 12, right), (5, 13, left)):
                    send(ds.at[src, piece(e)], ds.at[dst, piece(e)], s_ds, r_e.at[e], dev).start()

        @pl.when((k > 0) & (lax.rem(k, 4) == 0))
        def _():
            for d in range(2):
                ds_copy(k + d, k + 2 + d, i, partner).start()

        products(k, i)

    for e in range(PIECES):
        arrived(ds.at[pl.ds(12, 2), piece(e)], r_e.at[e])
        for d in range(2):
            to = late.at[d, pl.ds(e * (quarter // PIECES), quarter // PIECES)]
            send(ds.at[12 + d, piece(e)], to, s_ds, r_e.at[PIECES], partner).start()
    products(12, 1)
    left_here(ds.at[pl.ds(0, 14)], s_ds)
    arrived(late, r_e.at[PIECES])


def solution(mesh):
    tp = mesh.shape["tp"]
    token_spec = P(("dp", "tp"), None)
    split_cols = P("dp", "tp")
    weight_cols = P(None, "tp")
    weight_rows = P("tp", None)

    def local_backward(x_norm, grad_y, u_gate, u_up, w_gate, w_up, w_down, x_in, gamma, grad_res, attn_out, w_out):
        rows, hid = x_norm.shape
        tokens, cols = u_gate.shape
        ocols = attn_out.shape[1]
        half = rows // 2
        quarter = half // 2
        any_spec = pl.BlockSpec(memory_space=pl.ANY)
        vmem_spec = pl.BlockSpec(memory_space=pltpu.VMEM)
        dma = pltpu.SemaphoreType.DMA
        results = pl.pallas_call(
            functools.partial(kernel, tp),
            out_shape=(
                pltpu.VMEM((rows, hid), BF16),
                pltpu.VMEM((ocols, tokens), BF16),
                pltpu.VMEM((2 * cols, hid), F32),
                pltpu.VMEM((cols, hid), F32),
                pltpu.VMEM((ocols, hid), F32),
                pltpu.VMEM((2, quarter, hid), BF16),
            ),
            in_specs=[any_spec] * 12,
            out_specs=(vmem_spec,) * 6,
            scratch_shapes=[
                pltpu.VMEM((16, half, hid), BF16),
                pltpu.VMEM((16, half, hid), BF16),
                pltpu.VMEM((16, half, hid), BF16),
                pltpu.VMEM((8, half, hid), BF16),
                pltpu.VMEM((2, half, hid), BF16),
                pltpu.VMEM((2, 2, 2, quarter, hid), BF16),
                pltpu.VMEM((16, 2 * cols, half), BF16),
                pltpu.VMEM((3 * cols + ocols, hid), BF16),
                pltpu.VMEM((2, 2, cols, half), BF16),
                pltpu.VMEM((32, ocols, quarter), BF16),
                pltpu.VMEM((2, rows, hid), BF16),
                pltpu.VMEM((hid,), BF16),
                dma((3,)),
                dma((13,)), dma((8,)), dma((PIECES + 1,)), dma((2,)), dma, dma, dma((2,)), dma,
            ],
            compiler_params=pltpu.CompilerParams(
                collective_id=0, has_side_effects=True, vmem_limit_bytes=54_000_000),
            name="layer_backward",
        )(x_norm, grad_y, u_gate.T, u_up.T, w_gate.T, w_up.T, w_down, x_in, gamma, grad_res, attn_out.T,
          w_out)
        results = [pltpu.with_memory_space_constraint(r, pltpu.VMEM) for r in results]
        ds, do, dwg, dwu, dwd, dwo = pl.pallas_call(
            functools.partial(write_kernel, tp, half),
            out_shape=(
                jax.ShapeDtypeStruct((rows, hid), BF16),
                jax.ShapeDtypeStruct((ocols, tokens), BF16),
                jax.ShapeDtypeStruct((cols, hid), F32),
                jax.ShapeDtypeStruct((cols, hid), F32),
                jax.ShapeDtypeStruct((cols, hid), F32),
                jax.ShapeDtypeStruct((ocols, hid), F32),
            ),
            in_specs=[vmem_spec] * 6 + [pl.BlockSpec(memory_space=pltpu.HBM)] * 2,
            out_specs=(any_spec,) * 6,
            scratch_shapes=[
                pltpu.VMEM((2, ocols, quarter), BF16),
                pltpu.VMEM((ocols, hid), BF16),
                pltpu.VMEM((2, ocols, quarter), BF16),
                pltpu.VMEM((ocols, hid), F32),
                dma, dma,
            ],
            compiler_params=pltpu.CompilerParams(vmem_limit_bytes=4_000_000),
            name="write_results",
        )(*results, attn_out.T, w_out)
        return ds, do.T, dwg.T, dwu.T, dwd, dwo

    return jax.shard_map(
        local_backward,
        mesh=mesh,
        in_specs=(token_spec, token_spec, split_cols, split_cols, weight_cols, weight_cols, weight_rows,
                  token_spec, P(None), token_spec, split_cols, weight_rows),
        out_specs=(token_spec, split_cols, split_cols, split_cols, token_spec, token_spec),
        check_vma=False,
    )
```

```python
import functools

import jax
import jax.numpy as jnp
from jax import lax
from jax.experimental import pallas as pl
from jax.experimental.pallas import tpu as pltpu
from jax.sharding import PartitionSpec as P

NORM_EPS = 1e-5
F32 = jnp.float32
BF16 = jnp.bfloat16
ROWS_ROWS = (((0,), (0,)), ((), ()))
COLS_COLS = (((1,), (1,)), ((), ()))
COLS_ROWS = (((1,), (0,)), ((), ()))
MESH = pl.DeviceIdType.MESH
PIECES = 4


def dot(a, b, dims):
    return lax.dot_general(a, b, dims, preferred_element_type=F32)


def slot_token(tp, half, k):
    me = lax.axis_index("tp")
    g, b, i = k // 4, lax.rem(k, 4) // 2, lax.rem(k, 2)
    dx = jnp.where(g == 0, 0, jnp.where(g == 3, 2, 2 * i - 1))
    h = jnp.where(g == 2, 1 - i, i)
    chip = lax.rem(me // 2 + dx + tp // 2, tp // 2)
    shard = 2 * chip + lax.rem(lax.rem(me, 2) + b, 2)
    return pl.multiple_of((2 * shard + h) * half, half)


def write_kernel(tp, half, dso, dob, dwgu, dwd, dwo, late, ob, wo, ds_out, do_out, dwg_out, dwu_out, dwd_out, dwo_out,
                 dob_late, dwo_all, sem):
    cols, quarter = dwd.shape[0], half // 2
    first = slot_token(tp, half, 14)

    def tokens(n):
        return pl.ds(pl.multiple_of(first + n * quarter, quarter), quarter)

    def shard(n):
        rows = pl.ds(pl.multiple_of(lax.rem(first + n * 2 * half, tp * 2 * half), 2 * half), 2 * half)
        return dob.at[:, rows], do_out.at[:, rows]

    copies = [pltpu.make_async_copy(src, dst, sem) for src, dst in (
        (dwgu.at[pl.ds(0, cols)], dwg_out), (dwgu.at[pl.ds(cols, cols)], dwu_out), (dwd, dwd_out), (dso, ds_out),
        *(shard(n) for n in range(1, tp)), *((dob.at[:, tokens(n)], do_out.at[:, tokens(n)]) for n in (0, 2)))]
    for c in copies:
        c.start()
    total = dwo[...]
    for d in range(2):
        dob_late[d] = dot(wo[...], late[d], COLS_COLS).astype(BF16)
        total = total + dot(ob[:, tokens(2 * d + 1)], late[d], COLS_ROWS)
    dwo_all[...] = total
    last = [pltpu.make_async_copy(dwo_all, dwo_out, sem)] + [
        pltpu.make_async_copy(dob_late.at[d], do_out.at[:, tokens(2 * d + 1)], sem) for d in range(2)]
    for c in last:
        c.start()
    for c in copies + last:
        c.wait()


def kernel(tp, x_hbm, gy_hbm, ug_hbm, uu_hbm, wg_hbm, wu_hbm, wd_hbm, xin_hbm, gamma_hbm, gr_hbm, o_hbm, wo_hbm,
           dso, dob, dwgu, dwd, dwo, late,
           gy, xb, part, peer, hop, frm, du, weights, ub, ob, tok, gamma_ref,
           sent, r_gy, r_x, r_e, r_t, r_p, r_h, l_u, l_w):
    half = gy.shape[1]
    cols, ocols = dwd.shape[0], dwo.shape[0]
    wgu = weights.at[pl.ds(0, 2 * cols)]
    wd = weights.at[pl.ds(2 * cols, cols)]
    wo = weights.at[pl.ds(3 * cols, ocols)]
    s_gy, s_x, s_p = (sent.at[i] for i in range(3))
    s_h = s_t = s_gy
    s_ds = s_x
    quarter = half // 2
    me = lax.axis_index("tp")
    right = lax.rem(me + 2, tp)
    left = lax.rem(me + tp - 2, tp)
    partner = me + 1 - 2 * lax.rem(me, 2)
    slot_row = functools.partial(slot_token, tp, half)

    def send(src, dst, ssem, rsem, dev):
        return pltpu.make_async_remote_copy(
            src_ref=src, dst_ref=dst, send_sem=ssem, recv_sem=rsem, device_id={"tp": dev}, device_id_type=MESH)

    def u_copies(k):
        tokens = pl.ds(slot_row(k), half)
        at = lax.rem(k, 2)
        return (pltpu.make_async_copy(ug_hbm.at[:, tokens], ub.at[at, 0], l_u.at[at]),
                pltpu.make_async_copy(uu_hbm.at[:, tokens], ub.at[at, 1], l_u.at[at]))

    def o_copy(n):
        tokens = pl.ds(pl.multiple_of(slot_row(n // 2) + lax.rem(n, 2) * quarter, quarter), quarter)
        return pltpu.make_async_copy(o_hbm.at[:, tokens], ob.at[n], l_w)

    def own(hbm, h):
        return hbm.at[pl.ds(h * half, half)]

    barrier = pltpu.get_barrier_semaphore()
    for dev in (left, right, partner):
        pl.semaphore_signal(barrier, inc=1, device_id={"tp": dev}, device_id_type=MESH)
    pl.semaphore_wait(barrier, 3)

    def send_own(hbm, buf, ssem, rsem):
        for src, dst, dev in ((0, 4, right), (1, 5, left), (1, 8, right), (0, 9, left), (0, 2, partner), (1, 3, partner)):
            send(own(hbm, src), buf.at[dst], ssem, rsem.at[dst // 2], dev).start()

    def arrived(ref, rsem):
        pltpu.make_async_copy(ref, ref, rsem).wait()

    def left_here(ref, ssem):
        send(ref, ref, ssem, ssem, partner).wait_send()

    def gather_step(buf, ssem, rsem, k, also):
        place = lax.rem(k, 4)

        @pl.when((k >= 2) & (lax.rem(place, 2) == 0))
        def _():
            arrived(buf.at[pl.ds(k, 2)], rsem.at[k // 2])

        @pl.when(k == 4)
        def _():
            send(buf.at[4], buf.at[12], ssem, rsem.at[6], right).start()
            send(buf.at[5], buf.at[13], ssem, rsem.at[6], left).start()

        @pl.when((k >= 4) & (place == 0))
        def _():
            for d in range(2):
                send(buf.at[k + d], buf.at[k + 2 + d], ssem, rsem.at[k // 2 + 1], partner).start()
            if also is not None:
                pl.when(k == 4)(also)

    send_own(gy_hbm, gy, s_gy, r_gy)
    for h in range(2):
        pltpu.make_async_copy(own(gy_hbm, h), gy.at[h], r_gy.at[0]).start()
        pltpu.make_async_copy(own(x_hbm, h), xb.at[h], r_x.at[0]).start()
    for i, src in enumerate((wg_hbm, wu_hbm, wd_hbm, wo_hbm)):
        pltpu.make_async_copy(src, weights.at[pl.ds(i * cols, src.shape[0])], l_w).start()
    for c in u_copies(0):
        c.start()
    dwd[...] = jnp.zeros_like(dwd)
    dwgu[...] = jnp.zeros_like(dwgu)
    dwo[...] = jnp.zeros_like(dwo)
    arrived(weights, l_w)
    arrived(gy.at[pl.ds(0, 2)], r_gy.at[0])
    arrived(xb.at[pl.ds(0, 2)], r_x.at[0])

    pltpu.make_async_copy(xin_hbm, tok.at[0], r_gy.at[0]).start()
    pltpu.make_async_copy(gr_hbm, tok.at[1], r_gy.at[0]).start()
    pltpu.make_async_copy(gamma_hbm, gamma_ref, r_x.at[0]).start()

    @pl.loop(0, 32)
    def _(n):
        o_copy(n).start()

    def part_copy(k):
        j = (k // 4) * 2 + lax.rem(k, 2)
        return send(part.at[k], peer.at[j], s_p, r_p, partner)

    @pl.loop(0, 16)
    def _(k):
        @pl.when(k + 1 < 16)
        def _():
            for c in u_copies(k + 1):
                c.start()

        @pl.when((k > 0) & (lax.rem(k + 3, 4) >= 2))
        def _():
            part_copy(k - 1).start()

        gather_step(gy, s_gy, r_gy, k, lambda: send_own(x_hbm, xb, s_x, r_x))
        at = lax.rem(k, 2)
        arrived(ub.at[at], l_u.at[at])
        gyk = gy[k]
        gh = dot(wd[...], gyk, COLS_COLS)
        gate = ub[at, 0].astype(F32)
        up = ub[at, 1].astype(F32)
        sig = jax.nn.sigmoid(gate)
        act = gate * sig
        silu = sig * (1.0 + gate * (1.0 - sig))
        z = (act * up).astype(BF16)
        du_up = (gh * act).astype(BF16)
        du_gate = (gh * up * silu).astype(BF16)
        du[k, pl.ds(0, cols)] = du_gate
        du[k, pl.ds(cols, cols)] = du_up
        dwd[...] += dot(z, gyk, COLS_ROWS)
        part[k] = dot(du[k], wgu[...], ROWS_ROWS).astype(BF16)

    part_copy(15).start()

    left_here(gy.at[pl.ds(0, 14)], s_gy)

    def add_peer(k, more=()):
        j = (k // 4) * 2 + k % 2
        t = part[k].astype(F32) + peer[j].astype(F32)
        for m in more:
            t = t + m[...].astype(F32)
        part[k] = t.astype(BF16)

    def q(ref, i):
        return ref.at[pl.ds(i * quarter, quarter)]

    arrived(peer, r_p)

    def hop_copy(k, i):
        side = k - 12
        return send(q(part.at[k], i), q(hop.at[side], i), s_h, r_h, (right, left)[side])

    for k in (12, 13):
        add_peer(k)
    for i in range(2):
        for k in (12, 13):
            hop_copy(k, i).start()

    def dw_step(j):
        xk = xb[pl.ds(2 * j, 2)].reshape(2 * half, xb.shape[2])
        duk = jnp.concatenate((du[2 * j], du[2 * j + 1]), axis=1)
        dwgu[...] += dot(duk, xk, COLS_ROWS)

    def tail_copy(side, qi):
        k = ((9, 5), (4, 8))[side][qi // 2]
        return send(q(part.at[k], qi % 2), frm.at[qi % 2, qi // 2, side], s_t, r_t.at[qi % 2], (right, left)[side])

    tail_order = ((2, 0, 3, 1), (0, 2, 1, 3))

    def tails():
        add_peer(5)
        add_peer(4)
        arrived(hop, r_h)
        add_peer(9, (hop.at[0],))
        add_peer(8, (hop.at[1],))
        for n in range(4):
            for side in range(2):
                tail_copy(side, tail_order[side][n]).start()

    @pl.loop(0, 8)
    def _(j):
        pl.when(j == 6)(tails)
        gather_step(xb, s_x, r_x, 2 * j, None)
        dw_step(j)

    ds = gy
    arrived(tok, r_gy.at[0])
    arrived(gamma_ref, r_x.at[0])
    left_here(xb.at[pl.ds(0, 14)], s_x)
    left_here(peer, s_p)
    gamma = gamma_ref[...].astype(F32).reshape(1, gamma_ref.shape[0])

    def norm_quarter(qi):
        h, i = qi // 2, qi % 2
        step = 32

        @pl.loop(0, quarter // step)
        def _(n):
            rows = pl.ds(pl.multiple_of(n * step, step), step)
            inner = pl.ds(pl.multiple_of(i * quarter + n * step, step), step)
            tokens = pl.ds(pl.multiple_of(qi * quarter + n * step, step), step)
            dx = (part[h, inner].astype(F32) + peer[h, inner].astype(F32)
                  + frm[i, h, 0, rows].astype(F32) + frm[i, h, 1, rows].astype(F32)).astype(BF16)
            xf = tok[0, tokens].astype(F32)
            inv = lax.rsqrt(jnp.mean(xf * xf, axis=-1, keepdims=True) + NORM_EPS)
            scaled = dx.astype(F32) * gamma
            proj = jnp.mean(scaled * xf, axis=-1, keepdims=True)
            out = (tok[1, tokens].astype(F32) + inv * (scaled - xf * (inv * inv) * proj)).astype(BF16)
            ds[h, inner] = out
            dso[tokens] = out

    def ds_copy(src, dst, i, dev):
        return send(q(ds.at[src], i), q(ds.at[dst], i), s_ds, r_gy.at[dst // 2 + 7 * i], dev)

    for i in range(2):
        arrived(frm.at[i], r_t.at[i])
        for h in (0, 1):
            norm_quarter(2 * h + i)
        for src, dst, dev in ((0, 4, right), (1, 5, left), (1, 8, right), (0, 9, left), (0, 2, partner), (1, 3, partner)):
            ds_copy(src, dst, i, dev).start()

    arrived(ob, l_w)
    left_here(part.at[pl.ds(0, 6)], s_t)

    def piece(e):
        return pl.ds(quarter + e * (quarter // PIECES), quarter // PIECES)

    def products(k, i):
        rows = pl.ds(pl.multiple_of(i * quarter, quarter), quarter)
        for d in range(2):
            block = ds[k + d, rows]
            n = 2 * (k + d) + i
            tokens = pl.ds(pl.multiple_of(slot_row(k + d) + i * quarter, quarter), quarter)
            dob[:, tokens] = dot(wo[...], block, COLS_COLS).astype(BF16)
            dwo[...] += dot(ob[n], block, COLS_ROWS)

    @pl.loop(0, 14)
    def _(u):
        v, w = u - 4, u - 12
        i = jnp.where(u < 4, lax.rem(u, 2), jnp.where(u < 12, v // 4, w // 2))
        k = jnp.where(u < 4, 2 * (u // 2), jnp.where(u < 12, 4 + 2 * lax.rem(v, 4), 12 + 2 * lax.rem(w, 2)))

        @pl.when(k > 0)
        def _():
            rows = pl.ds(pl.multiple_of(i * quarter, quarter), quarter)
            arrived(ds.at[pl.ds(k, 2), rows], r_gy.at[k // 2 + 7 * i])

        @pl.when((k == 4) & (i == 0))
        def _():
            for src, dst, dev in ((4, 12, right), (5, 13, left)):
                ds_copy(src, dst, 0, dev).start()

        @pl.when((k == 4) & (i == 1))
        def _():
            for e in range(PIECES):
                for src, dst, dev in ((4, 12, right), (5, 13, left)):
                    send(ds.at[src, piece(e)], ds.at[dst, piece(e)], s_ds, r_e.at[e], dev).start()

        @pl.when((k > 0) & (lax.rem(k, 4) == 0))
        def _():
            for d in range(2):
                ds_copy(k + d, k + 2 + d, i, partner).start()

        products(k, i)

    for e in range(PIECES):
        arrived(ds.at[pl.ds(12, 2), piece(e)], r_e.at[e])
        for d in range(2):
            to = late.at[d, pl.ds(e * (quarter // PIECES), quarter // PIECES)]
            send(ds.at[12 + d, piece(e)], to, s_ds, r_e.at[PIECES], partner).start()
    products(12, 1)
    left_here(ds.at[pl.ds(0, 14)], s_ds)
    arrived(late, r_e.at[PIECES])


def solution(mesh):
    tp = mesh.shape["tp"]
    token_spec = P(("dp", "tp"), None)
    split_cols = P("dp", "tp")
    weight_cols = P(None, "tp")
    weight_rows = P("tp", None)

    def local_backward(x_norm, grad_y, u_gate, u_up, w_gate, w_up, w_down, x_in, gamma, grad_res, attn_out, w_out):
        rows, hid = x_norm.shape
        tokens, cols = u_gate.shape
        ocols = attn_out.shape[1]
        half = rows // 2
        quarter = half // 2
        any_spec = pl.BlockSpec(memory_space=pl.ANY)
        vmem_spec = pl.BlockSpec(memory_space=pltpu.VMEM)
        dma = pltpu.SemaphoreType.DMA
        results = pl.pallas_call(
            functools.partial(kernel, tp),
            out_shape=(
                pltpu.VMEM((rows, hid), BF16),
                pltpu.VMEM((ocols, tokens), BF16),
                pltpu.VMEM((2 * cols, hid), F32),
                pltpu.VMEM((cols, hid), F32),
                pltpu.VMEM((ocols, hid), F32),
                pltpu.VMEM((2, quarter, hid), BF16),
            ),
            in_specs=[any_spec] * 12,
            out_specs=(vmem_spec,) * 6,
            scratch_shapes=[
                pltpu.VMEM((16, half, hid), BF16),
                pltpu.VMEM((16, half, hid), BF16),
                pltpu.VMEM((16, half, hid), BF16),
                pltpu.VMEM((8, half, hid), BF16),
                pltpu.VMEM((2, half, hid), BF16),
                pltpu.VMEM((2, 2, 2, quarter, hid), BF16),
                pltpu.VMEM((16, 2 * cols, half), BF16),
                pltpu.VMEM((3 * cols + ocols, hid), BF16),
                pltpu.VMEM((2, 2, cols, half), BF16),
                pltpu.VMEM((32, ocols, quarter), BF16),
                pltpu.VMEM((2, rows, hid), BF16),
                pltpu.VMEM((hid,), BF16),
                dma((3,)),
                dma((13,)), dma((8,)), dma((PIECES + 1,)), dma((2,)), dma, dma, dma((2,)), dma,
            ],
            compiler_params=pltpu.CompilerParams(
                collective_id=0, has_side_effects=True, vmem_limit_bytes=54_000_000),
            name="layer_backward",
        )(x_norm, grad_y, u_gate.T, u_up.T, w_gate.T, w_up.T, w_down, x_in, gamma, grad_res, attn_out.T,
          w_out)
        results = [pltpu.with_memory_space_constraint(r, pltpu.VMEM) for r in (*results, attn_out.T, w_out)]
        ds, do, dwg, dwu, dwd, dwo = pl.pallas_call(
            functools.partial(write_kernel, tp, half),
            out_shape=(
                jax.ShapeDtypeStruct((rows, hid), BF16),
                jax.ShapeDtypeStruct((ocols, tokens), BF16),
                jax.ShapeDtypeStruct((cols, hid), F32),
                jax.ShapeDtypeStruct((cols, hid), F32),
                jax.ShapeDtypeStruct((cols, hid), F32),
                jax.ShapeDtypeStruct((ocols, hid), F32),
            ),
            in_specs=[vmem_spec] * 8,
            out_specs=(any_spec,) * 6,
            scratch_shapes=[
                pltpu.VMEM((2, ocols, quarter), BF16),
                pltpu.VMEM((ocols, hid), F32),
                dma,
            ],
            compiler_params=pltpu.CompilerParams(vmem_limit_bytes=4_000_000),
            name="write_results",
        )(*results)
        return ds, do.T, dwg.T, dwu.T, dwd, dwo

    return jax.shard_map(
        local_backward,
        mesh=mesh,
        in_specs=(token_spec, token_spec, split_cols, split_cols, weight_cols, weight_cols, weight_rows,
                  token_spec, P(None), token_spec, split_cols, weight_rows),
        out_specs=(token_spec, split_cols, split_cols, split_cols, token_spec, token_spec),
        check_vma=False,
    )
```

```python
import functools

import jax
import jax.numpy as jnp
from jax import lax
from jax.experimental import pallas as pl
from jax.experimental.pallas import tpu as pltpu
from jax.sharding import PartitionSpec as P

NORM_EPS = 1e-5
F32 = jnp.float32
BF16 = jnp.bfloat16
ROWS_ROWS = (((0,), (0,)), ((), ()))
COLS_COLS = (((1,), (1,)), ((), ()))
COLS_ROWS = (((1,), (0,)), ((), ()))
MESH = pl.DeviceIdType.MESH
LAST = 16


def dot(a, b, dims):
    return lax.dot_general(a, b, dims, preferred_element_type=F32)


def slot_token(tp, half, k):
    me = lax.axis_index("tp")
    g, b, i = k // 4, lax.rem(k, 4) // 2, lax.rem(k, 2)
    dx = jnp.where(g == 0, 0, jnp.where(g == 3, 2, 2 * i - 1))
    h = jnp.where(g == 2, 1 - i, i)
    chip = lax.rem(me // 2 + dx + tp // 2, tp // 2)
    shard = 2 * chip + lax.rem(lax.rem(me, 2) + b, 2)
    return pl.multiple_of((2 * shard + h) * half, half)


def write_kernel(tp, half, dso, dob, dwgu, dwd, dwo, late, ob, wo, ds_out, do_out, dwg_out, dwu_out, dwd_out, dwo_out,
                 dob_late, dwo_all, sem):
    cols, quarter = dwd.shape[0], half // 2
    first = slot_token(tp, half, 14)

    def tokens(n):
        return pl.ds(pl.multiple_of(first + n * quarter, quarter), quarter)

    def shard(n):
        rows = pl.ds(pl.multiple_of(lax.rem(first + n * 2 * half, tp * 2 * half), 2 * half), 2 * half)
        return dob.at[:, rows], do_out.at[:, rows]

    copies = [pltpu.make_async_copy(src, dst, sem) for src, dst in (
        *((src.at[pl.ds(at + r, cols // 4)], dst.at[pl.ds(r, cols // 4)])
          for src, at, dst in ((dwgu, 0, dwg_out), (dwgu, cols, dwu_out), (dwd, 0, dwd_out)) for r in range(0, cols, cols // 4)),
        (dso, ds_out), *(shard(n) for n in range(1, tp)), *((dob.at[:, tokens(n)], do_out.at[:, tokens(n)]) for n in (0, 2)))]
    for c in copies:
        c.start()
    total = dwo[...]
    for d in range(2):
        dob_late[d] = dot(wo[...], late[d], COLS_COLS).astype(BF16)
        total = total + dot(ob[:, tokens(2 * d + 1)], late[d], COLS_ROWS)
    dwo_all[...] = total
    last = [pltpu.make_async_copy(dwo_all, dwo_out, sem)] + [
        pltpu.make_async_copy(dob_late.at[d], do_out.at[:, tokens(2 * d + 1)], sem) for d in range(2)]
    for c in last:
        c.start()
    for c in copies + last:
        c.wait()


def kernel(tp, x_hbm, gy_hbm, ug_hbm, uu_hbm, wg_hbm, wu_hbm, wd_hbm, xin_hbm, gamma_hbm, gr_hbm, o_hbm, wo_hbm,
           dso, dob, dwgu, dwd, dwo, late,
           gy, xb, part, peer, hop, frm, du, weights, ub, ob, tok, gamma_ref,
           sent, r_gy, r_x, r_t, r_p, r_h, l_u, l_w):
    half = gy.shape[1]
    cols, ocols = dwd.shape[0], dwo.shape[0]
    wgu = weights.at[pl.ds(0, 2 * cols)]
    wd = weights.at[pl.ds(2 * cols, cols)]
    wo = weights.at[pl.ds(3 * cols, ocols)]
    s_gy, s_x, s_p = (sent.at[i] for i in range(3))
    s_h = s_t = s_gy
    s_ds = s_x
    quarter = half // 2
    me = lax.axis_index("tp")
    right = lax.rem(me + 2, tp)
    left = lax.rem(me + tp - 2, tp)
    partner = me + 1 - 2 * lax.rem(me, 2)
    slot_row = functools.partial(slot_token, tp, half)

    def send(src, dst, ssem, rsem, dev):
        return pltpu.make_async_remote_copy(
            src_ref=src, dst_ref=dst, send_sem=ssem, recv_sem=rsem, device_id={"tp": dev}, device_id_type=MESH)

    def u_copies(k):
        tokens = pl.ds(slot_row(k), half)
        at = lax.rem(k, 2)
        return (pltpu.make_async_copy(ug_hbm.at[:, tokens], ub.at[at, 0], l_u.at[at]),
                pltpu.make_async_copy(uu_hbm.at[:, tokens], ub.at[at, 1], l_u.at[at]))

    def o_copy(n):
        tokens = pl.ds(pl.multiple_of(slot_row(n // 2) + lax.rem(n, 2) * quarter, quarter), quarter)
        return pltpu.make_async_copy(o_hbm.at[:, tokens], ob.at[n], l_w)

    def own(hbm, h):
        return hbm.at[pl.ds(h * half, half)]

    barrier = pltpu.get_barrier_semaphore()
    for dev in (left, right, partner):
        pl.semaphore_signal(barrier, inc=1, device_id={"tp": dev}, device_id_type=MESH)
    pl.semaphore_wait(barrier, 3)

    def send_own(hbm, buf, ssem, rsem):
        for src, dst, dev in ((0, 4, right), (1, 5, left), (1, 8, right), (0, 9, left), (0, 2, partner), (1, 3, partner)):
            send(own(hbm, src), buf.at[dst], ssem, rsem.at[dst // 2], dev).start()

    def arrived(ref, rsem):
        pltpu.make_async_copy(ref, ref, rsem).wait()

    def left_here(ref, ssem):
        send(ref, ref, ssem, ssem, partner).wait_send()

    def gather_step(buf, ssem, rsem, k, also):
        place = lax.rem(k, 4)

        @pl.when((k >= 2) & (lax.rem(place, 2) == 0))
        def _():
            arrived(buf.at[pl.ds(k, 2)], rsem.at[k // 2])

        @pl.when(k == 4)
        def _():
            send(buf.at[4], buf.at[12], ssem, rsem.at[6], right).start()
            send(buf.at[5], buf.at[13], ssem, rsem.at[6], left).start()

        @pl.when((k >= 4) & (place == 0))
        def _():
            for d in range(2):
                send(buf.at[k + d], buf.at[k + 2 + d], ssem, rsem.at[k // 2 + 1], partner).start()
            if also is not None:
                pl.when(k == 4)(also)

    send_own(gy_hbm, gy, s_gy, r_gy)
    for h in range(2):
        pltpu.make_async_copy(own(gy_hbm, h), gy.at[h], r_gy.at[0]).start()
        pltpu.make_async_copy(own(x_hbm, h), xb.at[h], r_x.at[0]).start()
    for i, src in enumerate((wg_hbm, wu_hbm, wd_hbm, wo_hbm)):
        pltpu.make_async_copy(src, weights.at[pl.ds(i * cols, src.shape[0])], l_w).start()
    for c in u_copies(0):
        c.start()
    dwd[...] = jnp.zeros_like(dwd)
    dwgu[...] = jnp.zeros_like(dwgu)
    dwo[...] = jnp.zeros_like(dwo)
    arrived(weights, l_w)
    arrived(gy.at[pl.ds(0, 2)], r_gy.at[0])
    arrived(xb.at[pl.ds(0, 2)], r_x.at[0])

    pltpu.make_async_copy(xin_hbm, tok.at[0], r_gy.at[0]).start()
    pltpu.make_async_copy(gr_hbm, tok.at[1], r_gy.at[0]).start()
    pltpu.make_async_copy(gamma_hbm, gamma_ref, r_x.at[0]).start()

    @pl.loop(0, 32)
    def _(n):
        o_copy(n).start()

    def part_copy(k):
        j = (k // 4) * 2 + lax.rem(k, 2)
        return send(part.at[k], peer.at[j], s_p, r_p, partner)

    @pl.loop(0, 16)
    def _(k):
        @pl.when(k + 1 < 16)
        def _():
            for c in u_copies(k + 1):
                c.start()

        @pl.when((k > 0) & (lax.rem(k + 3, 4) >= 2))
        def _():
            part_copy(k - 1).start()

        gather_step(gy, s_gy, r_gy, k, lambda: send_own(x_hbm, xb, s_x, r_x))
        at = lax.rem(k, 2)
        arrived(ub.at[at], l_u.at[at])
        gyk = gy[k]
        gh = dot(wd[...], gyk, COLS_COLS)
        gate = ub[at, 0].astype(F32)
        up = ub[at, 1].astype(F32)
        sig = jax.nn.sigmoid(gate)
        act = gate * sig
        silu = sig * (1.0 + gate * (1.0 - sig))
        z = (act * up).astype(BF16)
        du_up = (gh * act).astype(BF16)
        du_gate = (gh * up * silu).astype(BF16)
        du[k, pl.ds(0, cols)] = du_gate
        du[k, pl.ds(cols, cols)] = du_up
        dwd[...] += dot(z, gyk, COLS_ROWS)
        part[k] = dot(du[k], wgu[...], ROWS_ROWS).astype(BF16)

    part_copy(15).start()

    left_here(gy.at[pl.ds(0, 14)], s_gy)

    def add_peer(k, more=()):
        j = (k // 4) * 2 + k % 2
        t = part[k].astype(F32) + peer[j].astype(F32)
        for m in more:
            t = t + m[...].astype(F32)
        part[k] = t.astype(BF16)

    def q(ref, i):
        return ref.at[pl.ds(i * quarter, quarter)]

    arrived(peer, r_p)

    for k in (12, 13):
        add_peer(k)
    for side, dev in enumerate((right, left)):
        send(part.at[12 + side], hop.at[side], s_h, r_h, dev).start()

    def dw_step(j):
        xk = xb[pl.ds(2 * j, 2)].reshape(2 * half, xb.shape[2])
        duk = jnp.concatenate((du[2 * j], du[2 * j + 1]), axis=1)
        dwgu[...] += dot(duk, xk, COLS_ROWS)

    def tail_copy(side, qi):
        k = ((9, 5), (4, 8))[side][qi // 2]
        return send(q(part.at[k], qi % 2), frm.at[qi % 2, qi // 2, side], s_t, r_t.at[qi % 2], (right, left)[side])

    tail_order = ((2, 0, 3, 1), (0, 2, 1, 3))

    def tails():
        add_peer(5)
        add_peer(4)
        arrived(hop, r_h)
        add_peer(9, (hop.at[0],))
        add_peer(8, (hop.at[1],))
        for n in range(4):
            for side in range(2):
                tail_copy(side, tail_order[side][n]).start()

    @pl.loop(0, 8)
    def _(j):
        pl.when(j == 6)(tails)
        gather_step(xb, s_x, r_x, 2 * j, None)
        dw_step(j)

    ds = gy
    arrived(tok, r_gy.at[0])
    arrived(gamma_ref, r_x.at[0])
    left_here(xb.at[pl.ds(0, 14)], s_x)
    left_here(peer, s_p)
    gamma = gamma_ref[...].astype(F32).reshape(1, gamma_ref.shape[0])

    def norm_quarter(qi):
        h, i = qi // 2, qi % 2
        step = 32

        @pl.loop(0, quarter // step)
        def _(n):
            rows = pl.ds(pl.multiple_of(n * step, step), step)
            inner = pl.ds(pl.multiple_of(i * quarter + n * step, step), step)
            tokens = pl.ds(pl.multiple_of(qi * quarter + n * step, step), step)
            dx = (part[h, inner].astype(F32) + peer[h, inner].astype(F32)
                  + frm[i, h, 0, rows].astype(F32) + frm[i, h, 1, rows].astype(F32)).astype(BF16)
            xf = tok[0, tokens].astype(F32)
            inv = lax.rsqrt(jnp.mean(xf * xf, axis=-1, keepdims=True) + NORM_EPS)
            scaled = dx.astype(F32) * gamma
            proj = jnp.mean(scaled * xf, axis=-1, keepdims=True)
            out = (tok[1, tokens].astype(F32) + inv * (scaled - xf * (inv * inv) * proj)).astype(BF16)
            ds[h, inner] = out
            dso[tokens] = out

    def ds_copy(src, dst, i, dev):
        return send(q(ds.at[src], i), q(ds.at[dst], i), s_ds, r_gy.at[dst // 2 + 7 * i], dev)

    for i in range(2):
        arrived(frm.at[i], r_t.at[i])
        for h in (0, 1):
            norm_quarter(2 * h + i)
        for src, dst, dev in ((0, 4, right), (1, 5, left), (1, 8, right), (0, 9, left), (0, 2, partner), (1, 3, partner)):
            ds_copy(src, dst, i, dev).start()

    arrived(ob, l_w)
    left_here(part.at[pl.ds(0, 6)], s_t)

    pieces = ((0, quarter - LAST), (quarter - LAST, LAST))
    r_e, r_late = (r_x.at[1], r_x.at[2]), r_x.at[3]

    def products(k, i):
        rows = pl.ds(pl.multiple_of(i * quarter, quarter), quarter)
        for d in range(2):
            block = ds[k + d, rows]
            n = 2 * (k + d) + i
            tokens = pl.ds(pl.multiple_of(slot_row(k + d) + i * quarter, quarter), quarter)
            dob[:, tokens] = dot(wo[...], block, COLS_COLS).astype(BF16)
            dwo[...] += dot(ob[n], block, COLS_ROWS)

    @pl.loop(0, 14)
    def _(u):
        v, w = u - 4, u - 12
        i = jnp.where(u < 4, lax.rem(u, 2), jnp.where(u < 12, v // 4, w // 2))
        k = jnp.where(u < 4, 2 * (u // 2), jnp.where(u < 12, 4 + 2 * lax.rem(v, 4), 12 + 2 * lax.rem(w, 2)))

        @pl.when(k > 0)
        def _():
            rows = pl.ds(pl.multiple_of(i * quarter, quarter), quarter)
            arrived(ds.at[pl.ds(k, 2), rows], r_gy.at[k // 2 + 7 * i])

        @pl.when((k == 4) & (i == 0))
        def _():
            for src, dst, dev in ((4, 12, right), (5, 13, left)):
                ds_copy(src, dst, 0, dev).start()

        @pl.when((k == 4) & (i == 1))
        def _():
            for (lo, n), rsem in zip(pieces, r_e):
                rows = pl.ds(quarter + lo, n)
                for src, dst, dev in ((4, 12, right), (5, 13, left)):
                    send(ds.at[src, rows], ds.at[dst, rows], s_ds, rsem, dev).start()

        @pl.when((k > 0) & (lax.rem(k, 4) == 0))
        def _():
            for d in range(2):
                ds_copy(k + d, k + 2 + d, i, partner).start()

        products(k, i)

    for (lo, n), rsem in zip(pieces, r_e):
        rows = pl.ds(quarter + lo, n)
        arrived(ds.at[pl.ds(12, 2), rows], rsem)
        for d in range(2):
            send(ds.at[12 + d, rows], late.at[d, pl.ds(lo, n)], s_ds, r_late, partner).start()
    products(12, 1)
    left_here(ds.at[pl.ds(0, 14)], s_ds)
    arrived(late, r_late)


def solution(mesh):
    tp = mesh.shape["tp"]
    token_spec = P(("dp", "tp"), None)
    split_cols = P("dp", "tp")
    weight_cols = P(None, "tp")
    weight_rows = P("tp", None)

    def local_backward(x_norm, grad_y, u_gate, u_up, w_gate, w_up, w_down, x_in, gamma, grad_res, attn_out, w_out):
        rows, hid = x_norm.shape
        tokens, cols = u_gate.shape
        ocols = attn_out.shape[1]
        half = rows // 2
        quarter = half // 2
        any_spec = pl.BlockSpec(memory_space=pl.ANY)
        vmem_spec = pl.BlockSpec(memory_space=pltpu.VMEM)
        dma = pltpu.SemaphoreType.DMA
        results = pl.pallas_call(
            functools.partial(kernel, tp),
            out_shape=(
                pltpu.VMEM((rows, hid), BF16),
                pltpu.VMEM((ocols, tokens), BF16),
                pltpu.VMEM((2 * cols, hid), F32),
                pltpu.VMEM((cols, hid), F32),
                pltpu.VMEM((ocols, hid), F32),
                pltpu.VMEM((2, quarter, hid), BF16),
            ),
            in_specs=[any_spec] * 12,
            out_specs=(vmem_spec,) * 6,
            scratch_shapes=[
                pltpu.VMEM((16, half, hid), BF16),
                pltpu.VMEM((16, half, hid), BF16),
                pltpu.VMEM((16, half, hid), BF16),
                pltpu.VMEM((8, half, hid), BF16),
                pltpu.VMEM((2, half, hid), BF16),
                pltpu.VMEM((2, 2, 2, quarter, hid), BF16),
                pltpu.VMEM((16, 2 * cols, half), BF16),
                pltpu.VMEM((3 * cols + ocols, hid), BF16),
                pltpu.VMEM((2, 2, cols, half), BF16),
                pltpu.VMEM((32, ocols, quarter), BF16),
                pltpu.VMEM((2, rows, hid), BF16),
                pltpu.VMEM((hid,), BF16),
                dma((3,)),
                dma((13,)), dma((8,)), dma((2,)), dma, dma, dma((2,)), dma,
            ],
            compiler_params=pltpu.CompilerParams(
                collective_id=0, has_side_effects=True, vmem_limit_bytes=54_000_000),
            name="layer_backward",
        )(x_norm, grad_y, u_gate.T, u_up.T, w_gate.T, w_up.T, w_down, x_in, gamma, grad_res, attn_out.T,
          w_out)
        results = [pltpu.with_memory_space_constraint(r, pltpu.VMEM) for r in (*results, attn_out.T, w_out)]
        ds, do, dwg, dwu, dwd, dwo = pl.pallas_call(
            functools.partial(write_kernel, tp, half),
            out_shape=(
                jax.ShapeDtypeStruct((rows, hid), BF16),
                jax.ShapeDtypeStruct((ocols, tokens), BF16),
                jax.ShapeDtypeStruct((cols, hid), F32),
                jax.ShapeDtypeStruct((cols, hid), F32),
                jax.ShapeDtypeStruct((cols, hid), F32),
                jax.ShapeDtypeStruct((ocols, hid), F32),
            ),
            in_specs=[vmem_spec] * 8,
            out_specs=(any_spec,) * 6,
            scratch_shapes=[
                pltpu.VMEM((2, ocols, quarter), BF16),
                pltpu.VMEM((ocols, hid), F32),
                dma,
            ],
            compiler_params=pltpu.CompilerParams(vmem_limit_bytes=4_000_000),
            name="write_results",
        )(*results)
        return ds, do.T, dwg.T, dwu.T, dwd, dwo

    return jax.shard_map(
        local_backward,
        mesh=mesh,
        in_specs=(token_spec, token_spec, split_cols, split_cols, weight_cols, weight_cols, weight_rows,
                  token_spec, P(None), token_spec, split_cols, weight_rows),
        out_specs=(token_spec, split_cols, split_cols, split_cols, token_spec, token_spec),
        check_vma=False,
    )
```

```python
import functools

import jax
import jax.numpy as jnp
from jax import lax
from jax.experimental import pallas as pl
from jax.experimental.pallas import tpu as pltpu
from jax.sharding import PartitionSpec as P

NORM_EPS = 1e-5
F32 = jnp.float32
BF16 = jnp.bfloat16
ROWS_ROWS = (((0,), (0,)), ((), ()))
COLS_COLS = (((1,), (1,)), ((), ()))
COLS_ROWS = (((1,), (0,)), ((), ()))
MESH = pl.DeviceIdType.MESH


def dot(a, b, dims):
    return lax.dot_general(a, b, dims, preferred_element_type=F32)


def slot_token(tp, half, k):
    me = lax.axis_index("tp")
    g, b, i = k // 4, lax.rem(k, 4) // 2, lax.rem(k, 2)
    dx = jnp.where(g == 0, 0, jnp.where(g == 3, 2, 2 * i - 1))
    h = jnp.where(g == 2, 1 - i, i)
    chip = lax.rem(me // 2 + dx + tp // 2, tp // 2)
    shard = 2 * chip + lax.rem(lax.rem(me, 2) + b, 2)
    return pl.multiple_of((2 * shard + h) * half, half)


def write_kernel(tp, half, dso, dob, dwgu, dwd, dwo, late, ob, wo, ds_out, do_out, dwg_out, dwu_out, dwd_out, dwo_out,
                 dob_late, dwo_all, sem):
    cols, quarter = dwd.shape[0], half // 2
    first = slot_token(tp, half, 14)

    def tokens(n):
        return pl.ds(pl.multiple_of(first + n * quarter, quarter), quarter)

    def shard(n):
        rows = pl.ds(pl.multiple_of(lax.rem(first + n * 2 * half, tp * 2 * half), 2 * half), 2 * half)
        return dob.at[:, rows], do_out.at[:, rows]

    copies = [pltpu.make_async_copy(src, dst, sem) for src, dst in (
        *((src.at[pl.ds(at + r, cols // 4)], dst.at[pl.ds(r, cols // 4)])
          for src, at, dst in ((dwgu, 0, dwg_out), (dwgu, cols, dwu_out), (dwd, 0, dwd_out)) for r in range(0, cols, cols // 4)),
        (dso, ds_out), *(shard(n) for n in range(1, tp)), *((dob.at[:, tokens(n)], do_out.at[:, tokens(n)]) for n in (0, 2)))]
    for c in copies:
        c.start()
    total = dwo[...]
    for d in range(2):
        dob_late[d] = dot(wo[...], late[d], COLS_COLS).astype(BF16)
        total = total + dot(ob[:, tokens(2 * d + 1)], late[d], COLS_ROWS)
    dwo_all[...] = total
    last = [pltpu.make_async_copy(dwo_all, dwo_out, sem)] + [
        pltpu.make_async_copy(dob_late.at[d], do_out.at[:, tokens(2 * d + 1)], sem) for d in range(2)]
    for c in last:
        c.start()
    for c in copies + last:
        c.wait()


def kernel(tp, x_hbm, gy_hbm, ug_hbm, uu_hbm, wg_hbm, wu_hbm, wd_hbm, xin_hbm, gamma_hbm, gr_hbm, o_hbm, wo_hbm,
           dso, dob, dwgu, dwd, dwo, late,
           gy, xb, part, peer, hop, frm, du, weights, ub, ob, tok, gamma_ref,
           sent, r_gy, r_x, r_t, r_p, r_h, l_u, l_w):
    half = gy.shape[1]
    cols, ocols = dwd.shape[0], dwo.shape[0]
    wgu = weights.at[pl.ds(0, 2 * cols)]
    wd = weights.at[pl.ds(2 * cols, cols)]
    wo = weights.at[pl.ds(3 * cols, ocols)]
    s_gy, s_x, s_p = (sent.at[i] for i in range(3))
    s_h = s_t = s_gy
    s_ds = s_x
    quarter = half // 2
    me = lax.axis_index("tp")
    right = lax.rem(me + 2, tp)
    left = lax.rem(me + tp - 2, tp)
    partner = me + 1 - 2 * lax.rem(me, 2)
    slot_row = functools.partial(slot_token, tp, half)

    def send(src, dst, ssem, rsem, dev):
        return pltpu.make_async_remote_copy(
            src_ref=src, dst_ref=dst, send_sem=ssem, recv_sem=rsem, device_id={"tp": dev}, device_id_type=MESH)

    def u_copies(k):
        tokens = pl.ds(slot_row(k), half)
        at = lax.rem(k, 2)
        return (pltpu.make_async_copy(ug_hbm.at[:, tokens], ub.at[at, 0], l_u.at[at]),
                pltpu.make_async_copy(uu_hbm.at[:, tokens], ub.at[at, 1], l_u.at[at]))

    def o_copy(n):
        tokens = pl.ds(pl.multiple_of(slot_row(n // 2) + lax.rem(n, 2) * quarter, quarter), quarter)
        return pltpu.make_async_copy(o_hbm.at[:, tokens], ob.at[n], l_w)

    def own(hbm, h):
        return hbm.at[pl.ds(h * half, half)]

    barrier = pltpu.get_barrier_semaphore()
    for dev in (left, right, partner):
        pl.semaphore_signal(barrier, inc=1, device_id={"tp": dev}, device_id_type=MESH)
    pl.semaphore_wait(barrier, 3)

    def send_own(hbm, buf, ssem, rsem):
        for src, dst, dev in ((0, 4, right), (1, 5, left), (1, 8, right), (0, 9, left), (0, 2, partner), (1, 3, partner)):
            send(own(hbm, src), buf.at[dst], ssem, rsem.at[dst // 2], dev).start()

    def arrived(ref, rsem):
        pltpu.make_async_copy(ref, ref, rsem).wait()

    def left_here(ref, ssem):
        send(ref, ref, ssem, ssem, partner).wait_send()

    def gather_step(buf, ssem, rsem, k, also):
        place = lax.rem(k, 4)

        @pl.when((k >= 2) & (lax.rem(place, 2) == 0))
        def _():
            arrived(buf.at[pl.ds(k, 2)], rsem.at[k // 2])

        @pl.when(k == 4)
        def _():
            send(buf.at[4], buf.at[12], ssem, rsem.at[6], right).start()
            send(buf.at[5], buf.at[13], ssem, rsem.at[6], left).start()

        @pl.when((k >= 4) & (place == 0))
        def _():
            for d in range(2):
                send(buf.at[k + d], buf.at[k + 2 + d], ssem, rsem.at[k // 2 + 1], partner).start()
            if also is not None:
                pl.when(k == 4)(also)

    send_own(gy_hbm, gy, s_gy, r_gy)
    for h in range(2):
        pltpu.make_async_copy(own(gy_hbm, h), gy.at[h], r_gy.at[0]).start()
        pltpu.make_async_copy(own(x_hbm, h), xb.at[h], r_x.at[0]).start()
    for i, src in enumerate((wg_hbm, wu_hbm, wd_hbm, wo_hbm)):
        pltpu.make_async_copy(src, weights.at[pl.ds(i * cols, src.shape[0])], l_w).start()
    for c in u_copies(0):
        c.start()
    dwd[...] = jnp.zeros_like(dwd)
    dwgu[...] = jnp.zeros_like(dwgu)
    dwo[...] = jnp.zeros_like(dwo)
    arrived(weights, l_w)
    arrived(gy.at[pl.ds(0, 2)], r_gy.at[0])
    arrived(xb.at[pl.ds(0, 2)], r_x.at[0])

    pltpu.make_async_copy(xin_hbm, tok.at[0], r_gy.at[0]).start()
    pltpu.make_async_copy(gr_hbm, tok.at[1], r_gy.at[0]).start()
    pltpu.make_async_copy(gamma_hbm, gamma_ref, r_x.at[0]).start()

    @pl.loop(0, 32)
    def _(n):
        o_copy(n).start()

    def part_copy(k):
        j = (k // 4) * 2 + lax.rem(k, 2)
        return send(part.at[k], peer.at[j], s_p, r_p, partner)

    @pl.loop(0, 16)
    def _(k):
        @pl.when(k + 1 < 16)
        def _():
            for c in u_copies(k + 1):
                c.start()

        @pl.when((k > 0) & (lax.rem(k + 3, 4) >= 2))
        def _():
            part_copy(k - 1).start()

        gather_step(gy, s_gy, r_gy, k, lambda: send_own(x_hbm, xb, s_x, r_x))
        at = lax.rem(k, 2)
        arrived(ub.at[at], l_u.at[at])
        gyk = gy[k]
        gh = dot(wd[...], gyk, COLS_COLS)
        gate = ub[at, 0].astype(F32)
        up = ub[at, 1].astype(F32)
        sig = jax.nn.sigmoid(gate)
        act = gate * sig
        silu = sig * (1.0 + gate * (1.0 - sig))
        z = (act * up).astype(BF16)
        du_up = (gh * act).astype(BF16)
        du_gate = (gh * up * silu).astype(BF16)
        du[k, pl.ds(0, cols)] = du_gate
        du[k, pl.ds(cols, cols)] = du_up
        dwd[...] += dot(z, gyk, COLS_ROWS)
        part[k] = dot(du[k], wgu[...], ROWS_ROWS).astype(BF16)

    part_copy(15).start()

    left_here(gy.at[pl.ds(0, 14)], s_gy)

    def add_peer(k, more=()):
        j = (k // 4) * 2 + k % 2
        t = part[k].astype(F32) + peer[j].astype(F32)
        for m in more:
            t = t + m[...].astype(F32)
        part[k] = t.astype(BF16)

    def q(ref, i):
        return ref.at[pl.ds(i * quarter, quarter)]

    arrived(peer, r_p)

    for k in (12, 13):
        add_peer(k)
    for side, dev in enumerate((right, left)):
        send(part.at[12 + side], hop.at[side], s_h, r_h, dev).start()

    def dw_step(j):
        xk = xb[pl.ds(2 * j, 2)].reshape(2 * half, xb.shape[2])
        duk = jnp.concatenate((du[2 * j], du[2 * j + 1]), axis=1)
        dwgu[...] += dot(duk, xk, COLS_ROWS)

    def tail_copy(side, qi):
        k = ((9, 5), (4, 8))[side][qi // 2]
        return send(q(part.at[k], qi % 2), frm.at[qi % 2, qi // 2, side], s_t, r_t.at[qi % 2], (right, left)[side])

    tail_order = ((2, 0, 3, 1), (0, 2, 1, 3))

    def tails():
        add_peer(5)
        add_peer(4)
        arrived(hop, r_h)
        add_peer(9, (hop.at[0],))
        add_peer(8, (hop.at[1],))
        for n in range(4):
            for side in range(2):
                tail_copy(side, tail_order[side][n]).start()

    @pl.loop(0, 8)
    def _(j):
        pl.when(j == 6)(tails)
        gather_step(xb, s_x, r_x, 2 * j, None)
        dw_step(j)

    ds = gy
    arrived(tok, r_gy.at[0])
    arrived(gamma_ref, r_x.at[0])
    left_here(xb.at[pl.ds(0, 14)], s_x)
    left_here(peer, s_p)
    gamma = gamma_ref[...].astype(F32).reshape(1, gamma_ref.shape[0])

    def norm_quarter(qi):
        h, i = qi // 2, qi % 2
        step = 32

        @pl.loop(0, quarter // step)
        def _(n):
            rows = pl.ds(pl.multiple_of(n * step, step), step)
            inner = pl.ds(pl.multiple_of(i * quarter + n * step, step), step)
            tokens = pl.ds(pl.multiple_of(qi * quarter + n * step, step), step)
            dx = (part[h, inner].astype(F32) + peer[h, inner].astype(F32)
                  + frm[i, h, 0, rows].astype(F32) + frm[i, h, 1, rows].astype(F32)).astype(BF16)
            xf = tok[0, tokens].astype(F32)
            inv = lax.rsqrt(jnp.mean(xf * xf, axis=-1, keepdims=True) + NORM_EPS)
            scaled = dx.astype(F32) * gamma
            proj = jnp.mean(scaled * xf, axis=-1, keepdims=True)
            out = (tok[1, tokens].astype(F32) + inv * (scaled - xf * (inv * inv) * proj)).astype(BF16)
            ds[h, inner] = out
            dso[tokens] = out

    def ds_copy(src, dst, i, dev):
        return send(q(ds.at[src], i), q(ds.at[dst], i), s_ds, r_gy.at[dst // 2 + 7 * i], dev)

    for i in range(2):
        arrived(frm.at[i], r_t.at[i])
        for h in (0, 1):
            norm_quarter(2 * h + i)
        for src, dst, dev in ((0, 4, right), (1, 5, left), (1, 8, right), (0, 9, left), (0, 2, partner), (1, 3, partner)):
            ds_copy(src, dst, i, dev).start()

    arrived(ob, l_w)
    left_here(part.at[pl.ds(0, 6)], s_t)

    pieces = [(quarter * lo // 8, quarter * n // 8) for lo, n in ((0, 4), (4, 2), (6, 1), (7, 1))]
    r_e, r_late = [r_x.at[1 + e] for e in range(len(pieces))], r_x.at[5]

    def products(k, i):
        rows = pl.ds(pl.multiple_of(i * quarter, quarter), quarter)
        for d in range(2):
            block = ds[k + d, rows]
            n = 2 * (k + d) + i
            tokens = pl.ds(pl.multiple_of(slot_row(k + d) + i * quarter, quarter), quarter)
            dob[:, tokens] = dot(wo[...], block, COLS_COLS).astype(BF16)
            dwo[...] += dot(ob[n], block, COLS_ROWS)

    @pl.loop(0, 14)
    def _(u):
        v, w = u - 4, u - 12
        i = jnp.where(u < 4, lax.rem(u, 2), jnp.where(u < 12, v // 4, w // 2))
        k = jnp.where(u < 4, 2 * (u // 2), jnp.where(u < 12, 4 + 2 * lax.rem(v, 4), 12 + 2 * lax.rem(w, 2)))

        @pl.when(k > 0)
        def _():
            rows = pl.ds(pl.multiple_of(i * quarter, quarter), quarter)
            arrived(ds.at[pl.ds(k, 2), rows], r_gy.at[k // 2 + 7 * i])

        @pl.when((k == 4) & (i == 0))
        def _():
            for src, dst, dev in ((4, 12, right), (5, 13, left)):
                ds_copy(src, dst, 0, dev).start()

        @pl.when((k == 4) & (i == 1))
        def _():
            for (lo, n), rsem in zip(pieces, r_e):
                rows = pl.ds(quarter + lo, n)
                for src, dst, dev in ((4, 12, right), (5, 13, left)):
                    send(ds.at[src, rows], ds.at[dst, rows], s_ds, rsem, dev).start()

        @pl.when((k > 0) & (lax.rem(k, 4) == 0))
        def _():
            for d in range(2):
                ds_copy(k + d, k + 2 + d, i, partner).start()

        products(k, i)

    for (lo, n), rsem in zip(pieces, r_e):
        rows = pl.ds(quarter + lo, n)
        arrived(ds.at[pl.ds(12, 2), rows], rsem)
        for d in range(2):
            send(ds.at[12 + d, rows], late.at[d, pl.ds(lo, n)], s_ds, r_late, partner).start()
    products(12, 1)
    left_here(ds.at[pl.ds(0, 14)], s_ds)
    arrived(late, r_late)


def solution(mesh):
    tp = mesh.shape["tp"]
    token_spec = P(("dp", "tp"), None)
    split_cols = P("dp", "tp")
    weight_cols = P(None, "tp")
    weight_rows = P("tp", None)

    def local_backward(x_norm, grad_y, u_gate, u_up, w_gate, w_up, w_down, x_in, gamma, grad_res, attn_out, w_out):
        rows, hid = x_norm.shape
        tokens, cols = u_gate.shape
        ocols = attn_out.shape[1]
        half = rows // 2
        quarter = half // 2
        any_spec = pl.BlockSpec(memory_space=pl.ANY)
        vmem_spec = pl.BlockSpec(memory_space=pltpu.VMEM)
        dma = pltpu.SemaphoreType.DMA
        results = pl.pallas_call(
            functools.partial(kernel, tp),
            out_shape=(
                pltpu.VMEM((rows, hid), BF16),
                pltpu.VMEM((ocols, tokens), BF16),
                pltpu.VMEM((2 * cols, hid), F32),
                pltpu.VMEM((cols, hid), F32),
                pltpu.VMEM((ocols, hid), F32),
                pltpu.VMEM((2, quarter, hid), BF16),
            ),
            in_specs=[any_spec] * 12,
            out_specs=(vmem_spec,) * 6,
            scratch_shapes=[
                pltpu.VMEM((16, half, hid), BF16),
                pltpu.VMEM((16, half, hid), BF16),
                pltpu.VMEM((16, half, hid), BF16),
                pltpu.VMEM((8, half, hid), BF16),
                pltpu.VMEM((2, half, hid), BF16),
                pltpu.VMEM((2, 2, 2, quarter, hid), BF16),
                pltpu.VMEM((16, 2 * cols, half), BF16),
                pltpu.VMEM((3 * cols + ocols, hid), BF16),
                pltpu.VMEM((2, 2, cols, half), BF16),
                pltpu.VMEM((32, ocols, quarter), BF16),
                pltpu.VMEM((2, rows, hid), BF16),
                pltpu.VMEM((hid,), BF16),
                dma((3,)),
                dma((13,)), dma((8,)), dma((2,)), dma, dma, dma((2,)), dma,
            ],
            compiler_params=pltpu.CompilerParams(
                collective_id=0, has_side_effects=True, vmem_limit_bytes=54_000_000),
            name="layer_backward",
        )(x_norm, grad_y, u_gate.T, u_up.T, w_gate.T, w_up.T, w_down, x_in, gamma, grad_res, attn_out.T,
          w_out)
        results = [pltpu.with_memory_space_constraint(r, pltpu.VMEM) for r in (*results, attn_out.T, w_out)]
        ds, do, dwg, dwu, dwd, dwo = pl.pallas_call(
            functools.partial(write_kernel, tp, half),
            out_shape=(
                jax.ShapeDtypeStruct((rows, hid), BF16),
                jax.ShapeDtypeStruct((ocols, tokens), BF16),
                jax.ShapeDtypeStruct((cols, hid), F32),
                jax.ShapeDtypeStruct((cols, hid), F32),
                jax.ShapeDtypeStruct((cols, hid), F32),
                jax.ShapeDtypeStruct((ocols, hid), F32),
            ),
            in_specs=[vmem_spec] * 8,
            out_specs=(any_spec,) * 6,
            scratch_shapes=[
                pltpu.VMEM((2, ocols, quarter), BF16),
                pltpu.VMEM((ocols, hid), F32),
                dma,
            ],
            compiler_params=pltpu.CompilerParams(vmem_limit_bytes=4_000_000),
            name="write_results",
        )(*results)
        return ds, do.T, dwg.T, dwu.T, dwd, dwo

    return jax.shard_map(
        local_backward,
        mesh=mesh,
        in_specs=(token_spec, token_spec, split_cols, split_cols, weight_cols, weight_cols, weight_rows,
                  token_spec, P(None), token_spec, split_cols, weight_rows),
        out_specs=(token_spec, split_cols, split_cols, split_cols, token_spec, token_spec),
        check_vma=False,
    )
```
